32 devices in a mesh: seq: 8 (over z, y), head: 4 (over x, core).
Axes of the slice: x: 2, y: 2, z: 4, core: 2. Of those that a mesh axis runs over, the one named last changes fastest.
Arguments:
- hidden_in: bfloat16 [4096, 1536], P('seq', 'head'), may hold values from -6 to 6
- norm_gain: bfloat16 [1536], P('head'), may hold values from 0.5 to 1.5
- gate_weight: bfloat16 [1536, 3072], P(None, 'head'), may hold values from -0.15625 to 0.15625
- value_weight: bfloat16 [1536, 3072], P(None, 'head'), may hold values from -0.15625 to 0.15625
- step_weight: bfloat16 [1536, 48], P(None, 'head'), may hold values from -0.15625 to 0.15625
- state_weight: bfloat16 [1536, 256], replicated, may hold values from -0.15625 to 0.15625
- value_filter: float32 [4, 3072], P(None, 'head'), may hold values from -3 to 3
- value_offset: float32 [3072], P('head'), may hold values from -0.5 to 0.5
- state_filter: float32 [4, 256], replicated, may hold values from -3 to 3
- state_offset: float32 [256], replicated, may hold values from -0.5 to 0.5
- step_bias: float32 [48], P('head'), may hold values from -1 to 0.5
- decay_log: float32 [48], P('head'), as said below
- skip_gain: float32 [48], P('head'), may hold values from 0.5 to 1.5
- mix_gain: float32 [3072], P('head'), may hold values from 0.5 to 1.5
- out_weight: bfloat16 [3072, 1536], P('head'), may hold values from -0.109375 to 0.109375
- lengths: int32 [4], replicated, may hold values from 1 to 2048, 4096 in all
- cotangent: bfloat16 [4096, 1536], P('seq', 'head'), may hold values from -6 to 6
Outputs:
- block_out: bfloat16 [4096, 1536], P('seq', 'head')
- delta_hidden: float32 [4096, 1536], P('seq', 'head')
- delta_norm_gain: float32 [1536], P('head')
- delta_gate_weight: float32 [1536, 3072], P(None, 'head')
- delta_value_weight: float32 [1536, 3072], P(None, 'head')
- delta_step_weight: float32 [1536, 48], P(None, 'head')
- delta_state_weight: float32 [1536, 256], replicated
- delta_value_filter: float32 [4, 3072], P(None, 'head')
- delta_value_offset: float32 [3072], P('head')
- delta_state_filter: float32 [4, 256], replicated
- delta_state_offset: float32 [256], replicated
- delta_step_bias: float32 [48], P('head')
- delta_decay_log: float32 [48], P('head')
- delta_skip_gain: float32 [48], P('head')
- delta_mix_gain: float32 [3072], P('head')
- delta_out_weight: float32 [3072, 1536], P('head')
The draws below stay inside these ranges and needn't reach their ends.
Inputs may be any that keep to these rules, and one draw needn't show every extreme that they name: `lengths`: they sum to 4096; the longest has exactly 2048 tokens. `decay_log`: one value for each head, between log(0.25 / 4096) and log(1 / 25).
All inputs are finite; a program needn't handle non-finite values.
Results may differ from the reference program's by a relative error of at most 0.01.
Values may be sent and summed in bfloat16 or wider, within the bound.
A program may use at most 128 MiB of HBM per device.

```python
import math
import jax
import jax.numpy as jnp
import numpy as np
from jax import lax

D = 1536
HEADS = 48
HEAD_DIM = 64
STATE = 128
CONV_WIDTH = 4
SPAN = 256
SEQS = 4
INNER = 3072
TOKENS = 4096
LONGEST = 2048


def draw_decay_log(key, part):
    pick_key, rate_key = jax.random.split(jax.random.fold_in(key, 17))
    uniform_pick = jax.random.uniform(pick_key, (HEADS,), jnp.float32)
    uniform_rate = jax.random.uniform(rate_key, (HEADS,), jnp.float32)
    forgetful = uniform_pick < 0.5
    slow_log = jnp.log(0.25 / TOKENS) + uniform_rate * jnp.log(8.0)
    fast_log = jnp.log(1.0 / 50.0) + uniform_rate * jnp.log(2.0)
    return jnp.where(forgetful, fast_log, slow_log).astype(jnp.float32)


def shard_levels(rng, extent, pieces, smallest, largest):
    gain, own = 1.0, jax.random.fold_in(rng, 6)
    for dim, parts in pieces:
        draws = jnp.exp(jax.random.uniform(jax.random.fold_in(own, dim), (parts,), jnp.float32, smallest / len(pieces), largest / len(pieces)))
        gain = gain * jnp.repeat(draws, extent[dim] // parts).reshape([-1 if axis == dim else 1 for axis in range(len(extent))])
    return gain


def profile(count, total, reach, lean):
    weights = [(1 << 20) // math.isqrt(rank ** lean) + 1 for rank in range(2, count + 1)]
    spare, counts = total - reach - (count - 1), [1] * (count - 1)
    while spare > 0:
        movable = [i for i in range(count - 1) if counts[i] < reach]
        whole, budget = sum([weights[i] for i in movable]), spare
        for i in movable:
            more = min(reach - counts[i], max(1, budget * weights[i] // whole), spare)
            counts[i] = counts[i] + more
            spare = spare - more
    return np.array([reach] + counts)


def uneven(key, number_of, total, most, slope):
    if number_of == 2:
        one = jax.random.randint(key, (), max(1, total - most), min(most, total - 1) + 1)
        return jnp.stack([one, total - one])
    sizes = jnp.asarray(profile(number_of, total, most, slope), jnp.int32)
    couples = (number_of - 1) // 2
    giver, taker = sizes[1:1 + 2 * couples:2], sizes[2:2 + 2 * couples:2]
    room = jnp.minimum(giver - 1, most - taker)
    shifted = jax.random.randint(jax.random.fold_in(key, 1), (couples,), 0, 1 << 20) % (room + 1)
    sizes = sizes.at[1:1 + 2 * couples:2].set(giver - shifted).at[2:2 + 2 * couples:2].set(taker + shifted)
    return sizes[jax.random.permutation(jax.random.fold_in(key, 2), number_of)]


def bell_draw(key, extent, spread, bound, cuts=(), kind=jnp.bfloat16):
    values = spread * jax.random.normal(key, extent, jnp.float32)
    if cuts:
        values = values * shard_levels(key, extent, cuts, -0.22, 0.18)
    return jnp.clip(values, -bound, bound).astype(kind)


def setup_inputs(seed: int = 0) -> dict:
    arg_keys = jax.random.split(jax.random.key(seed), 18)
    hidden_in = bell_draw(arg_keys[0], (TOKENS, D), 1.0, 6.0, ((0, 8), (1, 4)))
    norm_gain = jnp.clip(1.0 + 0.1 * jax.random.normal(arg_keys[1], (D,), jnp.float32), 0.5, 1.5).astype(jnp.bfloat16)
    gate_weight = bell_draw(arg_keys[2], (D, INNER), D ** -0.5, 0.15625, ((1, 4),))
    value_weight = bell_draw(arg_keys[3], (D, INNER), D ** -0.5, 0.15625, ((1, 4),))
    step_weight = bell_draw(arg_keys[4], (D, HEADS), D ** -0.5, 0.15625, ((1, 4),))
    state_weight = bell_draw(arg_keys[5], (D, 2 * STATE), D ** -0.5, 0.15625)
    value_filter = bell_draw(arg_keys[6], (CONV_WIDTH, INNER), CONV_WIDTH ** -0.5, 3.0, ((1, 4),), jnp.float32)
    value_offset = jnp.clip(jax.random.uniform(arg_keys[7], (INNER,), jnp.float32, -0.5, 0.5) * shard_levels(arg_keys[7], (INNER,), ((0, 4),), -0.4, 0.0), -0.5, 0.5)
    state_filter = bell_draw(arg_keys[8], (CONV_WIDTH, 2 * STATE), CONV_WIDTH ** -0.5, 3.0, (), jnp.float32)
    state_offset = jnp.clip(jax.random.uniform(arg_keys[9], (2 * STATE,), jnp.float32, -0.5, 0.5), -0.5, 0.5)
    step_bias = jnp.clip(-1.0 + 1.5 * jax.random.uniform(arg_keys[10], (HEADS,), jnp.float32) ** shard_levels(arg_keys[10], (HEADS,), ((0, 4),), -0.2, 0.2), -1.0, 0.5)
    decay_log = draw_decay_log(jax.random.fold_in(arg_keys[17], 71), 0)
    skip_gain = jnp.clip(0.5 + 1.0 * jax.random.uniform(arg_keys[12], (HEADS,), jnp.float32) ** shard_levels(arg_keys[12], (HEADS,), ((0, 4),), -0.2, 0.2), 0.5, 1.5)
    mix_gain = jnp.clip(1.0 + 0.1 * jax.random.normal(arg_keys[13], (INNER,), jnp.float32), 0.5, 1.5)
    out_weight = bell_draw(arg_keys[14], (INNER, D), INNER ** -0.5, 0.109375, ((0, 4),))
    lengths = uneven(arg_keys[15], SEQS, TOKENS, LONGEST, 2).astype(jnp.int32)
    cotangent = bell_draw(arg_keys[16], (TOKENS, D), 1.0, 6.0, ((0, 8), (1, 4)))
    return dict(hidden_in=hidden_in, norm_gain=norm_gain, gate_weight=gate_weight, value_weight=value_weight, step_weight=step_weight, state_weight=state_weight, value_filter=value_filter, value_offset=value_offset, state_filter=state_filter, state_offset=state_offset, step_bias=step_bias, decay_log=decay_log, skip_gain=skip_gain, mix_gain=mix_gain, out_weight=out_weight, lengths=lengths, cotangent=cotangent)


EPS = 1e-05
HIGH = lax.Precision.HIGHEST

@jax.custom_vjp
def low(v):
    return lax.optimization_barrier(v.astype(jnp.bfloat16)).astype(jnp.float32)

@jax.custom_vjp
def low_back(v):
    return v

def low_keep(v):
    return (low(v), None)

def low_pass(kept, grad):
    return (grad,)

def back_keep(v):
    return (v, None)

def back_low(kept, grad):
    return (low(grad),)
low.defvjp(low_keep, low_pass)
low_back.defvjp(back_keep, back_low)

def matmul(left, right):
    return jnp.dot(left, right, precision=HIGH, preferred_element_type=jnp.float32)

def sequence_of(places, lengths):
    bounds = jnp.cumsum(lengths, dtype=jnp.int32)
    return lax.optimization_barrier(jnp.sum((places[:, None] >= bounds[None, :]).astype(jnp.int32), axis=1, dtype=jnp.int32))

def filter_apply(mixed_in, edge_rows, segment, edge_segment, filters, offsets):
    extended = jnp.concatenate([edge_rows, mixed_in], axis=0)
    ext_segment = jnp.concatenate([edge_segment, segment], axis=0)
    count = mixed_in.shape[0]
    summed = jnp.zeros_like(mixed_in) + offsets[None, :]
    for position in range(CONV_WIDTH):
        same_seq = (ext_segment[position:position + count] == segment).astype(jnp.float32)[:, None]
        summed = summed + filters[position][None, :] * extended[position:position + count] * same_seq
    return jax.nn.silu(summed)

def span_states(values, inflow, step_size, running, grouped, entering):
    last_sum = running[:, -1:, :]
    tail_mask = (grouped == grouped[:, -1:]).astype(jnp.float32)
    toward_end = jnp.exp(last_sum - running) * tail_mask[:, :, None] * step_size
    span_sums = jnp.einsum('cqh,cqhp,cqn->chpn', toward_end, values, inflow, precision=HIGH)
    passing = jnp.exp(running[:, -1, :]) * (grouped[:, -1] == entering).astype(jnp.float32)[:, None]

    def advance(carried, element):
        state_now, product_now = carried
        span_sum, factor = element
        return ((factor[:, None, None] * state_now + span_sum, factor * product_now), (state_now, product_now))
    initial = (jnp.zeros(span_sums.shape[1:], jnp.float32), jnp.ones(passing.shape[1:], jnp.float32))
    (state_end, product_end), (entries, products) = lax.scan(advance, initial, (span_sums, passing))
    return (entries, products, product_end, state_end)

def span_outputs(values, inflow, readout, step_size, running, grouped, entering, entries, products, incoming):
    starts = entries + products[:, :, None, None] * incoming[None]
    lower = jnp.arange(SPAN)[:, None] >= jnp.arange(SPAN)[None, :]
    together = (grouped[:, :, None] == grouped[:, None, :]) & lower[None]
    gaps = running[:, :, None, :] - running[:, None, :, :]
    decays = jnp.exp(jnp.where(together[..., None], gaps, 0.0)) * together[..., None].astype(jnp.float32)
    intersections = jnp.einsum('cin,cjn->cij', readout, inflow, precision=HIGH)
    mixing = decays * intersections[..., None] * step_size[:, None, :, :]
    result = jnp.einsum('cijh,cjhp->cihp', mixing, values, precision=HIGH)
    entering_mask = (grouped == entering[:, None]).astype(jnp.float32)
    carried = jnp.exp(running) * entering_mask[:, :, None]
    return result + carried[..., None] * jnp.einsum('cin,chpn->cihp', readout, starts, precision=HIGH)

def reference(hidden_in, norm_gain, gate_weight, value_weight, step_weight, state_weight, value_filter, value_offset, state_filter, state_offset, step_bias, decay_log, skip_gain, mix_gain, out_weight, lengths, cotangent):
    block_len = math.gcd(TOKENS, 4096)
    block_count = TOKENS // block_len
    spans = block_len // SPAN
    tail_rows = CONV_WIDTH - 1
    floats = (norm_gain.astype(jnp.float32), gate_weight.astype(jnp.float32), value_weight.astype(jnp.float32), step_weight.astype(jnp.float32), state_weight.astype(jnp.float32), value_filter.astype(jnp.float32), value_offset.astype(jnp.float32), state_filter.astype(jnp.float32), state_offset.astype(jnp.float32), step_bias.astype(jnp.float32), decay_log.astype(jnp.float32), skip_gain.astype(jnp.float32), mix_gain.astype(jnp.float32), out_weight.astype(jnp.float32))
    hidden_all = hidden_in.astype(jnp.float32)
    segment_all = sequence_of(jnp.arange(TOKENS, dtype=jnp.int32), lengths)

    def forward(params, hidden_rows):
        gain_in, gate_matrix, value_matrix, step_matrix, state_matrix, filter_value, offset_value, filter_state, offset_state, bias_step, rate_log, skip_term, gain_mix, out_matrix = params
        filters = jnp.concatenate([filter_value, filter_state], axis=1)
        offsets = jnp.concatenate([offset_value, offset_state], axis=0)

        def block(carried, element):
            edge_rows, edge_segment, state_now, before = carried
            block_rows, segment = element
            scale_in = lax.rsqrt(lax.optimization_barrier(jnp.mean(block_rows * block_rows, axis=1, keepdims=True)) + EPS)
            normed = low(block_rows * scale_in * gain_in[None, :])
            gate_in = low_back(matmul(normed, gate_matrix))
            value_in = low_back(matmul(normed, value_matrix))
            state_in = low_back(matmul(normed, state_matrix))
            step_in = low_back(matmul(normed, step_matrix))
            mixed_in = jnp.concatenate([value_in, state_in], axis=1)
            activated = filter_apply(mixed_in, edge_rows, segment, edge_segment, filters, offsets)
            values = activated[:, :INNER].reshape(block_len, HEADS, HEAD_DIM)
            inflow = activated[:, INNER:INNER + STATE]
            readout = activated[:, INNER + STATE:]
            step_size = jax.nn.softplus(step_in + bias_step[None, :])
            log_decay = -jnp.exp(rate_log)[None, :] * step_size
            grouped = segment.reshape(spans, SPAN)
            entering = jnp.concatenate([jnp.reshape(before, (1,)), segment[:-1]]).reshape(spans, SPAN)[:, 0]
            running = jnp.cumsum(log_decay.reshape(spans, SPAN, HEADS), axis=1)
            values_c = values.reshape(spans, SPAN, HEADS, HEAD_DIM)
            inflow_c = inflow.reshape(spans, SPAN, STATE)
            readout_c = readout.reshape(spans, SPAN, STATE)
            steps_c = step_size.reshape(spans, SPAN, HEADS)
            entries, products, product_end, state_end = span_states(values_c, inflow_c, steps_c, running, grouped, entering)
            scanned = span_outputs(values_c, inflow_c, readout_c, steps_c, running, grouped, entering, entries, products, state_now)
            mixer = scanned.reshape(block_len, HEADS, HEAD_DIM) + skip_term[None, :, None] * values
            mixer = mixer.reshape(block_len, INNER)
            gated = mixer * jax.nn.silu(gate_in)
            scale_mix = lax.rsqrt(lax.optimization_barrier(jnp.mean(gated * gated, axis=1, keepdims=True)) + EPS)
            mix_out = low(gated * scale_mix * gain_mix[None, :])
            result = block_rows + matmul(mix_out, out_matrix)
            state_next = product_end[:, None, None] * state_now + state_end
            return ((mixed_in[block_len - tail_rows:], segment[block_len - tail_rows:], state_next, segment[block_len - 1]), result)
        initial = (jnp.zeros((tail_rows, INNER + 2 * STATE), jnp.float32), jnp.zeros((tail_rows,), jnp.int32), jnp.zeros((HEADS, HEAD_DIM, STATE), jnp.float32), jnp.zeros((), jnp.int32))
        ignored, results = lax.scan(jax.checkpoint(block), initial, (hidden_rows.reshape(block_count, block_len, D), segment_all.reshape(block_count, block_len)))
        return results.reshape(TOKENS, D)
    block_value, pullback = jax.vjp(forward, floats, hidden_all)
    deltas, delta_hidden = pullback(cotangent.astype(jnp.float32))
    return (block_value.astype(jnp.bfloat16), delta_hidden, deltas[0], deltas[1], deltas[2], deltas[3], deltas[4], deltas[5], deltas[6], deltas[7], deltas[8], deltas[9], deltas[10], deltas[11], deltas[12], deltas[13])
```

```python
import functools

import jax
import jax.numpy as jnp
from jax import lax
from jax.experimental import pallas as pl
from jax.experimental.pallas import tpu as pltpu
from jax.sharding import PartitionSpec as P

D = 1536
CONV_WIDTH = 4
SPAN = 256
INNER = 3072


EPS = 1e-05
HIGH = lax.Precision.HIGHEST


MESH = pl.DeviceIdType.MESH
LINE = 4


def sum_rows(jobs, lines, count_in, *refs):
    ins, outs = refs[:count_in], refs[count_in : 2 * count_in]
    scratch = refs[2 * count_in :]
    count = len(jobs)
    own, y_in, z_in, final = (scratch[k * count : (k + 1) * count] for k in range(4))
    (own_sem, ys, yr, zs, zr, gzs, gzr, gys, gyr, keep_sem) = scratch[4 * count :]
    seq = lax.axis_index("seq")
    z, y = seq // lines, seq % lines
    barrier = pltpu.get_barrier_semaphore()

    def at(zz, yy):
        return {"seq": zz * lines + yy}

    peers = [at(z, lax.rem(y + d, lines)) for d in range(1, lines)]
    peers += [at(lax.rem(z + d, LINE), y) for d in range(1, LINE)]
    for peer in peers:
        pl.semaphore_signal(barrier, inc=1, device_id=peer, device_id_type=MESH)
    pl.semaphore_wait(barrier, len(peers))

    def remote(src, dst, send, recv, peer):
        return pltpu.make_async_remote_copy(
            src_ref=src, dst_ref=dst, send_sem=send, recv_sem=recv, device_id=peer, device_id_type=MESH
        )

    sizes = []
    for which, start, rows in jobs:
        sizes.append((which, start, rows, rows // lines, rows // lines // LINE))

    def y_copies(j):
        which, start, rows, part, piece = sizes[j]
        copies = []
        for d in range(1, lines):
            to = lax.rem(y + d, lines)
            copies.append(
                remote(
                    ins[which].at[pl.ds(start + to * part, part)],
                    y_in[j].at[d - 1],
                    ys.at[j, d - 1],
                    yr.at[j, d - 1],
                    at(z, to),
                )
            )
        return copies

    def own_copy(j):
        which, start, rows, part, piece = sizes[j]
        return pltpu.make_async_copy(
            ins[which].at[pl.ds(start + y * part, part)], own[j], own_sem.at[j]
        )

    def z_copies(j):
        piece = sizes[j][4]
        copies = []
        for d in (1, LINE - 1, 2):
            to = lax.rem(z + d, LINE)
            copies.append(
                remote(
                    own[j].at[pl.ds(to * piece, piece)],
                    z_in[j].at[d - 1],
                    zs.at[j, d - 1],
                    zr.at[j, d - 1],
                    at(to, y),
                )
            )
        return copies

    def place(j, zz, yy):
        which, start, rows, part, piece = sizes[j]
        return outs[which].at[pl.ds(start + yy * part + zz * piece, piece)]

    def gather_z(j):
        return [
            remote(final[j], place(j, z, y), gzs.at[j, d - 1], gzr.at[j, d - 1], at(lax.rem(z + d, LINE), y))
            for d in (1, LINE - 1, 2)
        ]

    def gather_y(j, d):
        source = lax.rem(z + LINE - d, LINE)
        src = final[j] if d == 0 else place(j, source, y)
        return [
            remote(
                src,
                place(j, source, y),
                gys.at[j, d, e - 1],
                gyr.at[j, d, e - 1],
                at(z, lax.rem(y + e, lines)),
            )
            for e in range(1, lines)
        ]

    def keep(j):
        return pltpu.make_async_copy(final[j], place(j, z, y), keep_sem.at[j])

    for j in range(count):
        own_copy(j).start()
        for copy in y_copies(j):
            copy.start()

    def reduce_y(j):
        own_copy(j).wait()
        for copy in y_copies(j):
            copy.wait_recv()
        part = sizes[j][3]
        tile = 16 if part % 16 == 0 else 8

        def step(i, carry):
            rows = pl.ds(pl.multiple_of(i * tile, tile), tile)
            total = own[j][rows].astype(jnp.float32)
            for d in range(lines - 1):
                total = total + y_in[j][d, rows].astype(jnp.float32)
            own[j][rows] = total.astype(jnp.bfloat16)
            return carry

        lax.fori_loop(0, part // tile, step, 0)
        for copy in z_copies(j):
            copy.start()

    def reduce_z(j):
        for copy in z_copies(j):
            copy.wait_recv()
        piece = sizes[j][4]
        tile = 16 if piece % 16 == 0 else 8
        base = z * piece

        def step(i, carry):
            rows = pl.ds(pl.multiple_of(i * tile, tile), tile)
            mine = pl.ds(pl.multiple_of(base + i * tile, tile), tile)
            total = own[j][mine].astype(jnp.float32)
            for d in range(LINE - 1):
                total = total + z_in[j][d, rows].astype(jnp.float32)
            final[j][rows] = total.astype(jnp.bfloat16)
            return carry

        lax.fori_loop(0, piece // tile, step, 0)
        keep(j).start()
        for copy in gather_z(j):
            copy.start()
        for copy in gather_y(j, 0):
            copy.start()

    def forward(j):
        copies = dict(zip((1, LINE - 1, 2), gather_z(j)))
        for d in (1, LINE - 1, 2):
            copies[d].wait_recv()
            for copy in gather_y(j, d):
                copy.start()

    for i in range(count + 2):
        if i < count:
            reduce_y(i)
        if 0 <= i - 1 < count:
            reduce_z(i - 1)
        if 0 <= i - 2 < count:
            forward(i - 2)
    for j in range(count):
        keep(j).wait()
        for copy in y_copies(j) + z_copies(j) + gather_z(j):
            copy.wait_send()
        for d in range(LINE):
            for copy in gather_y(j, d):
                copy.wait_recv()
                copy.wait_send()


def sum_over_seq(arrays, lines, split, collective_id):
    jobs = []
    for which, (array, parts) in enumerate(zip(arrays, split)):
        rows = array.shape[0] // parts
        jobs += [(which, k * rows, rows) for k in range(parts)]
    count = len(jobs)
    widths = [arrays[job[0]].shape[1] for job in jobs]
    bf16 = jnp.bfloat16
    scratch = [pltpu.VMEM((job[2] // lines, w), bf16) for job, w in zip(jobs, widths)]
    scratch += [pltpu.VMEM((lines - 1, job[2] // lines, w), bf16) for job, w in zip(jobs, widths)]
    scratch += [
        pltpu.VMEM((LINE - 1, job[2] // lines // LINE, w), bf16) for job, w in zip(jobs, widths)
    ]
    scratch += [pltpu.VMEM((job[2] // lines // LINE, w), bf16) for job, w in zip(jobs, widths)]
    dma = pltpu.SemaphoreType.DMA
    scratch += [
        dma((count,)),
        dma((count, lines - 1)),
        dma((count, lines - 1)),
        dma((count, LINE - 1)),
        dma((count, LINE - 1)),
        dma((count, LINE - 1)),
        dma((count, LINE - 1)),
        dma((count, LINE, lines - 1)),
        dma((count, LINE, lines - 1)),
        dma((count,)),
    ]
    anywhere = pl.BlockSpec(memory_space=pl.ANY)
    return pl.pallas_call(
        functools.partial(sum_rows, jobs, lines, len(arrays)),
        out_shape=[jax.ShapeDtypeStruct(array.shape, bf16) for array in arrays],
        in_specs=[anywhere] * len(arrays),
        out_specs=[anywhere] * len(arrays),
        scratch_shapes=scratch,
        compiler_params=pltpu.CompilerParams(
            collective_id=collective_id, has_side_effects=True, vmem_limit_bytes=60 * 1024 * 1024
        ),
    )(*arrays)


def shifted(value, axis, steps):
    count = lax.axis_size(axis)
    leading, last = (max(0, -steps), min(count, count - steps))
    return lax.ppermute(value, axis, [(source, source + steps) for source in range(leading, last)])


def sequence_of(places, lengths):
    bounds = jnp.cumsum(lengths, dtype=jnp.int32)
    return jnp.sum((places[:, None] >= bounds[None, :]).astype(jnp.int32), axis=1, dtype=jnp.int32)


def filter_apply(mixed_in, edge_rows, segment, edge_segment, filters, offsets):
    extended = jnp.concatenate([edge_rows, mixed_in], axis=0)
    ext_segment = jnp.concatenate([edge_segment, segment], axis=0)
    count = mixed_in.shape[0]
    summed = jnp.zeros_like(mixed_in) + offsets[None, :]
    for position in range(CONV_WIDTH):
        same_seq = (ext_segment[position : position + count] == segment).astype(jnp.float32)[
            :, None
        ]
        summed = (
            summed + filters[position][None, :] * extended[position : position + count] * same_seq
        )
    return jax.nn.silu(summed)


def span_states(values, inflow, step_size, running, grouped, entering):
    last_sum = running[:, -1:, :]
    tail_mask = (grouped == grouped[:, -1:]).astype(jnp.float32)
    toward_end = jnp.exp(last_sum - running) * tail_mask[:, :, None] * step_size
    span_sums = jnp.einsum("cqh,cqhp,cqn->chpn", toward_end, values, inflow, precision=HIGH)
    passing = jnp.exp(running[:, -1, :]) * (grouped[:, -1] == entering).astype(jnp.float32)[:, None]

    def advance(carried, element):
        state_now, product_now = carried
        span_sum, factor = element
        return (
            (factor[:, None, None] * state_now + span_sum, factor * product_now),
            (state_now, product_now),
        )

    initial = (
        jnp.zeros(span_sums.shape[1:], jnp.float32),
        jnp.ones(passing.shape[1:], jnp.float32),
    )
    (state_end, product_end), (entries, products) = lax.scan(advance, initial, (span_sums, passing))
    return (entries, products, product_end, state_end)


def span_outputs(
    values, inflow, readout, step_size, running, grouped, entering, entries, products, incoming
):
    starts = entries + products[:, :, None, None] * incoming[None]
    lower = jnp.arange(SPAN)[:, None] >= jnp.arange(SPAN)[None, :]
    together = (grouped[:, :, None] == grouped[:, None, :]) & lower[None]
    gaps = running[:, :, None, :] - running[:, None, :, :]
    decays = jnp.exp(jnp.where(together[..., None], gaps, 0.0)) * together[..., None].astype(
        jnp.float32
    )
    intersections = jnp.einsum("cin,cjn->cij", readout, inflow, precision=HIGH)
    mixing = decays * intersections[..., None] * step_size[:, None, :, :]
    result = jnp.einsum("cijh,cjhp->cihp", mixing, values, precision=HIGH)
    entering_mask = (grouped == entering[:, None]).astype(jnp.float32)
    carried = jnp.exp(running) * entering_mask[:, :, None]
    return result + carried[..., None] * jnp.einsum(
        "cin,chpn->cihp", readout, starts, precision=HIGH
    )


def carry_chain(factors, pushed, direction):
    count = lax.axis_size("seq")
    window = count // 2
    factor, total, width = factors, pushed, 1
    while width < window // 2:
        from_far, factor_far = (
            shifted(total, "seq", direction * width),
            shifted(factor, "seq", direction * width),
        )
        total = total + factor[:, None, None] * from_far
        factor = factor * factor_far
        width *= 2
    near = shifted(total, "seq", direction)
    near_factor = shifted(factor, "seq", direction)
    far = shifted(total, "seq", direction * (1 + width))
    return near + near_factor[:, None, None] * far


def contract_rows(left, right):
    return lax.dot_general(
        left, right, (((0,), (0,)), ((), ())), preferred_element_type=jnp.float32
    )


def contract_cols(left, right):
    return lax.dot_general(
        left, right, (((1,), (1,)), ((), ())), preferred_element_type=jnp.float32
    )


def local(
    hidden_in,
    norm_gain,
    gate_weight,
    value_weight,
    step_weight,
    state_weight,
    value_filter,
    value_offset,
    state_filter,
    state_offset,
    step_bias,
    decay_log,
    skip_gain,
    mix_gain,
    out_weight,
    lengths,
    cotangent,
):
    tokens_dev = hidden_in.shape[0]
    width_dev = hidden_in.shape[1]
    heads_dev = step_weight.shape[1]
    inner_dev = value_weight.shape[1]
    head_size = inner_dev // heads_dev
    state_size = state_weight.shape[1] // 2
    spans = tokens_dev // SPAN
    tail_rows = CONV_WIDTH - 1
    anchor = lax.axis_index("seq") * tokens_dev
    segment = sequence_of(anchor + jnp.arange(tokens_dev, dtype=jnp.int32), lengths)
    edge_segment = sequence_of(anchor - tail_rows + jnp.arange(tail_rows, dtype=jnp.int32), lengths)
    before = sequence_of(jnp.reshape(anchor - 1, (1,)), lengths)
    grouped = segment.reshape(spans, SPAN)
    entering = jnp.concatenate([before, segment[:-1]]).reshape(spans, SPAN)[:, 0]
    gathered, gain_full = (
        lax.all_gather(hidden_in, "head", axis=1, tiled=True),
        lax.all_gather(norm_gain, "head", axis=0, tiled=True),
    )
    gathered_f = gathered.astype(jnp.float32)
    scale_in = lax.rsqrt(jnp.mean(gathered_f * gathered_f, axis=1, keepdims=True) + EPS)
    normed = (gathered_f * scale_in * gain_full.astype(jnp.float32)[None, :]).astype(jnp.bfloat16)
    gate_in = jnp.dot(normed, gate_weight, preferred_element_type=jnp.float32)
    value_in = jnp.dot(normed, value_weight, preferred_element_type=jnp.float32)
    state_in = jnp.dot(normed, state_weight, preferred_element_type=jnp.float32)
    step_in = jnp.dot(normed, step_weight, preferred_element_type=jnp.float32)
    mixed_in = jnp.concatenate([value_in, state_in], axis=1)
    edge_rows = shifted(mixed_in[tokens_dev - tail_rows :], "seq", 1)
    filters = jnp.concatenate([value_filter, state_filter], axis=1)
    offsets = jnp.concatenate([value_offset, state_offset], axis=0)

    def front(mixed_part, edge_part, filter_part, offset_part, step_part, bias_part, rate_part):
        activated = filter_apply(
            mixed_part, edge_part, segment, edge_segment, filter_part, offset_part
        )
        step_size = jax.nn.softplus(step_part + bias_part[None, :])
        return (activated, step_size, -jnp.exp(rate_part)[None, :] * step_size)

    (activated, step_size, log_decay), front_back = jax.vjp(
        front, mixed_in, edge_rows, filters, offsets, step_in, step_bias, decay_log
    )
    values = activated[:, :inner_dev].reshape(spans, SPAN, heads_dev, head_size)
    inflow = activated[:, inner_dev : inner_dev + state_size].reshape(spans, SPAN, state_size)
    readout = activated[:, inner_dev + state_size :].reshape(spans, SPAN, state_size)
    steps_c = step_size.reshape(spans, SPAN, heads_dev)
    logs_c = log_decay.reshape(spans, SPAN, heads_dev)

    def state_part(values_p, inflow_p, steps_p, logs_p):
        return span_states(
            values_p, inflow_p, steps_p, jnp.cumsum(logs_p, axis=1), grouped, entering
        )

    def output_part(
        values_p, inflow_p, readout_p, steps_p, logs_p, entries_p, products_p, incoming_p
    ):
        return span_outputs(
            values_p,
            inflow_p,
            readout_p,
            steps_p,
            jnp.cumsum(logs_p, axis=1),
            grouped,
            entering,
            entries_p,
            products_p,
            incoming_p,
        )

    (entries, products, product_end, state_end), states_back = jax.vjp(
        state_part, values, inflow, steps_c, logs_c
    )
    incoming = carry_chain(product_end, state_end, 1)
    scanned, outputs_back = jax.vjp(
        output_part, values, inflow, readout, steps_c, logs_c, entries, products, incoming
    )
    values_flat = values.reshape(tokens_dev, heads_dev, head_size)
    mixer = (
        scanned.reshape(tokens_dev, heads_dev, head_size) + skip_gain[None, :, None] * values_flat
    ).reshape(tokens_dev, inner_dev)
    gate_act = jax.nn.silu(gate_in)
    gated = mixer * gate_act
    cot_full = lax.all_gather(cotangent, "head", axis=1, tiled=True)
    d_mix = contract_cols(cot_full, out_weight)
    weighted_mix = d_mix * mix_gain[None, :]
    row_sums = lax.psum(
        jnp.stack([jnp.sum(gated * gated, axis=1), jnp.sum(weighted_mix * gated, axis=1)]), "head"
    )
    square_sum, mix_dot = row_sums[0], row_sums[1]
    scale_mix = lax.rsqrt(square_sum / INNER + EPS)[:, None]
    mix_out = (gated * scale_mix * mix_gain[None, :]).astype(jnp.bfloat16)
    partial_out = jnp.dot(mix_out, out_weight, preferred_element_type=jnp.float32)
    mixed_sum = lax.psum_scatter(
        partial_out.astype(jnp.bfloat16), "head", scatter_dimension=1, tiled=True
    ).astype(jnp.float32)
    own_rows = hidden_in.astype(jnp.float32)
    block_out = (own_rows + mixed_sum).astype(jnp.bfloat16)
    half = cot_full.shape[1] // 2
    out_part = jnp.concatenate(
        [contract_rows(mix_out, cot_full[:, :half]), contract_rows(mix_out, cot_full[:, half:])]
    ).astype(jnp.bfloat16)
    delta_mix_gain = jnp.sum(d_mix * gated * scale_mix, axis=0)
    d_gated = scale_mix * weighted_mix - gated * scale_mix**3 * (mix_dot / INNER)[:, None]
    d_mixer = d_gated * gate_act
    sigmoid_gate = jax.nn.sigmoid(gate_in)
    d_gate = (d_gated * mixer * sigmoid_gate * (1.0 + gate_in * (1.0 - sigmoid_gate))).astype(
        jnp.bfloat16
    )
    d_mixer3 = d_mixer.reshape(tokens_dev, heads_dev, head_size)
    delta_skip_gain = jnp.sum(d_mixer3 * values_flat, axis=(0, 2))
    d_values_a, d_inflow_a, d_readout, d_steps_a, d_logs_a, d_entries, d_products, d_incoming = (
        outputs_back(d_mixer3.reshape(spans, SPAN, heads_dev, head_size))
    )
    costate = carry_chain(product_end, d_incoming, -1)
    d_factor = jnp.sum(costate * incoming, axis=(1, 2))
    d_values_b, d_inflow_b, d_steps_b, d_logs_b = states_back(
        (d_entries, d_products, d_factor, costate)
    )
    d_shared = jnp.concatenate(
        [
            (d_inflow_a + d_inflow_b).reshape(tokens_dev, state_size),
            d_readout.reshape(tokens_dev, state_size),
        ],
        axis=1,
    )
    d_shared = lax.psum(d_shared, "head")
    d_values = (d_values_a + d_values_b).reshape(tokens_dev, inner_dev) + (
        skip_gain[None, :, None] * d_mixer3
    ).reshape(tokens_dev, inner_dev)
    d_activated = jnp.concatenate([d_values, d_shared], axis=1)
    d_steps = (d_steps_a + d_steps_b).reshape(tokens_dev, heads_dev)
    d_logs = (d_logs_a + d_logs_b).reshape(tokens_dev, heads_dev)
    d_mixed, d_edge, d_filters, d_offsets, d_step_in, delta_step_bias, delta_decay_log = front_back(
        (d_activated, d_steps, d_logs)
    )
    back_edge = shifted(d_edge, "seq", -1)
    d_mixed = d_mixed + jnp.pad(back_edge, ((tokens_dev - tail_rows, 0), (0, 0)))
    d_value = d_mixed[:, :inner_dev].astype(jnp.bfloat16)
    d_state = d_mixed[:, inner_dev:].astype(jnp.bfloat16)
    d_step_raw = d_step_in.astype(jnp.bfloat16)
    gate_part = contract_rows(normed, d_gate).astype(jnp.bfloat16)
    value_part = contract_rows(normed, d_value).astype(jnp.bfloat16)
    own_columns = lax.dynamic_slice_in_dim(normed, lax.axis_index("head") * width_dev, width_dev, 1)
    state_part_sum = contract_rows(own_columns, d_state)
    delta_step_weight = contract_rows(normed, d_step_raw)
    d_normed_part = (
        contract_cols(d_gate, gate_weight)
        + contract_cols(d_value, value_weight)
        + contract_cols(d_step_raw, step_weight)
    )
    d_normed = lax.psum_scatter(
        d_normed_part.astype(jnp.bfloat16), "head", scatter_dimension=1, tiled=True
    ).astype(jnp.float32)
    state_rows = lax.dynamic_slice_in_dim(
        state_weight, lax.axis_index("head") * width_dev, width_dev, 0
    )
    d_normed = d_normed + contract_cols(d_state, state_rows)
    gain_own = norm_gain.astype(jnp.float32)[None, :]
    delta_norm_gain = jnp.sum(d_normed * own_rows * scale_in, axis=0)
    weighted_in = d_normed * gain_own
    input_dot = lax.psum(jnp.sum(weighted_in * own_rows, axis=1), "head")
    delta_hidden = (
        cotangent.astype(jnp.float32)
        + scale_in * weighted_in
        - own_rows * scale_in**3 * (input_dot / D)[:, None]
    )
    small = (
        delta_norm_gain,
        delta_step_weight,
        d_filters,
        d_offsets,
        delta_step_bias,
        delta_decay_log,
        delta_skip_gain,
        delta_mix_gain,
    )
    packed = jnp.concatenate([jnp.reshape(part, (-1,)) for part in small])
    state_rows_packed = state_part_sum.size // inner_dev
    packed = jnp.pad(packed, (0, state_part_sum.size - packed.size))
    extra = jnp.concatenate(
        [state_part_sum.reshape(-1, inner_dev), packed.reshape(-1, inner_dev)]
    ).astype(jnp.bfloat16)
    lines = lax.axis_size("seq") // LINE
    extra, out_sum, gate_sum, value_sum = sum_over_seq(
        [extra, out_part, gate_part, value_part], lines, (1, 3, 3, 3), 3
    )
    delta_state_weight = lax.all_gather(
        extra[:state_rows_packed].reshape(width_dev, -1), "head", axis=0, tiled=True
    ).astype(jnp.float32)
    packed = extra[state_rows_packed:].reshape(-1).astype(jnp.float32)
    delta_out_weight = jnp.concatenate(jnp.split(out_sum, 2, axis=0), axis=1).astype(jnp.float32)
    delta_gate_weight = gate_sum.astype(jnp.float32)
    delta_value_weight = value_sum.astype(jnp.float32)
    pieces, start = [], 0
    for part in small:
        pieces.append(jnp.reshape(packed[start : start + part.size], part.shape))
        start += part.size
    norm_sum, step_sum, filter_sum, offset_sum, bias_sum, decay_sum, skip_sum, gain_sum = pieces
    return (
        block_out,
        delta_hidden,
        norm_sum,
        delta_gate_weight,
        delta_value_weight,
        step_sum,
        delta_state_weight,
        filter_sum[:, :inner_dev],
        offset_sum[:inner_dev],
        filter_sum[:, inner_dev:],
        offset_sum[inner_dev:],
        bias_sum,
        decay_sum,
        skip_sum,
        gain_sum,
        delta_out_weight,
    )


def solution(mesh):
    in_specs = (
        P("seq", "head"),
        P("head"),
        P(None, "head"),
        P(None, "head"),
        P(None, "head"),
        P(),
        P(None, "head"),
        P("head"),
        P(),
        P(),
        P("head"),
        P("head"),
        P("head"),
        P("head"),
        P("head", None),
        P(),
        P("seq", "head"),
    )
    out_specs = (
        P("seq", "head"),
        P("seq", "head"),
        P("head"),
        P(None, "head"),
        P(None, "head"),
        P(None, "head"),
        P(),
        P(None, "head"),
        P("head"),
        P(),
        P(),
        P("head"),
        P("head"),
        P("head"),
        P("head"),
        P("head", None),
    )
    return jax.shard_map(local, mesh=mesh, in_specs=in_specs, out_specs=out_specs, check_vma=False)
```

```python
import functools

import jax
import jax.numpy as jnp
from jax import lax
from jax.experimental import pallas as pl
from jax.experimental.pallas import tpu as pltpu
from jax.sharding import PartitionSpec as P

MESH = pl.DeviceIdType.MESH
F32, BF16 = jnp.float32, jnp.bfloat16
HIGH = lax.Precision.HIGHEST
EPS = 1e-05
Q = 128
LANES = 128
HEAD = 64
SUB = 8
FAR = -1e30
LINE = 4


def gather_kernel(peers_head, flat, count_in, *refs):
    ins, outs = refs[:count_in], refs[count_in : 2 * count_in]
    local_sem, send, recv = refs[2 * count_in :]
    head = lax.axis_index("head")
    chips = peers_head // 2
    x, core = head // 2, lax.rem(head, 2)
    partner = {"head": x * 2 + (1 - core)}
    across = [{"head": lax.rem(x + d, chips) * 2 + core} for d in range(1, chips)]
    barrier = pltpu.get_barrier_semaphore()
    for peer in [partner] + across:
        pl.semaphore_signal(barrier, inc=1, device_id=peer, device_id_type=MESH)
    pl.semaphore_wait(barrier, chips)

    def place(k, who):
        if flat[k]:
            width = ins[k].shape[1]
            return outs[k].at[:, pl.ds(pl.multiple_of(who * width, width), width)]
        return outs[k].at[who]

    def remote(src, dst, k, slot, peer):
        return pltpu.make_async_remote_copy(
            src_ref=src, dst_ref=dst, send_sem=send.at[k, slot], recv_sem=recv.at[k, slot],
            device_id=peer, device_id_type=MESH,
        )

    def first(k):
        copies = [remote(ins[k], place(k, head), k, d, across[d - 1]) for d in range(1, chips)]
        return copies + [remote(ins[k], place(k, head), k, 0, partner)]

    def second(k, d):
        source = lax.rem(x + chips - d, chips) * 2 + core
        return remote(place(k, source), place(k, source), k, chips - 1 + d, partner)

    own = [pltpu.make_async_copy(ins[k], place(k, head), local_sem.at[k]) for k in range(count_in)]
    for k in range(count_in):
        for copy in first(k):
            copy.start()
        own[k].start()
    for k in range(count_in):
        for d in range(1, chips):
            first(k)[d - 1].wait_recv()
            second(k, d).start()
    for k in range(count_in):
        own[k].wait()
        for copy in first(k):
            copy.wait_send()
        first(k)[-1].wait_recv()
        for d in range(1, chips):
            second(k, d).wait()


def gather_heads(arrays, peers_head, collective_id):
    flat = [array.ndim == 2 and array.shape[1] % 128 == 0 for array in arrays]
    shapes = [
        (a.shape[0], a.shape[1] * peers_head) if f else (peers_head,) + a.shape
        for a, f in zip(arrays, flat)
    ]
    count, chips = len(arrays), peers_head // 2
    dma = pltpu.SemaphoreType.DMA
    anywhere = pl.BlockSpec(memory_space=pl.ANY)
    gathered = pl.pallas_call(
        functools.partial(gather_kernel, peers_head, flat, count),
        out_shape=[jax.ShapeDtypeStruct(s, a.dtype) for s, a in zip(shapes, arrays)],
        in_specs=[anywhere] * count,
        out_specs=[anywhere] * count,
        scratch_shapes=[dma((count,)), dma((count, 2 * chips - 1)), dma((count, 2 * chips - 1))],
        compiler_params=pltpu.CompilerParams(collective_id=collective_id, has_side_effects=True),
    )(*arrays)
    return [
        g if f else jnp.moveaxis(g, 0, 1).reshape(a.shape[0], -1)
        for g, a, f in zip(gathered, arrays, flat)
    ]


def mm(left, right, contract=((1,), (0,)), precision=None):
    return lax.dot_general(
        left, right, (contract, ((), ())), precision=precision, preferred_element_type=F32
    )


def split(value):
    high = value.astype(BF16)
    return high, (value - high.astype(F32)).astype(BF16)


def twice(value, axis):
    return jnp.concatenate([value, value], axis=axis)


def sigmoid(v):
    return 1.0 / (1.0 + jnp.exp(-v))


def mixer_kernel(
    count, peers_head, inner,
    lengths, v_in, s_in, g_in, t_in, d_mix, taps_v, taps_s, off_v, off_s, bias, rate, skip, gain,
    mix_out, d_gate, d_value, d_state, d_step, grads_v, grads_s, grads_h,
    edge_v, edge_s, first_v, first_s, val, inf, inf_low, rea, rea_low, slope_v, slope_s, segs, mask_f, mask_b,
    step, sig, logs, run, run_t, tail, into, passing, pair, scaled, scaled_low, out, inter, d_u,
    states, starts, starts_low, before, total, factors, push, got, kept, prefix, spread_sum,
    rows_out, rows_in, pre_v, pre_s, back_v, back_s, back_in_v, back_in_s,
    edge_sems, p_send, p_recv, carry_send, carry_recv, row_send, row_recv, back_sems,
):
    tokens, channels = v_in.shape
    chunks, pairs, heads = tokens // Q, channels // LANES, channels // HEAD
    seq, head = lax.axis_index("seq"), lax.axis_index("head")
    window = count // 2
    steps = []
    width = window // 2
    while width >= 2:
        steps.append(width)
        width //= 2

    def remote(src, dst, send, recv, device):
        return pltpu.make_async_remote_copy(
            src_ref=src, dst_ref=dst, send_sem=send, recv_sem=recv, device_id=device, device_id_type=MESH
        )

    barrier = pltpu.get_barrier_semaphore()
    others = [{"seq": lax.rem(seq + d, count)} for d in range(1, count)]
    others += [{"head": lax.rem(head + d, peers_head)} for d in range(1, peers_head)]
    for other in others:
        pl.semaphore_signal(barrier, inc=1, device_id=other, device_id_type=MESH)
    pl.semaphore_wait(barrier, len(others))

    def edge_copies():
        there = {"seq": lax.rem(seq + 1, count)}
        return [
            remote(v_in.at[pl.ds(tokens - SUB, SUB)], edge_v, edge_sems.at[0], edge_sems.at[1], there),
            remote(s_in.at[pl.ds(tokens - SUB, SUB)], edge_s, edge_sems.at[2], edge_sems.at[3], there),
        ]

    @pl.when(seq < count - 1)
    def _():
        for copy in edge_copies():
            copy.start()

    lane = lax.broadcasted_iota(jnp.int32, (Q, LANES), 1)
    row = lax.broadcasted_iota(jnp.int32, (Q, LANES), 0)
    left = lane < HEAD

    anchor = seq * tokens
    bounds, bound = [], 0
    for k in range(lengths.shape[0]):
        bound = bound + lengths[k]
        bounds.append(bound)

    def sequence(places):
        number = jnp.zeros(places.shape, F32)
        for bound in bounds:
            number = number + jnp.where(places >= bound, 1.0, 0.0)
        return number

    places = lax.broadcasted_iota(jnp.int32, (tokens + 2 * SUB, LANES), 0) + (anchor - SUB)
    segs[...] = sequence(places)
    for k in range(3):
        same = segs[pl.ds(SUB, tokens)] == segs[pl.ds(SUB - 3 + k, tokens)]
        mask_f[k] = jnp.where(same, 1.0, 0.0)
        same = segs[pl.ds(0, tokens + SUB)] == segs[pl.ds(3 - k, tokens + SUB)]
        mask_b[k] = jnp.where(same, 1.0, 0.0)
    head_of = lax.broadcasted_iota(jnp.int32, (channels, LANES), 0) // HEAD
    column = lax.broadcasted_iota(jnp.int32, (channels, LANES), 1)
    spread_sum[...] = jnp.where(head_of == column, 1.0, 0.0).astype(BF16)
    grads_v[...] = jnp.zeros_like(grads_v)
    grads_s[...] = jnp.zeros_like(grads_s)

    raw = t_in[...] + bias[...]
    step[...] = jnp.maximum(raw, 0.0) + jnp.log1p(jnp.exp(-jnp.abs(raw)))
    sig[...] = sigmoid(raw)
    logs[...] = -jnp.exp(rate[...]) * step[...]
    lower = jnp.where(row >= lane, 1.0, 0.0)

    @pl.loop(0, chunks)
    def _(c):
        here = pl.ds(pl.multiple_of(c * Q, Q), Q)
        run[here] = mm(lower, logs[here], precision=HIGH)
        summed = run[here]
        run_t[c] = summed.T[:16]
        last = run[pl.ds(c * Q + Q - 1, 1)]
        mine = segs[pl.ds(pl.multiple_of(c * Q + SUB, SUB), Q)]
        at_end = segs[pl.ds(c * Q + SUB + Q - 1, 1)]
        entering = segs[pl.ds(c * Q + SUB - 1, 1)]
        tail[here] = jnp.exp(last - summed) * jnp.where(mine == at_end, 1.0, 0.0)
        into[here] = jnp.exp(summed) * jnp.where(mine == entering, 1.0, 0.0)
        through = jnp.exp(last) * jnp.where(at_end == entering, 1.0, 0.0)
        passing[c] = jnp.broadcast_to(through, (Q, LANES)).T[:16]

    product = jnp.ones((16, LANES), F32)
    for c in range(chunks):
        before[c] = product
        product = product * passing[c]
    factors[seq] = product

    def factor_copies():
        return [
            remote(
                factors.at[seq], factors.at[seq], p_send.at[d - 1], p_recv.at[d - 1],
                {"seq": lax.rem(seq + d, count)},
            )
            for d in range(1, count)
        ]

    for copy in factor_copies():
        copy.start()

    def convolve(source, base, rows, lanes, taps, offset):
        begin, size = rows
        summed = offset[:, lanes] + taps[3:4, lanes] * source[pl.ds(base, size), lanes]
        for k in range(3):
            term = taps[k : k + 1, lanes] * source[pl.ds(base - 3 + k, size), lanes]
            summed = summed + term * mask_f[k, pl.ds(begin, size)]
        s = sigmoid(summed)
        return summed * s, s * (1.0 + summed * (1.0 - s))

    def convolve_rows(c):
        rows = (c * Q, Q)
        span = pl.ds(c * Q, Q)

        @pl.loop(0, pairs)
        def _(b):
            lanes = pl.ds(pl.multiple_of(b * LANES, LANES), LANES)
            source, base = (v_in, c * Q) if c else (first_v, SUB)
            val[span, lanes], slope_v[span, lanes] = convolve(source, base, rows, lanes, taps_v, off_v)

        for b, (target, low) in enumerate(((inf, inf_low), (rea, rea_low))):
            lanes = pl.ds(b * LANES, LANES)
            source, base = (s_in, c * Q) if c else (first_s, SUB)
            active, slope_s[span, lanes] = convolve(source, base, rows, lanes, taps_s, off_s)
            target[span], low[span] = split(active)

    for c in range(1, chunks):
        convolve_rows(c)

    @pl.when(seq > 0)
    def _():
        for copy in edge_copies():
            copy.wait_recv()

    @pl.when(seq == 0)
    def _():
        edge_v[...] = jnp.zeros_like(edge_v)
        edge_s[...] = jnp.zeros_like(edge_s)

    first_v[pl.ds(0, SUB)] = edge_v[...]
    first_s[pl.ds(0, SUB)] = edge_s[...]
    first_v[pl.ds(SUB, Q)] = v_in[pl.ds(0, Q)]
    first_s[pl.ds(SUB, Q)] = s_in[pl.ds(0, Q)]
    convolve_rows(0)

    def both(ref, here, p):
        return jnp.where(left, ref[here, 2 * p : 2 * p + 1], ref[here, 2 * p + 1 : 2 * p + 2])

    def halves(value):
        return jnp.concatenate(
            [jnp.where(left, value, 0.0), jnp.where(left, 0.0, value)], axis=0
        ).astype(BF16)

    @pl.loop(0, chunks)
    def _(c):
        here = pl.ds(pl.multiple_of(c * Q, Q), Q)
        for p in range(pairs):
            lanes = pl.ds(p * LANES, LANES)
            weighted = both(step, here, p) * val[here, lanes]
            scaled[here, lanes], scaled_low[here, lanes] = split(both(tail, here, p) * weighted)
        states[c] = mm(
            twice(scaled[here], 0), jnp.concatenate([inf[here], inf_low[here]], axis=0), ((0,), (0,))
        )

    for h in range(heads):
        rows = pl.ds(h * HEAD, HEAD)
        held = jnp.zeros((HEAD, LANES), F32)
        for c in range(chunks):
            added = states[c, rows]
            states[c, rows] = held
            held = passing[c, h : h + 1] * held + added
        total[rows] = held

    def carry(direction):
        bank = 0 if direction == 1 else 1

        def reach(d):
            there = seq + direction * d
            return jnp.logical_and(there >= 0, there < count)

        def heard(d):
            there = seq - direction * d
            return jnp.logical_and(there >= 0, there < count)

        def copy(slot, d):
            source = min(slot, len(steps))
            return remote(
                push.at[bank, source], got.at[bank, slot],
                carry_send.at[bank, slot], carry_recv.at[bank, slot],
                {"seq": lax.rem(seq + direction * d + count, count)},
            )

        plan = [(k, d) for k, d in enumerate(steps)]
        ends = [(len(steps), 1), (len(steps) + 1, 2)]

        def send(slot, d):
            @pl.when(reach(d))
            def _():
                copy(slot, d).start()

        def factor(first, many, h):
            product = factors[first, h : h + 1]
            for i in range(1, many):
                product = product * factors[first - direction * i, h : h + 1]
            return product

        def launch(slot):
            push[bank, slot] = total[...].astype(BF16)
            if slot < len(steps):
                send(*plan[slot])
            else:
                for end in ends:
                    send(*end)

        def join(slot):
            d = plan[slot][1]

            @pl.when(heard(d))
            def _():
                copy(slot, d).wait_recv()
                for h in range(heads):
                    rows = pl.ds(h * HEAD, HEAD)
                    total[rows] = total[rows] + factor(seq, d, h) * got[bank, slot, rows].astype(F32)

            launch(slot + 1)

        def finish():
            total[...] = jnp.zeros_like(total)

            @pl.when(heard(1))
            def _():
                copy(*ends[0]).wait_recv()
                total[...] = got[bank, ends[0][0]].astype(F32)

            @pl.when(heard(2))
            def _():
                copy(*ends[1]).wait_recv()
                for h in range(heads):
                    rows = pl.ds(h * HEAD, HEAD)
                    far = got[bank, ends[1][0], rows].astype(F32)
                    total[rows] = total[rows] + factor(seq - direction, 1, h) * far

        def close():
            for slot, d in plan + ends:
                @pl.when(reach(d))
                def _(slot=slot, d=d):
                    copy(slot, d).wait_send()

        return launch, join, finish, close

    launch, join, finish, close_forward = carry(1)
    launch(0)

    def products(here):
        read = jnp.concatenate([rea[here], rea[here], rea_low[here]], axis=1)
        return mm(read, jnp.concatenate([inf[here], inf_low[here], inf[here]], axis=1), ((1,), (1,)))

    def from_state(high, low, c, lanes):
        state = jnp.concatenate([starts[c, lanes], starts_low[c, lanes], starts[c, lanes]], axis=1)
        return mm(jnp.concatenate([high, high, low], axis=1), state, ((1,), (1,)))

    def with_state(high, low, c, lanes):
        state = jnp.concatenate([starts[c, lanes], starts_low[c, lanes], starts[c, lanes]], axis=0)
        return mm(jnp.concatenate([high, high, low], axis=1), state)

    def within(c):
        here = pl.ds(pl.multiple_of(c * Q, Q), Q)
        mine = segs[pl.ds(pl.multiple_of(c * Q + SUB, SUB), Q)]
        across = sequence(lane + (anchor + c * Q))
        hidden = jnp.where(jnp.logical_and(mine == across, row >= lane), 0.0, FAR)
        cross = products(here)
        for p in range(pairs):
            lanes = pl.ds(p * LANES, LANES)
            mixing = []
            for h in (2 * p, 2 * p + 1):
                gap = (run[here, h : h + 1] - run_t[c, h : h + 1]) + hidden
                decay = jnp.exp(gap)
                pair[c * heads + h] = decay
                mixing.append((decay * cross).astype(BF16))
            weighted = both(step, here, p) * val[here, lanes]
            out[here, lanes] = mm(jnp.concatenate(mixing, axis=1), halves(weighted))

    @pl.loop(0, chunks // 2)
    def _(c):
        within(c)

    for copy in factor_copies():
        copy.wait_recv()
    for k in range(len(steps)):
        join(k)

    @pl.loop(chunks // 2, chunks)
    def _(c):
        within(c)

    finish()
    for h in range(heads):
        rows = pl.ds(h * HEAD, HEAD)
        incoming = total[rows]
        for c in range(chunks):
            starts[c, rows], starts_low[c, rows] = split(
                states[c, rows] + before[c, h : h + 1] * incoming
            )

    rows_out[...] = jnp.zeros_like(rows_out)

    @pl.loop(0, chunks)
    def _(c):
        here = pl.ds(pl.multiple_of(c * Q, Q), Q)
        squares, dots = jnp.zeros((Q, LANES), F32), jnp.zeros((Q, LANES), F32)
        for p in range(pairs):
            lanes = pl.ds(p * LANES, LANES)
            reached = from_state(rea[here], rea_low[here], c, lanes)
            reached = reached * both(into, here, p)
            inter[here, lanes] = reached
            mixed = out[here, lanes] + reached + skip[:, lanes] * val[here, lanes]
            out[here, lanes] = mixed
            gate = g_in[here, lanes]
            gated = mixed * (gate * sigmoid(gate))
            squares = squares + gated * gated
            dots = dots + d_mix[here, lanes] * gain[:, lanes] * gated
        rows_out[0:1, here] = jnp.sum(squares.T, axis=0, keepdims=True)
        rows_out[1:2, here] = jnp.sum(dots.T, axis=0, keepdims=True)

    row_copies = [
        remote(
            rows_out, rows_in.at[d - 1], row_send.at[d - 1], row_recv.at[d - 1],
            {"head": lax.rem(head + d, peers_head)},
        )
        for d in range(1, peers_head)
    ]
    for copy in row_copies:
        copy.start()
    summed = rows_out[...]
    for d, copy in enumerate(row_copies):
        copy.wait_recv()
        summed = summed + rows_in[d]
    for copy in row_copies:
        copy.wait_send()
    rows_out[0:1] = lax.rsqrt(summed[0:1] / inner + EPS)
    rows_out[1:2] = summed[1:2] / inner

    @pl.loop(0, chunks)
    def _(c):
        here = pl.ds(pl.multiple_of(c * Q, Q), Q)
        scale = jnp.broadcast_to(rows_out[0:1, here], (Q, LANES)).T
        dot = jnp.broadcast_to(rows_out[1:2, here], (Q, LANES)).T
        cubed = scale * scale * scale * dot
        for p in range(pairs):
            lanes = pl.ds(p * LANES, LANES)
            gate, mixed, slope = g_in[here, lanes], out[here, lanes], d_mix[here, lanes]
            s = sigmoid(gate)
            opened = gate * s
            gated = mixed * opened
            normed = gated * scale
            mix_out[here, lanes] = (normed * gain[:, lanes]).astype(BF16)
            d_gated = scale * (slope * gain[:, lanes]) - gated * cubed
            d_mixer = d_gated * opened
            d_gate[here, lanes] = (d_gated * mixed * (s * (1.0 + gate * (1.0 - s)))).astype(BF16)
            out[here, lanes] = d_mixer
            d_u[here, lanes] = both(into, here, p) * d_mixer
            grads_v[5:6, lanes] = grads_v[5:6, lanes] + jnp.sum(slope * normed, axis=0, keepdims=True)
            grads_v[6:7, lanes] = grads_v[6:7, lanes] + jnp.sum(
                d_mixer * val[here, lanes], axis=0, keepdims=True
            )
        carried = d_u[here].astype(BF16)
        states[c] = mm(
            twice(carried, 0), jnp.concatenate([rea[here], rea_low[here]], axis=0), ((0,), (0,))
        )
        d_read = jnp.zeros((Q, LANES), F32)
        for p in range(pairs):
            lanes = pl.ds(p * LANES, LANES)
            d_read = d_read + with_state(*split(d_u[here, lanes]), c, lanes)
        pre_s[pl.ds(pl.multiple_of(c * Q + SUB, SUB), Q), pl.ds(LANES, LANES)] = d_read

    for h in range(heads):
        rows = pl.ds(h * HEAD, HEAD)
        held = jnp.zeros((HEAD, LANES), F32)
        for c in reversed(range(chunks)):
            held = states[c, rows] + passing[c, h : h + 1] * held
        total[rows] = held

    launch, join, finish, close_backward = carry(-1)
    launch(0)
    upper = jnp.where(row < lane, 1.0, 0.0).astype(BF16)

    def within_back(c):
        here = pl.ds(pl.multiple_of(c * Q, Q), Q)
        padded = pl.ds(pl.multiple_of(c * Q + SUB, SUB), Q)
        cross = products(here)
        d_cross = jnp.zeros((Q, LANES), F32)
        from_inter = jnp.zeros((Q, LANES), F32)
        for p in range(pairs):
            lanes = pl.ds(p * LANES, LANES)
            weighted = (both(step, here, p) * val[here, lanes]).astype(BF16)
            d_out = out[here, lanes]
            d_halves = halves(d_out)
            d_pair = mm(d_halves, weighted, ((1,), (1,)))
            mixing, terms = [], []
            for i, h in enumerate((2 * p, 2 * p + 1)):
                decay = pair[c * heads + h]
                shared = d_pair[i * Q : (i + 1) * Q] * decay
                d_cross = d_cross + shared
                terms.append((shared * cross).astype(BF16))
                mixing.append((decay * cross).astype(BF16))
            d_u[here, lanes] = mm(jnp.concatenate(mixing, axis=0), d_halves, ((0,), (0,)))
            ahead = mm(jnp.concatenate(terms, axis=0), upper)
            for i, h in enumerate((2 * p, 2 * p + 1)):
                crossing = jnp.where(row >= lane, ahead[i * Q : (i + 1) * Q], 0.0)
                prefix[c, h : h + 1] = jnp.sum(crossing, axis=0, keepdims=True)
            from_inter = from_inter + mm(
                (d_out * inter[here, lanes]).astype(BF16), spread_sum[lanes]
            )
        kept[0, here] = from_inter
        d_cross = d_cross.astype(BF16)
        pre_s[padded, pl.ds(LANES, LANES)] = pre_s[padded, pl.ds(LANES, LANES)] + mm(
            d_cross, inf[here]
        )
        pre_s[padded, pl.ds(0, LANES)] = mm(d_cross, rea[here], ((0,), (0,)))

    prefix[...] = jnp.zeros_like(prefix)

    @pl.loop(0, chunks // 2)
    def _(c):
        within_back(c)

    for k in range(len(steps)):
        join(k)

    @pl.loop(chunks // 2, chunks)
    def _(c):
        within_back(c)

    finish()
    for h in range(heads):
        rows = pl.ds(h * HEAD, HEAD)
        held = total[rows]
        for c in reversed(range(chunks)):
            start = starts[c, rows].astype(F32) + starts_low[c, rows].astype(F32)
            met = jnp.sum(held * start, axis=0, keepdims=True)
            met = jnp.sum(met, axis=1, keepdims=True) * passing[c, h : h + 1]
            prefix[c, h : h + 1] = prefix[c, h : h + 1] + met
            added = states[c, rows]
            starts[c, rows], starts_low[c, rows] = split(held)
            held = added + passing[c, h : h + 1] * held

    from_here = jnp.where(row <= lane, 1.0, 0.0)
    under = jnp.where(row > lane, 1.0, 0.0)
    rates = -jnp.exp(rate[...])
    grads_h[...] = jnp.zeros_like(grads_h)
    pre_v[pl.ds(0, SUB)] = jnp.zeros((SUB, channels), F32)
    pre_v[pl.ds(tokens + SUB, SUB)] = jnp.zeros((SUB, channels), F32)
    pre_s[pl.ds(0, SUB)] = jnp.zeros((SUB, 2 * LANES), F32)
    pre_s[pl.ds(tokens + SUB, SUB)] = jnp.zeros((SUB, 2 * LANES), F32)

    @pl.loop(0, chunks)
    def _(c):
        here = pl.ds(pl.multiple_of(c * Q, Q), Q)
        padded = pl.ds(pl.multiple_of(c * Q + SUB, SUB), Q)
        from_tail, from_step = jnp.zeros((Q, LANES), F32), jnp.zeros((Q, LANES), F32)
        d_in = jnp.zeros((Q, LANES), F32)
        for p in range(pairs):
            lanes = pl.ds(p * LANES, LANES)
            sizes = both(step, here, p)
            value = val[here, lanes]
            d_tail = from_state(inf[here], inf_low[here], c, lanes)
            d_tail = d_tail * both(tail, here, p)
            d_weighted = d_u[here, lanes] + d_tail
            from_tail = from_tail + mm((sizes * value * d_tail).astype(BF16), spread_sum[lanes])
            from_step = from_step + mm((value * d_weighted).astype(BF16), spread_sum[lanes])
            d_val = sizes * d_weighted + skip[:, lanes] * out[here, lanes]
            pre_v[padded, lanes] = d_val * slope_v[here, lanes]
            d_in = d_in + with_state(scaled[here, lanes], scaled_low[here, lanes], c, lanes)
        inflow, readout = pl.ds(0, LANES), pl.ds(LANES, LANES)
        pre_s[padded, inflow] = (pre_s[padded, inflow] + d_in) * slope_s[here, inflow]
        pre_s[padded, readout] = pre_s[padded, readout] * slope_s[here, readout]
        d_log = mm(from_here, kept[0, here], precision=HIGH) + mm(under, from_tail, precision=HIGH)
        filled = jnp.concatenate([prefix[c], jnp.zeros((Q - 16, LANES), F32)], axis=0)
        d_log = d_log + filled.T
        d_size = (from_step + rates * d_log) * sig[here]
        d_step[here] = d_size.astype(BF16)
        grads_h[0:1] = grads_h[0:1] + jnp.sum(d_size, axis=0, keepdims=True)
        grads_h[1:2] = grads_h[1:2] + jnp.sum(d_log * logs[here], axis=0, keepdims=True)

    def back(source, base, size, lanes, taps):
        summed = taps[3:4, lanes] * source[pl.ds(base, size), lanes]
        for k in range(3):
            term = taps[k : k + 1, lanes] * source[pl.ds(base + 3 - k, size), lanes]
            summed = summed + term * mask_b[k, pl.ds(base, size)]
        return summed

    def back_copies():
        there = {"seq": lax.rem(seq + count - 1, count)}
        return [
            remote(back_v, back_in_v, back_sems.at[0], back_sems.at[1], there),
            remote(back_s, back_in_s, back_sems.at[2], back_sems.at[3], there),
        ]

    for b in range(pairs):
        lanes = pl.ds(b * LANES, LANES)
        back_v[:, lanes] = back(pre_v, 0, SUB, lanes, taps_v)
    for b in range(2):
        lanes = pl.ds(b * LANES, LANES)
        back_s[:, lanes] = back(pre_s, 0, SUB, lanes, taps_s)

    @pl.when(seq > 0)
    def _():
        for copy in back_copies():
            copy.start()

    def filter_grads(pre, source, base, c, lanes, grads):
        rows = pl.ds(c * Q + SUB, Q)
        slope = pre[rows, lanes]
        for k in range(3):
            term = slope * mask_f[k, pl.ds(c * Q, Q)] * source[pl.ds(base - 3 + k, Q), lanes]
            grads[k : k + 1, lanes] = grads[k : k + 1, lanes] + jnp.sum(term, axis=0, keepdims=True)
        term = slope * source[pl.ds(base, Q), lanes]
        grads[3:4, lanes] = grads[3:4, lanes] + jnp.sum(term, axis=0, keepdims=True)
        grads[4:5, lanes] = grads[4:5, lanes] + jnp.sum(slope, axis=0, keepdims=True)

    for c in range(chunks):
        if c == chunks - 1:
            @pl.when(seq < count - 1)
            def _():
                for copy in back_copies():
                    copy.wait_recv()

            @pl.when(seq == count - 1)
            def _():
                back_in_v[...] = jnp.zeros_like(back_in_v)
                back_in_s[...] = jnp.zeros_like(back_in_s)

        def one(pre, source, base, c, lanes, taps, grads, target, received):
            result = back(pre, c * Q + SUB, Q, lanes, taps)
            if c == chunks - 1:
                result = jnp.concatenate(
                    [result[: Q - SUB], result[Q - SUB :] + received[:, lanes]], axis=0
                )
            target[pl.ds(c * Q, Q), lanes] = result.astype(BF16)
            filter_grads(pre, source, base, c, lanes, grads)

        @pl.loop(0, pairs)
        def _(b, c=c):
            lanes = pl.ds(pl.multiple_of(b * LANES, LANES), LANES)
            source, base = (v_in, c * Q) if c else (first_v, SUB)
            one(pre_v, source, base, c, lanes, taps_v, grads_v, d_value, back_in_v)

        for b in range(2):
            lanes = pl.ds(b * LANES, LANES)
            source, base = (s_in, c * Q) if c else (first_s, SUB)
            one(pre_s, source, base, c, lanes, taps_s, grads_s, d_state, back_in_s)

    @pl.when(seq < count - 1)
    def _():
        for copy in edge_copies():
            copy.wait_send()

    @pl.when(seq > 0)
    def _():
        for copy in back_copies():
            copy.wait_send()

    for copy in factor_copies():
        copy.wait_send()
    close_forward()
    close_backward()


def mix(count, peers_head, inner, lengths, v_in, s_in, g_in, t_in, d_mix, *params, collective_id):
    tokens, channels = v_in.shape
    chunks, heads = tokens // Q, channels // HEAD
    slots = 1
    width = count // 4
    while width >= 2:
        slots += 1
        width //= 2
    vmem, dma = pltpu.VMEM, pltpu.SemaphoreType.DMA
    shape = jax.ShapeDtypeStruct
    outs = [
        shape((tokens, channels), BF16), shape((tokens, channels), BF16),
        shape((tokens, channels), BF16), shape((tokens, 2 * LANES), BF16),
        shape((tokens, LANES), BF16),
        shape((8, channels), F32), shape((8, 2 * LANES), F32), shape((8, LANES), F32),
    ]
    wide, narrow = (tokens, channels), (tokens, LANES)
    scratch = [
        vmem((SUB, channels), F32), vmem((SUB, 2 * LANES), F32),
        vmem((Q + SUB, channels), F32), vmem((Q + SUB, 2 * LANES), F32),
        vmem(wide, F32), vmem(narrow, BF16), vmem(narrow, BF16), vmem(narrow, BF16), vmem(narrow, BF16),
        vmem(wide, F32), vmem((tokens, 2 * LANES), F32),
        vmem((tokens + 2 * SUB, LANES), F32),
        vmem((3, tokens, LANES), F32), vmem((3, tokens + SUB, LANES), F32),
        vmem(narrow, F32), vmem(narrow, F32), vmem(narrow, F32), vmem(narrow, F32),
        vmem((chunks, 16, LANES), F32), vmem(narrow, F32), vmem(narrow, F32),
        vmem((chunks, 16, LANES), F32),
        vmem((chunks * heads, Q, LANES), F32), vmem(wide, BF16), vmem(wide, BF16),
        vmem(wide, F32), vmem(wide, F32), vmem(wide, F32),
        vmem((chunks, channels, LANES), F32),
        vmem((chunks, channels, LANES), BF16), vmem((chunks, channels, LANES), BF16),
        vmem((chunks, 16, LANES), F32), vmem((channels, LANES), F32),
        vmem((count, 16, LANES), F32),
        vmem((2, slots, channels, LANES), BF16), vmem((2, slots + 1, channels, LANES), BF16),
        vmem((1, tokens, LANES), F32), vmem((chunks, 16, LANES), F32),
        vmem((channels, LANES), BF16),
        vmem((8, tokens), F32), vmem((peers_head - 1, 8, tokens), F32),
        vmem((tokens + 2 * SUB, channels), F32), vmem((tokens + 2 * SUB, 2 * LANES), F32),
        vmem((SUB, channels), F32), vmem((SUB, 2 * LANES), F32),
        vmem((SUB, channels), F32), vmem((SUB, 2 * LANES), F32),
        dma((4,)), dma((count - 1,)), dma((count - 1,)),
        dma((2, slots + 1)), dma((2, slots + 1)),
        dma((peers_head - 1,)), dma((peers_head - 1,)), dma((4,)),
    ]
    inside = pl.BlockSpec(memory_space=pltpu.VMEM)
    return pl.pallas_call(
        functools.partial(mixer_kernel, count, peers_head, inner),
        out_shape=outs,
        in_specs=[pl.BlockSpec(memory_space=pltpu.SMEM)] + [inside] * (5 + len(params)),
        out_specs=[inside] * len(outs),
        scratch_shapes=scratch,
        compiler_params=pltpu.CompilerParams(
            collective_id=collective_id, has_side_effects=True, vmem_limit_bytes=60 * 1024 * 1024
        ),
    )(lengths, v_in, s_in, g_in, t_in, d_mix, *params)


def sum_rows(jobs, lines, peers_head, count_in, *refs):
    ins, rest = list(refs[:count_in]), refs[count_in:]
    blocks, tail, normed, mixed, dots = rest[:5]
    outs, rest = rest[5 : 5 + count_in + 1], rest[6 + count_in :]
    every, normed_sum, mixed_sum, dots_sum = rest[:4]
    scratch = rest[4:]
    count = len(jobs)
    own, y_in, z_in, final = (scratch[k * count : (k + 1) * count] for k in range(4))
    (own_sem, ys, yr, zs, zr, gzs, gzr, gys, gyr, keep_sem) = scratch[4 * count : 4 * count + 10]
    (packed, block_own, block_in, normed_own, normed_in, mixed_own, mixed_in, dots_in,
     local_sem, hs, hr) = scratch[4 * count + 10 :]
    ins = [packed] + ins
    seq, head = lax.axis_index("seq"), lax.axis_index("head")
    z, y = seq // lines, seq % lines
    barrier = pltpu.get_barrier_semaphore()

    def at(zz, yy):
        return {"seq": zz * lines + yy}

    def remote(src, dst, send, recv, peer):
        return pltpu.make_async_remote_copy(
            src_ref=src, dst_ref=dst, send_sem=send, recv_sem=recv, device_id=peer, device_id_type=MESH
        )

    peers = [at(z, lax.rem(y + d, lines)) for d in range(1, lines)]
    peers += [at(lax.rem(z + d, LINE), y) for d in range(1, LINE)]
    peers += [{"head": lax.rem(head + d, peers_head)} for d in range(1, peers_head)]
    for peer in peers:
        pl.semaphore_signal(barrier, inc=1, device_id=peer, device_id_type=MESH)
    pl.semaphore_wait(barrier, len(peers))

    width = normed_sum.shape[0]
    block = blocks.shape[1]

    def head_copies(kind):
        copies = []
        for d in range(1, peers_head):
            to = lax.rem(head + d, peers_head)
            rows = pl.ds(to * width, width)
            src, dst = (
                (blocks.at[to], block_in.at[d - 1]),
                (dots, dots_in.at[d - 1]),
                (normed.at[rows], normed_in.at[d - 1]),
                (mixed.at[rows], mixed_in.at[d - 1]),
                (outs[0].at[pl.ds(0, width)], every.at[head]),
            )[kind]
            copies.append(remote(src, dst, hs.at[kind, d - 1], hr.at[kind, d - 1], {"head": to}))
        return copies

    rows = pl.ds(head * width, width)
    local_copies = [
        pltpu.make_async_copy(blocks.at[head], block_own, local_sem.at[0]),
        pltpu.make_async_copy(tail, packed.at[pl.ds(block, tail.shape[0])], local_sem.at[1]),
        pltpu.make_async_copy(normed.at[rows], normed_own, local_sem.at[2]),
        pltpu.make_async_copy(mixed.at[rows], mixed_own, local_sem.at[3]),
    ]

    sizes = []
    for which, start, rows in jobs:
        sizes.append((which, start, rows, rows // lines, rows // lines // LINE))

    def y_copies(j):
        which, start, rows, part, piece = sizes[j]
        copies = []
        for d in range(1, lines):
            to = lax.rem(y + d, lines)
            copies.append(
                remote(
                    ins[which].at[pl.ds(start + to * part, part)],
                    y_in[j].at[d - 1],
                    ys.at[j, d - 1],
                    yr.at[j, d - 1],
                    at(z, to),
                )
            )
        return copies

    def own_copy(j):
        which, start, rows, part, piece = sizes[j]
        return pltpu.make_async_copy(
            ins[which].at[pl.ds(start + y * part, part)], own[j], own_sem.at[j]
        )

    def z_copies(j):
        piece = sizes[j][4]
        copies = []
        for d in (1, LINE - 1, 2):
            to = lax.rem(z + d, LINE)
            copies.append(
                remote(
                    own[j].at[pl.ds(to * piece, piece)],
                    z_in[j].at[d - 1],
                    zs.at[j, d - 1],
                    zr.at[j, d - 1],
                    at(to, y),
                )
            )
        return copies

    def place(j, zz, yy):
        which, start, rows, part, piece = sizes[j]
        return outs[which].at[pl.ds(start + yy * part + zz * piece, piece)]

    def gather_z(j):
        return [
            remote(final[j], place(j, z, y), gzs.at[j, d - 1], gzr.at[j, d - 1], at(lax.rem(z + d, LINE), y))
            for d in (1, LINE - 1, 2)
        ]

    def gather_y(j, d):
        source = lax.rem(z + LINE - d, LINE)
        src = final[j] if d == 0 else place(j, source, y)
        return [
            remote(
                src,
                place(j, source, y),
                gys.at[j, d, e - 1],
                gyr.at[j, d, e - 1],
                at(z, lax.rem(y + e, lines)),
            )
            for e in range(1, lines)
        ]

    def keep(j):
        return pltpu.make_async_copy(final[j], place(j, z, y), keep_sem.at[j])

    for copy in local_copies + head_copies(0):
        copy.start()
    for j in range(count):
        if jobs[j][0]:
            own_copy(j).start()
            for copy in y_copies(j):
                copy.start()
    for kind in (1, 2, 3):
        for copy in head_copies(kind):
            copy.start()

    def pack():
        local_copies[0].wait()
        local_copies[1].wait()
        for copy in head_copies(0):
            copy.wait_recv()

        def step(i, carry):
            rows = pl.ds(pl.multiple_of(i * 16, 16), 16)
            total = block_own[rows].astype(jnp.float32)
            for d in range(peers_head - 1):
                total = total + block_in[d, rows].astype(jnp.float32)
            packed[rows] = total.astype(jnp.bfloat16)
            return carry

        lax.fori_loop(0, block // 16, step, 0)

    def sum_heads(kind, mine, received, target, k):
        local_copies[k].wait()
        for copy in head_copies(kind):
            copy.wait_recv()

        def step(i, carry):
            rows = pl.ds(pl.multiple_of(i * 16, 16), 16)
            total = mine[rows].astype(jnp.float32)
            for d in range(peers_head - 1):
                total = total + received[d, rows].astype(jnp.float32)
            target[rows] = total
            return carry

        lax.fori_loop(0, width // 16, step, 0)

    def reduce_y(j):
        if not jobs[j][0]:
            pack()
            own_copy(j).start()
            for copy in y_copies(j):
                copy.start()
        own_copy(j).wait()
        for copy in y_copies(j):
            copy.wait_recv()
        part = sizes[j][3]
        tile = 16 if part % 16 == 0 else 8

        def step(i, carry):
            rows = pl.ds(pl.multiple_of(i * tile, tile), tile)
            total = own[j][rows].astype(jnp.float32)
            for d in range(lines - 1):
                total = total + y_in[j][d, rows].astype(jnp.float32)
            own[j][rows] = total.astype(jnp.bfloat16)
            return carry

        lax.fori_loop(0, part // tile, step, 0)
        for copy in z_copies(j):
            copy.start()

    def reduce_z(j):
        for copy in z_copies(j):
            copy.wait_recv()
        piece = sizes[j][4]
        tile = 16 if piece % 16 == 0 else 8
        base = z * piece

        def step(i, carry):
            rows = pl.ds(pl.multiple_of(i * tile, tile), tile)
            mine = pl.ds(pl.multiple_of(base + i * tile, tile), tile)
            total = own[j][mine].astype(jnp.float32)
            for d in range(LINE - 1):
                total = total + z_in[j][d, rows].astype(jnp.float32)
            final[j][rows] = total.astype(jnp.bfloat16)
            return carry

        lax.fori_loop(0, piece // tile, step, 0)
        keep(j).start()
        for copy in gather_z(j):
            copy.start()
        for copy in gather_y(j, 0):
            copy.start()

    def forward(j):
        copies = dict(zip((1, LINE - 1, 2), gather_z(j)))
        for d in (1, LINE - 1, 2):
            copies[d].wait_recv()
            for copy in gather_y(j, d):
                copy.start()

    for i in range(count + 2):
        if i < count:
            reduce_y(i)
        if 0 <= i - 1 < count:
            reduce_z(i - 1)
        if 0 <= i - 2 < count:
            forward(i - 2)
    total = dots[...]
    for d, copy in enumerate(head_copies(1)):
        copy.wait_recv()
        total = total + dots_in[d]
    dots_sum[...] = total
    sum_heads(2, normed_own, normed_in, normed_sum, 2)
    sum_heads(3, mixed_own, mixed_in, mixed_sum, 3)
    for j in sorted(range(count), key=lambda j: jobs[j][0]):
        keep(j).wait()
        for copy in y_copies(j) + z_copies(j) + gather_z(j):
            copy.wait_send()
        for d in range(LINE):
            for copy in gather_y(j, d):
                copy.wait_recv()
                copy.wait_send()
        if not jobs[j][0]:
            mine = pltpu.make_async_copy(outs[0].at[pl.ds(0, width)], every.at[head], local_sem.at[4])
            mine.start()
            for copy in head_copies(4):
                copy.start()
            mine.wait()
    for copy in head_copies(4):
        copy.wait_recv()
    for kind in range(5):
        for copy in head_copies(kind):
            copy.wait_send()


def sum_over_seq(arrays, split, blocks, tail, normed, mixed, dots, lines, peers_head, collective_id):
    bf16, f32 = jnp.bfloat16, jnp.float32
    width, tokens = normed.shape[0] // peers_head, normed.shape[1]
    packed = jax.ShapeDtypeStruct((blocks.shape[1] + tail.shape[0], tail.shape[1]), bf16)
    jobs = []
    for which, (array, parts) in enumerate(zip([packed] + arrays, (1,) + split)):
        rows = array.shape[0] // parts
        jobs += [(which, k * rows, rows) for k in range(parts)]
    jobs = jobs[1:3] + jobs[:1] + jobs[3:]
    count = len(jobs)
    widths = [([packed] + arrays)[job[0]].shape[1] for job in jobs]
    scratch = [pltpu.VMEM((job[2] // lines, w), bf16) for job, w in zip(jobs, widths)]
    scratch += [pltpu.VMEM((lines - 1, job[2] // lines, w), bf16) for job, w in zip(jobs, widths)]
    scratch += [
        pltpu.VMEM((LINE - 1, job[2] // lines // LINE, w), bf16) for job, w in zip(jobs, widths)
    ]
    scratch += [pltpu.VMEM((job[2] // lines // LINE, w), bf16) for job, w in zip(jobs, widths)]
    dma = pltpu.SemaphoreType.DMA
    scratch += [
        dma((count,)),
        dma((count, lines - 1)),
        dma((count, lines - 1)),
        dma((count, LINE - 1)),
        dma((count, LINE - 1)),
        dma((count, LINE - 1)),
        dma((count, LINE - 1)),
        dma((count, LINE, lines - 1)),
        dma((count, LINE, lines - 1)),
        dma((count,)),
        pltpu.VMEM(packed.shape, bf16),
        pltpu.VMEM(blocks.shape[1:], bf16),
        pltpu.VMEM((peers_head - 1,) + blocks.shape[1:], bf16),
        pltpu.VMEM((width, tokens), bf16),
        pltpu.VMEM((peers_head - 1, width, tokens), bf16),
        pltpu.VMEM((width, tokens), bf16),
        pltpu.VMEM((peers_head - 1, width, tokens), bf16),
        pltpu.VMEM((peers_head - 1,) + dots.shape, f32),
        dma((5,)),
        dma((5, peers_head - 1)),
        dma((5, peers_head - 1)),
    ]
    anywhere, inside = pl.BlockSpec(memory_space=pl.ANY), pl.BlockSpec(memory_space=pltpu.VMEM)
    shape = jax.ShapeDtypeStruct
    return pl.pallas_call(
        functools.partial(sum_rows, jobs, lines, peers_head, len(arrays)),
        out_shape=[packed]
        + [shape(array.shape, bf16) for array in arrays]
        + [shape((peers_head, width, tail.shape[1]), bf16)]
        + [shape((width, tokens), f32)] * 2
        + [shape(dots.shape, f32)],
        in_specs=[anywhere] * (len(arrays) + 4) + [inside],
        out_specs=[anywhere] * (len(arrays) + 2) + [inside] * 3,
        scratch_shapes=scratch,
        compiler_params=pltpu.CompilerParams(
            collective_id=collective_id, has_side_effects=True, vmem_limit_bytes=60 * 1024 * 1024
        ),
    )(*arrays, blocks, tail, normed, mixed, dots)


def contract_rows(left, right):
    return lax.dot_general(
        left, right, (((0,), (0,)), ((), ())), preferred_element_type=jnp.float32
    )


def contract_cols(left, right):
    return lax.dot_general(
        left, right, (((1,), (1,)), ((), ())), preferred_element_type=jnp.float32
    )


def local(
    hidden_in,
    norm_gain,
    gate_weight,
    value_weight,
    step_weight,
    state_weight,
    value_filter,
    value_offset,
    state_filter,
    state_offset,
    step_bias,
    decay_log,
    skip_gain,
    mix_gain,
    out_weight,
    lengths,
    cotangent,
):
    tokens, width = hidden_in.shape
    heads, channels = step_weight.shape[1], value_weight.shape[1]
    count, peers_head = lax.axis_size("seq"), lax.axis_size("head")
    features = width * peers_head
    gain_block = jnp.broadcast_to(norm_gain.astype(F32)[None, :], (8, width))
    hidden_full, cot_full, gain_full = gather_heads([hidden_in, cotangent, gain_block], peers_head, 1)
    gain_full = gain_full[:1]
    rows_full = hidden_full.astype(F32)
    scale_in = lax.rsqrt(jnp.mean(rows_full * rows_full, axis=1, keepdims=True) + EPS)
    normed = (rows_full * scale_in * gain_full).astype(BF16)

    def project(weight):
        return jnp.dot(normed, weight, preferred_element_type=F32)

    def lanes(vector):
        return jnp.pad(vector, (0, LANES - heads))[None, :]

    step_wide = jnp.pad(step_weight, ((0, 0), (0, LANES - heads)))
    d_mix = contract_cols(cot_full, out_weight)
    mix_out, d_gate, d_value, d_state, d_step, grads_v, grads_s, grads_h = mix(
        count,
        peers_head,
        channels * peers_head,
        lengths,
        project(value_weight),
        project(state_weight),
        project(gate_weight),
        project(step_wide),
        d_mix,
        value_filter,
        state_filter,
        value_offset[None, :],
        state_offset[None, :],
        lanes(step_bias),
        lanes(decay_log),
        jnp.repeat(skip_gain, HEAD)[None, :],
        mix_gain[None, :],
        collective_id=2,
    )
    half = features // 2
    out_part = jnp.concatenate(
        [contract_rows(mix_out, cot_full[:, :half]), contract_rows(mix_out, cot_full[:, half:])]
    ).astype(BF16)
    gate_part = contract_rows(normed, d_gate).astype(BF16)
    value_part = contract_rows(normed, d_value).astype(BF16)
    state_part = contract_rows(normed, d_state)
    step_part = contract_rows(normed, d_step)[:, :heads]
    normed_part = (
        contract_cols(gate_weight, d_gate)
        + contract_cols(value_weight, d_value)
        + contract_cols(state_weight, d_state)
        + contract_cols(step_wide, d_step)
    )
    mixed_part = lax.dot_general(
        out_weight, mix_out, (((0,), (1,)), ((), ())), preferred_element_type=F32
    )
    rows_t = rows_full.T
    weighted = normed_part * rows_t
    dots = jnp.sum(weighted * gain_full.T, axis=0)
    gain_part = jnp.sum(weighted * scale_in.T, axis=1)
    dots = jnp.broadcast_to(dots[None, :], (8, tokens))
    state_size = d_state.shape[1]
    shared = jnp.concatenate([grads_s[:5], gain_part.reshape(-1, state_size)])
    shared = jnp.pad(shared, ((0, 16 - shared.shape[0]), (0, 0)))
    blocks = jnp.concatenate(
        [
            state_part.reshape(peers_head, width, state_size),
            jnp.broadcast_to(shared[None], (peers_head, 16, state_size)),
        ],
        axis=1,
    ).astype(BF16)
    own = (
        step_part,
        grads_v[:4],
        grads_v[4],
        grads_h[0, :heads],
        grads_h[1, :heads],
        jnp.sum(grads_v[6].reshape(heads, HEAD), axis=1),
        grads_v[5],
    )
    packed = jnp.concatenate([jnp.reshape(part, (-1,)) for part in own])
    tail_rows = width // 3 - 16
    packed = jnp.pad(packed, (0, tail_rows * state_size - packed.size))
    packed = packed.reshape(tail_rows, state_size).astype(BF16)
    extra, out_sum, gate_sum, value_sum, state_sum, normed_sum, mixed_sum, dot_sum = sum_over_seq(
        [out_part, gate_part, value_part],
        (3, 3, 3),
        blocks,
        packed,
        normed_part.astype(BF16),
        mixed_part.astype(BF16),
        dots,
        count // LINE,
        peers_head,
        3,
    )
    own_rows = hidden_in.astype(F32)
    block_out = (own_rows + mixed_sum.T).astype(BF16)
    delta_hidden = (
        cotangent.astype(F32)
        + scale_in * (normed_sum.T * norm_gain.astype(F32)[None, :])
        - own_rows * scale_in**3 * (dot_sum[0] / features)[:, None]
    )
    extra = extra[width:].astype(F32)
    norm_sum = lax.dynamic_slice_in_dim(
        extra[5 : 5 + features // state_size].reshape(-1), lax.axis_index("head") * width, width, 0
    )
    packed = extra[16:].reshape(-1)
    pieces, start = [], 0
    for part in own:
        pieces.append(jnp.reshape(packed[start : start + part.size], part.shape))
        start += part.size
    step_sum, filter_sum, offset_sum, bias_sum, decay_sum, skip_sum, gain_sum = pieces
    return (
        block_out,
        delta_hidden,
        norm_sum,
        gate_sum.astype(F32),
        value_sum.astype(F32),
        step_sum,
        state_sum.reshape(features, state_size).astype(F32),
        filter_sum,
        offset_sum,
        extra[:4],
        extra[4],
        bias_sum,
        decay_sum,
        skip_sum,
        gain_sum,
        jnp.concatenate(jnp.split(out_sum, 2, axis=0), axis=1).astype(F32),
    )


def solution(mesh):
    in_specs = (
        P("seq", "head"),
        P("head"),
        P(None, "head"),
        P(None, "head"),
        P(None, "head"),
        P(),
        P(None, "head"),
        P("head"),
        P(),
        P(),
        P("head"),
        P("head"),
        P("head"),
        P("head"),
        P("head", None),
        P(),
        P("seq", "head"),
    )
    out_specs = (
        P("seq", "head"),
        P("seq", "head"),
        P("head"),
        P(None, "head"),
        P(None, "head"),
        P(None, "head"),
        P(),
        P(None, "head"),
        P("head"),
        P(),
        P(),
        P("head"),
        P("head"),
        P("head"),
        P("head"),
        P("head", None),
    )
    return jax.shard_map(local, mesh=mesh, in_specs=in_specs, out_specs=out_specs, check_vma=False)
```

```python
import functools

import jax
import jax.numpy as jnp
from jax import lax
from jax.experimental import pallas as pl
from jax.experimental.pallas import tpu as pltpu
from jax.sharding import PartitionSpec as P

MESH = pl.DeviceIdType.MESH
F32, BF16 = jnp.float32, jnp.bfloat16
HIGH = lax.Precision.HIGHEST
EPS = 1e-05
Q = 128
LANES = 128
HEAD = 64
SUB = 8
FAR = -1e30
LINE = 4


def gather_kernel(peers_head, flat, count_in, *refs):
    ins, outs = refs[:count_in], refs[count_in : 2 * count_in]
    local_sem, send, recv = refs[2 * count_in :]
    head = lax.axis_index("head")
    chips = peers_head // 2
    x, core = head // 2, lax.rem(head, 2)
    partner = {"head": x * 2 + (1 - core)}
    across = [{"head": lax.rem(x + d, chips) * 2 + core} for d in range(1, chips)]
    barrier = pltpu.get_barrier_semaphore()
    for peer in [partner] + across:
        pl.semaphore_signal(barrier, inc=1, device_id=peer, device_id_type=MESH)
    pl.semaphore_wait(barrier, chips)

    def place(k, who):
        if flat[k]:
            width = ins[k].shape[1]
            return outs[k].at[:, pl.ds(pl.multiple_of(who * width, width), width)]
        return outs[k].at[who]

    def remote(src, dst, k, slot, peer):
        return pltpu.make_async_remote_copy(
            src_ref=src, dst_ref=dst, send_sem=send.at[k, slot], recv_sem=recv.at[k, slot],
            device_id=peer, device_id_type=MESH,
        )

    def first(k):
        copies = [remote(ins[k], place(k, head), k, d, across[d - 1]) for d in range(1, chips)]
        return copies + [remote(ins[k], place(k, head), k, 0, partner)]

    def second(k, d):
        source = lax.rem(x + chips - d, chips) * 2 + core
        return remote(place(k, source), place(k, source), k, chips - 1 + d, partner)

    own = [pltpu.make_async_copy(ins[k], place(k, head), local_sem.at[k]) for k in range(count_in)]
    for k in range(count_in):
        for copy in first(k):
            copy.start()
        own[k].start()
    for k in range(count_in):
        for d in range(1, chips):
            first(k)[d - 1].wait_recv()
            second(k, d).start()
    for k in range(count_in):
        own[k].wait()
        for copy in first(k):
            copy.wait_send()
        first(k)[-1].wait_recv()
        for d in range(1, chips):
            second(k, d).wait()


def gather_heads(arrays, peers_head, collective_id):
    flat = [array.ndim == 2 and array.shape[1] % 128 == 0 for array in arrays]
    shapes = [
        (a.shape[0], a.shape[1] * peers_head) if f else (peers_head,) + a.shape
        for a, f in zip(arrays, flat)
    ]
    count, chips = len(arrays), peers_head // 2
    dma = pltpu.SemaphoreType.DMA
    anywhere = pl.BlockSpec(memory_space=pl.ANY)
    gathered = pl.pallas_call(
        functools.partial(gather_kernel, peers_head, flat, count),
        out_shape=[jax.ShapeDtypeStruct(s, a.dtype) for s, a in zip(shapes, arrays)],
        in_specs=[anywhere] * count,
        out_specs=[anywhere] * count,
        scratch_shapes=[dma((count,)), dma((count, 2 * chips - 1)), dma((count, 2 * chips - 1))],
        compiler_params=pltpu.CompilerParams(collective_id=collective_id, has_side_effects=True),
    )(*arrays)
    return [
        g if f else jnp.moveaxis(g, 0, 1).reshape(a.shape[0], -1)
        for g, a, f in zip(gathered, arrays, flat)
    ]


def mm(left, right, contract=((1,), (0,)), precision=None):
    return lax.dot_general(
        left, right, (contract, ((), ())), precision=precision, preferred_element_type=F32
    )


def split(value):
    high = value.astype(BF16)
    return high, (value - high.astype(F32)).astype(BF16)


def twice(value, axis):
    return jnp.concatenate([value, value], axis=axis)


def sigmoid(v):
    return 1.0 / (1.0 + jnp.exp(-v))


def mixer_kernel(
    count, peers_head, inner,
    lengths, v_in, s_in, g_in, t_in, d_mix, taps_v, taps_s, off_v, off_s, bias, rate, skip, gain,
    mix_out, d_gate, d_value, d_state, d_step, grads_v, grads_s, grads_h,
    edge_v, edge_s, first_v, first_s, val, inf, inf_low, rea, rea_low, slope_v, slope_s, segs, mask_f, mask_b,
    step, sig, logs, run, run_t, tail, into, passing, pair, scaled, scaled_low, out, inter, d_u,
    states, starts, starts_low, before, total, factors, push, got, kept, prefix, spread_sum,
    rows_out, rows_in, pre_v, pre_s, back_v, back_s, back_in_v, back_in_s,
    edge_sems, p_send, p_recv, carry_send, carry_recv, row_send, row_recv, back_sems,
):
    tokens, channels = v_in.shape
    chunks, pairs, heads = tokens // Q, channels // LANES, channels // HEAD
    seq, head = lax.axis_index("seq"), lax.axis_index("head")
    window = count // 2
    steps = []
    width = window // 2
    while width >= 2:
        steps.append(width)
        width //= 2

    def remote(src, dst, send, recv, device):
        return pltpu.make_async_remote_copy(
            src_ref=src, dst_ref=dst, send_sem=send, recv_sem=recv, device_id=device, device_id_type=MESH
        )

    barrier = pltpu.get_barrier_semaphore()
    others = [{"seq": lax.rem(seq + d, count)} for d in range(1, count)]
    others += [{"head": lax.rem(head + d, peers_head)} for d in range(1, peers_head)]
    for other in others:
        pl.semaphore_signal(barrier, inc=1, device_id=other, device_id_type=MESH)
    pl.semaphore_wait(barrier, len(others))

    def edge_copies():
        there = {"seq": lax.rem(seq + 1, count)}
        return [
            remote(v_in.at[pl.ds(tokens - SUB, SUB)], edge_v, edge_sems.at[0], edge_sems.at[1], there),
            remote(s_in.at[pl.ds(tokens - SUB, SUB)], edge_s, edge_sems.at[2], edge_sems.at[3], there),
        ]

    @pl.when(seq < count - 1)
    def _():
        for copy in edge_copies():
            copy.start()

    lane = lax.broadcasted_iota(jnp.int32, (Q, LANES), 1)
    row = lax.broadcasted_iota(jnp.int32, (Q, LANES), 0)
    left = lane < HEAD

    anchor = seq * tokens
    bounds, bound = [], 0
    for k in range(lengths.shape[0]):
        bound = bound + lengths[k]
        bounds.append(bound)

    def sequence(places):
        number = jnp.zeros(places.shape, F32)
        for bound in bounds:
            number = number + jnp.where(places >= bound, 1.0, 0.0)
        return number

    places = lax.broadcasted_iota(jnp.int32, (tokens + 2 * SUB, LANES), 0) + (anchor - SUB)
    segs[...] = sequence(places)
    for k in range(3):
        same = segs[pl.ds(SUB, tokens)] == segs[pl.ds(SUB - 3 + k, tokens)]
        mask_f[k] = jnp.where(same, 1.0, 0.0)
        same = segs[pl.ds(0, tokens + SUB)] == segs[pl.ds(3 - k, tokens + SUB)]
        mask_b[k] = jnp.where(same, 1.0, 0.0)
    head_of = lax.broadcasted_iota(jnp.int32, (channels, LANES), 0) // HEAD
    column = lax.broadcasted_iota(jnp.int32, (channels, LANES), 1)
    spread_sum[...] = jnp.where(head_of == column, 1.0, 0.0).astype(BF16)
    grads_v[...] = jnp.zeros_like(grads_v)
    grads_s[...] = jnp.zeros_like(grads_s)

    raw = t_in[...] + bias[...]
    step[...] = jnp.maximum(raw, 0.0) + jnp.log1p(jnp.exp(-jnp.abs(raw)))
    sig[...] = sigmoid(raw)
    logs[...] = -jnp.exp(rate[...]) * step[...]
    lower = jnp.where(row >= lane, 1.0, 0.0)

    @pl.loop(0, chunks)
    def _(c):
        here = pl.ds(pl.multiple_of(c * Q, Q), Q)
        run[here] = mm(lower, logs[here], precision=HIGH)
        summed = run[here]
        run_t[c] = summed.T[:16]
        last = run[pl.ds(c * Q + Q - 1, 1)]
        mine = segs[pl.ds(pl.multiple_of(c * Q + SUB, SUB), Q)]
        at_end = segs[pl.ds(c * Q + SUB + Q - 1, 1)]
        entering = segs[pl.ds(c * Q + SUB - 1, 1)]
        tail[here] = jnp.exp(last - summed) * jnp.where(mine == at_end, 1.0, 0.0)
        into[here] = jnp.exp(summed) * jnp.where(mine == entering, 1.0, 0.0)
        through = jnp.exp(last) * jnp.where(at_end == entering, 1.0, 0.0)
        passing[c] = jnp.broadcast_to(through, (Q, LANES)).T[:16]

    product = jnp.ones((16, LANES), F32)
    for c in range(chunks):
        before[c] = product
        product = product * passing[c]
    factors[seq] = product

    def factor_copies():
        return [
            remote(
                factors.at[seq], factors.at[seq], p_send.at[d - 1], p_recv.at[d - 1],
                {"seq": lax.rem(seq + d, count)},
            )
            for d in range(1, count)
        ]

    for copy in factor_copies():
        copy.start()

    def convolve(source, base, rows, lanes, taps, offset):
        begin, size = rows
        summed = offset[:, lanes] + taps[3:4, lanes] * source[pl.ds(base, size), lanes]
        for k in range(3):
            term = taps[k : k + 1, lanes] * source[pl.ds(base - 3 + k, size), lanes]
            summed = summed + term * mask_f[k, pl.ds(begin, size)]
        s = sigmoid(summed)
        return summed * s, s * (1.0 + summed * (1.0 - s))

    def convolve_rows(c):
        rows = (c * Q, Q)
        span = pl.ds(c * Q, Q)

        @pl.loop(0, pairs)
        def _(b):
            lanes = pl.ds(pl.multiple_of(b * LANES, LANES), LANES)
            source, base = (v_in, c * Q) if c else (first_v, SUB)
            val[span, lanes], slope_v[span, lanes] = convolve(source, base, rows, lanes, taps_v, off_v)

        for b, (target, low) in enumerate(((inf, inf_low), (rea, rea_low))):
            lanes = pl.ds(b * LANES, LANES)
            source, base = (s_in, c * Q) if c else (first_s, SUB)
            active, slope_s[span, lanes] = convolve(source, base, rows, lanes, taps_s, off_s)
            target[span], low[span] = split(active)

    for c in range(1, chunks):
        convolve_rows(c)

    @pl.when(seq > 0)
    def _():
        for copy in edge_copies():
            copy.wait_recv()

    @pl.when(seq == 0)
    def _():
        edge_v[...] = jnp.zeros_like(edge_v)
        edge_s[...] = jnp.zeros_like(edge_s)

    first_v[pl.ds(0, SUB)] = edge_v[...]
    first_s[pl.ds(0, SUB)] = edge_s[...]
    first_v[pl.ds(SUB, Q)] = v_in[pl.ds(0, Q)]
    first_s[pl.ds(SUB, Q)] = s_in[pl.ds(0, Q)]
    convolve_rows(0)

    def both(ref, here, p):
        return jnp.where(left, ref[here, 2 * p : 2 * p + 1], ref[here, 2 * p + 1 : 2 * p + 2])

    def halves(value):
        return jnp.concatenate(
            [jnp.where(left, value, 0.0), jnp.where(left, 0.0, value)], axis=0
        ).astype(BF16)

    @pl.loop(0, chunks)
    def _(c):
        here = pl.ds(pl.multiple_of(c * Q, Q), Q)
        for p in range(pairs):
            lanes = pl.ds(p * LANES, LANES)
            weighted = both(step, here, p) * val[here, lanes]
            scaled[here, lanes], scaled_low[here, lanes] = split(both(tail, here, p) * weighted)
        states[c] = mm(
            twice(scaled[here], 0), jnp.concatenate([inf[here], inf_low[here]], axis=0), ((0,), (0,))
        )

    for h in range(heads):
        rows = pl.ds(h * HEAD, HEAD)
        held = jnp.zeros((HEAD, LANES), F32)
        for c in range(chunks):
            added = states[c, rows]
            states[c, rows] = held
            held = passing[c, h : h + 1] * held + added
        total[rows] = held

    def carry(direction):
        bank = 0 if direction == 1 else 1

        def reach(d):
            there = seq + direction * d
            return jnp.logical_and(there >= 0, there < count)

        def heard(d):
            there = seq - direction * d
            return jnp.logical_and(there >= 0, there < count)

        def copy(slot, d):
            source = min(slot, len(steps))
            return remote(
                push.at[bank, source], got.at[bank, slot],
                carry_send.at[bank, slot], carry_recv.at[bank, slot],
                {"seq": lax.rem(seq + direction * d + count, count)},
            )

        plan = [(k, d) for k, d in enumerate(steps)]
        ends = [(len(steps), 1), (len(steps) + 1, 2)]

        def send(slot, d):
            @pl.when(reach(d))
            def _():
                copy(slot, d).start()

        def factor(first, many, h):
            product = factors[first, h : h + 1]
            for i in range(1, many):
                product = product * factors[first - direction * i, h : h + 1]
            return product

        def launch(slot):
            push[bank, slot] = total[...].astype(BF16)
            if slot < len(steps):
                send(*plan[slot])
            else:
                for end in ends:
                    send(*end)

        def join(slot):
            d = plan[slot][1]

            @pl.when(heard(d))
            def _():
                copy(slot, d).wait_recv()
                for h in range(heads):
                    rows = pl.ds(h * HEAD, HEAD)
                    total[rows] = total[rows] + factor(seq, d, h) * got[bank, slot, rows].astype(F32)

            launch(slot + 1)

        def finish():
            total[...] = jnp.zeros_like(total)

            @pl.when(heard(1))
            def _():
                copy(*ends[0]).wait_recv()
                total[...] = got[bank, ends[0][0]].astype(F32)

            @pl.when(heard(2))
            def _():
                copy(*ends[1]).wait_recv()
                for h in range(heads):
                    rows = pl.ds(h * HEAD, HEAD)
                    far = got[bank, ends[1][0], rows].astype(F32)
                    total[rows] = total[rows] + factor(seq - direction, 1, h) * far

        def close():
            for slot, d in plan + ends:
                @pl.when(reach(d))
                def _(slot=slot, d=d):
                    copy(slot, d).wait_send()

        return launch, join, finish, close

    launch, join, finish, close_forward = carry(1)
    launch(0)

    def products(here):
        read = jnp.concatenate([rea[here], rea[here], rea_low[here]], axis=1)
        return mm(read, jnp.concatenate([inf[here], inf_low[here], inf[here]], axis=1), ((1,), (1,)))

    def from_state(high, low, c, lanes):
        state = jnp.concatenate([starts[c, lanes], starts_low[c, lanes], starts[c, lanes]], axis=1)
        return mm(jnp.concatenate([high, high, low], axis=1), state, ((1,), (1,)))

    def with_state(high, low, c, lanes):
        state = jnp.concatenate([starts[c, lanes], starts_low[c, lanes], starts[c, lanes]], axis=0)
        return mm(jnp.concatenate([high, high, low], axis=1), state)

    def within(c):
        here = pl.ds(pl.multiple_of(c * Q, Q), Q)
        mine = segs[pl.ds(pl.multiple_of(c * Q + SUB, SUB), Q)]
        across = sequence(lane + (anchor + c * Q))
        hidden = jnp.where(jnp.logical_and(mine == across, row >= lane), 0.0, FAR)
        cross = products(here)
        for p in range(pairs):
            lanes = pl.ds(p * LANES, LANES)
            mixing = []
            for h in (2 * p, 2 * p + 1):
                gap = (run[here, h : h + 1] - run_t[c, h : h + 1]) + hidden
                decay = jnp.exp(gap)
                pair[c * heads + h] = decay
                mixing.append((decay * cross).astype(BF16))
            weighted = both(step, here, p) * val[here, lanes]
            out[here, lanes] = mm(jnp.concatenate(mixing, axis=1), halves(weighted))

    @pl.loop(0, chunks // 2)
    def _(c):
        within(c)

    for copy in factor_copies():
        copy.wait_recv()
    for k in range(len(steps)):
        join(k)

    @pl.loop(chunks // 2, chunks)
    def _(c):
        within(c)

    finish()
    for h in range(heads):
        rows = pl.ds(h * HEAD, HEAD)
        incoming = total[rows]
        for c in range(chunks):
            starts[c, rows], starts_low[c, rows] = split(
                states[c, rows] + before[c, h : h + 1] * incoming
            )

    rows_out[...] = jnp.zeros_like(rows_out)

    @pl.loop(0, chunks)
    def _(c):
        here = pl.ds(pl.multiple_of(c * Q, Q), Q)
        squares, dots = jnp.zeros((Q, LANES), F32), jnp.zeros((Q, LANES), F32)
        for p in range(pairs):
            lanes = pl.ds(p * LANES, LANES)
            reached = from_state(rea[here], rea_low[here], c, lanes)
            reached = reached * both(into, here, p)
            inter[here, lanes] = reached
            mixed = out[here, lanes] + reached + skip[:, lanes] * val[here, lanes]
            out[here, lanes] = mixed
            gate = g_in[here, lanes]
            gated = mixed * (gate * sigmoid(gate))
            squares = squares + gated * gated
            dots = dots + d_mix[here, lanes] * gain[:, lanes] * gated
        rows_out[0:1, here] = jnp.sum(squares.T, axis=0, keepdims=True)
        rows_out[1:2, here] = jnp.sum(dots.T, axis=0, keepdims=True)

    row_copies = [
        remote(
            rows_out, rows_in.at[d - 1], row_send.at[d - 1], row_recv.at[d - 1],
            {"head": lax.rem(head + d, peers_head)},
        )
        for d in range(1, peers_head)
    ]
    for copy in row_copies:
        copy.start()
    summed = rows_out[...]
    for d, copy in enumerate(row_copies):
        copy.wait_recv()
        summed = summed + rows_in[d]
    for copy in row_copies:
        copy.wait_send()
    rows_out[0:1] = lax.rsqrt(summed[0:1] / inner + EPS)
    rows_out[1:2] = summed[1:2] / inner

    @pl.loop(0, chunks)
    def _(c):
        here = pl.ds(pl.multiple_of(c * Q, Q), Q)
        scale = jnp.broadcast_to(rows_out[0:1, here], (Q, LANES)).T
        dot = jnp.broadcast_to(rows_out[1:2, here], (Q, LANES)).T
        cubed = scale * scale * scale * dot
        for p in range(pairs):
            lanes = pl.ds(p * LANES, LANES)
            gate, mixed, slope = g_in[here, lanes], out[here, lanes], d_mix[here, lanes]
            s = sigmoid(gate)
            opened = gate * s
            gated = mixed * opened
            normed = gated * scale
            mix_out[here, lanes] = (normed * gain[:, lanes]).astype(BF16)
            d_gated = scale * (slope * gain[:, lanes]) - gated * cubed
            d_mixer = d_gated * opened
            d_gate[here, lanes] = (d_gated * mixed * (s * (1.0 + gate * (1.0 - s)))).astype(BF16)
            out[here, lanes] = d_mixer
            d_u[here, lanes] = both(into, here, p) * d_mixer
            grads_v[5:6, lanes] = grads_v[5:6, lanes] + jnp.sum(slope * normed, axis=0, keepdims=True)
            grads_v[6:7, lanes] = grads_v[6:7, lanes] + jnp.sum(
                d_mixer * val[here, lanes], axis=0, keepdims=True
            )
        carried = d_u[here].astype(BF16)
        states[c] = mm(
            twice(carried, 0), jnp.concatenate([rea[here], rea_low[here]], axis=0), ((0,), (0,))
        )
        d_read = jnp.zeros((Q, LANES), F32)
        for p in range(pairs):
            lanes = pl.ds(p * LANES, LANES)
            d_read = d_read + with_state(*split(d_u[here, lanes]), c, lanes)
        pre_s[pl.ds(pl.multiple_of(c * Q + SUB, SUB), Q), pl.ds(LANES, LANES)] = d_read

    for h in range(heads):
        rows = pl.ds(h * HEAD, HEAD)
        held = jnp.zeros((HEAD, LANES), F32)
        for c in reversed(range(chunks)):
            held = states[c, rows] + passing[c, h : h + 1] * held
        total[rows] = held

    launch, join, finish, close_backward = carry(-1)
    launch(0)
    upper = jnp.where(row < lane, 1.0, 0.0).astype(BF16)

    def within_back(c):
        here = pl.ds(pl.multiple_of(c * Q, Q), Q)
        padded = pl.ds(pl.multiple_of(c * Q + SUB, SUB), Q)
        cross = products(here)
        d_cross = jnp.zeros((Q, LANES), F32)
        from_inter = jnp.zeros((Q, LANES), F32)
        for p in range(pairs):
            lanes = pl.ds(p * LANES, LANES)
            weighted = (both(step, here, p) * val[here, lanes]).astype(BF16)
            d_out = out[here, lanes]
            d_halves = halves(d_out)
            d_pair = mm(d_halves, weighted, ((1,), (1,)))
            mixing, terms = [], []
            for i, h in enumerate((2 * p, 2 * p + 1)):
                decay = pair[c * heads + h]
                shared = d_pair[i * Q : (i + 1) * Q] * decay
                d_cross = d_cross + shared
                terms.append((shared * cross).astype(BF16))
                mixing.append((decay * cross).astype(BF16))
            d_u[here, lanes] = mm(jnp.concatenate(mixing, axis=0), d_halves, ((0,), (0,)))
            ahead = mm(jnp.concatenate(terms, axis=0), upper)
            for i, h in enumerate((2 * p, 2 * p + 1)):
                crossing = jnp.where(row >= lane, ahead[i * Q : (i + 1) * Q], 0.0)
                prefix[c, h : h + 1] = jnp.sum(crossing, axis=0, keepdims=True)
            from_inter = from_inter + mm(
                (d_out * inter[here, lanes]).astype(BF16), spread_sum[lanes]
            )
        kept[0, here] = from_inter
        d_cross = d_cross.astype(BF16)
        pre_s[padded, pl.ds(LANES, LANES)] = pre_s[padded, pl.ds(LANES, LANES)] + mm(
            d_cross, inf[here]
        )
        pre_s[padded, pl.ds(0, LANES)] = mm(d_cross, rea[here], ((0,), (0,)))

    prefix[...] = jnp.zeros_like(prefix)

    @pl.loop(0, chunks // 2)
    def _(c):
        within_back(c)

    for k in range(len(steps)):
        join(k)

    @pl.loop(chunks // 2, chunks)
    def _(c):
        within_back(c)

    finish()
    for h in range(heads):
        rows = pl.ds(h * HEAD, HEAD)
        held = total[rows]
        for c in reversed(range(chunks)):
            start = starts[c, rows].astype(F32) + starts_low[c, rows].astype(F32)
            met = jnp.sum(held * start, axis=0, keepdims=True)
            met = jnp.sum(met, axis=1, keepdims=True) * passing[c, h : h + 1]
            prefix[c, h : h + 1] = prefix[c, h : h + 1] + met
            added = states[c, rows]
            starts[c, rows], starts_low[c, rows] = split(held)
            held = added + passing[c, h : h + 1] * held

    from_here = jnp.where(row <= lane, 1.0, 0.0)
    under = jnp.where(row > lane, 1.0, 0.0)
    rates = -jnp.exp(rate[...])
    grads_h[...] = jnp.zeros_like(grads_h)
    pre_v[pl.ds(0, SUB)] = jnp.zeros((SUB, channels), F32)
    pre_v[pl.ds(tokens + SUB, SUB)] = jnp.zeros((SUB, channels), F32)
    pre_s[pl.ds(0, SUB)] = jnp.zeros((SUB, 2 * LANES), F32)
    pre_s[pl.ds(tokens + SUB, SUB)] = jnp.zeros((SUB, 2 * LANES), F32)

    @pl.loop(0, chunks)
    def _(c):
        here = pl.ds(pl.multiple_of(c * Q, Q), Q)
        padded = pl.ds(pl.multiple_of(c * Q + SUB, SUB), Q)
        from_tail, from_step = jnp.zeros((Q, LANES), F32), jnp.zeros((Q, LANES), F32)
        d_in = jnp.zeros((Q, LANES), F32)
        for p in range(pairs):
            lanes = pl.ds(p * LANES, LANES)
            sizes = both(step, here, p)
            value = val[here, lanes]
            d_tail = from_state(inf[here], inf_low[here], c, lanes)
            d_tail = d_tail * both(tail, here, p)
            d_weighted = d_u[here, lanes] + d_tail
            from_tail = from_tail + mm((sizes * value * d_tail).astype(BF16), spread_sum[lanes])
            from_step = from_step + mm((value * d_weighted).astype(BF16), spread_sum[lanes])
            d_val = sizes * d_weighted + skip[:, lanes] * out[here, lanes]
            pre_v[padded, lanes] = d_val * slope_v[here, lanes]
            d_in = d_in + with_state(scaled[here, lanes], scaled_low[here, lanes], c, lanes)
        inflow, readout = pl.ds(0, LANES), pl.ds(LANES, LANES)
        pre_s[padded, inflow] = (pre_s[padded, inflow] + d_in) * slope_s[here, inflow]
        pre_s[padded, readout] = pre_s[padded, readout] * slope_s[here, readout]
        d_log = mm(from_here, kept[0, here], precision=HIGH) + mm(under, from_tail, precision=HIGH)
        filled = jnp.concatenate([prefix[c], jnp.zeros((Q - 16, LANES), F32)], axis=0)
        d_log = d_log + filled.T
        d_size = (from_step + rates * d_log) * sig[here]
        d_step[here] = d_size.astype(BF16)
        grads_h[0:1] = grads_h[0:1] + jnp.sum(d_size, axis=0, keepdims=True)
        grads_h[1:2] = grads_h[1:2] + jnp.sum(d_log * logs[here], axis=0, keepdims=True)

    def back(source, base, size, lanes, taps):
        summed = taps[3:4, lanes] * source[pl.ds(base, size), lanes]
        for k in range(3):
            term = taps[k : k + 1, lanes] * source[pl.ds(base + 3 - k, size), lanes]
            summed = summed + term * mask_b[k, pl.ds(base, size)]
        return summed

    def back_copies():
        there = {"seq": lax.rem(seq + count - 1, count)}
        return [
            remote(back_v, back_in_v, back_sems.at[0], back_sems.at[1], there),
            remote(back_s, back_in_s, back_sems.at[2], back_sems.at[3], there),
        ]

    for b in range(pairs):
        lanes = pl.ds(b * LANES, LANES)
        back_v[:, lanes] = back(pre_v, 0, SUB, lanes, taps_v)
    for b in range(2):
        lanes = pl.ds(b * LANES, LANES)
        back_s[:, lanes] = back(pre_s, 0, SUB, lanes, taps_s)

    @pl.when(seq > 0)
    def _():
        for copy in back_copies():
            copy.start()

    def filter_grads(pre, source, base, c, lanes, grads):
        rows = pl.ds(c * Q + SUB, Q)
        slope = pre[rows, lanes]
        for k in range(3):
            term = slope * mask_f[k, pl.ds(c * Q, Q)] * source[pl.ds(base - 3 + k, Q), lanes]
            grads[k : k + 1, lanes] = grads[k : k + 1, lanes] + jnp.sum(term, axis=0, keepdims=True)
        term = slope * source[pl.ds(base, Q), lanes]
        grads[3:4, lanes] = grads[3:4, lanes] + jnp.sum(term, axis=0, keepdims=True)
        grads[4:5, lanes] = grads[4:5, lanes] + jnp.sum(slope, axis=0, keepdims=True)

    for c in range(chunks):
        if c == chunks - 1:
            @pl.when(seq < count - 1)
            def _():
                for copy in back_copies():
                    copy.wait_recv()

            @pl.when(seq == count - 1)
            def _():
                back_in_v[...] = jnp.zeros_like(back_in_v)
                back_in_s[...] = jnp.zeros_like(back_in_s)

        def one(pre, source, base, c, lanes, taps, grads, target, received):
            result = back(pre, c * Q + SUB, Q, lanes, taps)
            if c == chunks - 1:
                result = jnp.concatenate(
                    [result[: Q - SUB], result[Q - SUB :] + received[:, lanes]], axis=0
                )
            target[pl.ds(c * Q, Q), lanes] = result.astype(BF16)
            filter_grads(pre, source, base, c, lanes, grads)

        @pl.loop(0, pairs)
        def _(b, c=c):
            lanes = pl.ds(pl.multiple_of(b * LANES, LANES), LANES)
            source, base = (v_in, c * Q) if c else (first_v, SUB)
            one(pre_v, source, base, c, lanes, taps_v, grads_v, d_value, back_in_v)

        for b in range(2):
            lanes = pl.ds(b * LANES, LANES)
            source, base = (s_in, c * Q) if c else (first_s, SUB)
            one(pre_s, source, base, c, lanes, taps_s, grads_s, d_state, back_in_s)

    @pl.when(seq < count - 1)
    def _():
        for copy in edge_copies():
            copy.wait_send()

    @pl.when(seq > 0)
    def _():
        for copy in back_copies():
            copy.wait_send()

    for copy in factor_copies():
        copy.wait_send()
    close_forward()
    close_backward()


def mix(count, peers_head, inner, lengths, v_in, s_in, g_in, t_in, d_mix, *params, collective_id):
    tokens, channels = v_in.shape
    chunks, heads = tokens // Q, channels // HEAD
    slots = 1
    width = count // 4
    while width >= 2:
        slots += 1
        width //= 2
    vmem, dma = pltpu.VMEM, pltpu.SemaphoreType.DMA
    shape = jax.ShapeDtypeStruct
    outs = [
        shape((tokens, channels), BF16), shape((tokens, channels), BF16),
        shape((tokens, channels), BF16), shape((tokens, 2 * LANES), BF16),
        shape((tokens, LANES), BF16),
        shape((8, channels), F32), shape((8, 2 * LANES), F32), shape((8, LANES), F32),
    ]
    wide, narrow = (tokens, channels), (tokens, LANES)
    scratch = [
        vmem((SUB, channels), F32), vmem((SUB, 2 * LANES), F32),
        vmem((Q + SUB, channels), F32), vmem((Q + SUB, 2 * LANES), F32),
        vmem(wide, F32), vmem(narrow, BF16), vmem(narrow, BF16), vmem(narrow, BF16), vmem(narrow, BF16),
        vmem(wide, F32), vmem((tokens, 2 * LANES), F32),
        vmem((tokens + 2 * SUB, LANES), F32),
        vmem((3, tokens, LANES), F32), vmem((3, tokens + SUB, LANES), F32),
        vmem(narrow, F32), vmem(narrow, F32), vmem(narrow, F32), vmem(narrow, F32),
        vmem((chunks, 16, LANES), F32), vmem(narrow, F32), vmem(narrow, F32),
        vmem((chunks, 16, LANES), F32),
        vmem((chunks * heads, Q, LANES), F32), vmem(wide, BF16), vmem(wide, BF16),
        vmem(wide, F32), vmem(wide, F32), vmem(wide, F32),
        vmem((chunks, channels, LANES), F32),
        vmem((chunks, channels, LANES), BF16), vmem((chunks, channels, LANES), BF16),
        vmem((chunks, 16, LANES), F32), vmem((channels, LANES), F32),
        vmem((count, 16, LANES), F32),
        vmem((2, slots, channels, LANES), BF16), vmem((2, slots + 1, channels, LANES), BF16),
        vmem((1, tokens, LANES), F32), vmem((chunks, 16, LANES), F32),
        vmem((channels, LANES), BF16),
        vmem((8, tokens), F32), vmem((peers_head - 1, 8, tokens), F32),
        vmem((tokens + 2 * SUB, channels), F32), vmem((tokens + 2 * SUB, 2 * LANES), F32),
        vmem((SUB, channels), F32), vmem((SUB, 2 * LANES), F32),
        vmem((SUB, channels), F32), vmem((SUB, 2 * LANES), F32),
        dma((4,)), dma((count - 1,)), dma((count - 1,)),
        dma((2, slots + 1)), dma((2, slots + 1)),
        dma((peers_head - 1,)), dma((peers_head - 1,)), dma((4,)),
    ]
    inside = pl.BlockSpec(memory_space=pltpu.VMEM)
    return pl.pallas_call(
        functools.partial(mixer_kernel, count, peers_head, inner),
        out_shape=outs,
        in_specs=[pl.BlockSpec(memory_space=pltpu.SMEM)] + [inside] * (5 + len(params)),
        out_specs=[inside] * len(outs),
        scratch_shapes=scratch,
        compiler_params=pltpu.CompilerParams(
            collective_id=collective_id, has_side_effects=True, vmem_limit_bytes=60 * 1024 * 1024
        ),
    )(lengths, v_in, s_in, g_in, t_in, d_mix, *params)


def add_rows(target, terms, rows, dtype=BF16):
    tile = next(t for t in (32, 16, 8) if rows % t == 0)

    @pl.loop(0, rows // tile)
    def _(i):
        def at(start):
            return pl.ds(pl.multiple_of(start + i * tile, 8), tile)

        total = terms[0][0][at(terms[0][1])].astype(F32)
        for ref, start in terms[1:]:
            total = total + ref[at(start)].astype(F32)
        target[0][at(target[1])] = total.astype(dtype)


class Job:
    def __init__(self, index, y_first, src, dst, start, rows, lines, y_in, right, left, total, final, sems, where):
        self.index, self.y_first, self.src, self.dst, self.start = index, y_first, src, dst, start
        self.lines, self.y_in, self.right, self.left = lines, y_in, right, left
        self.total, self.final = total, final
        self.sems = sems
        self.seq, self.z, self.y = where
        self.part = rows // lines
        self.chunk = rows // lines // LINE if y_first else rows // LINE
        self.piece = rows // lines // LINE
        self.rows = rows
        self.base = start + self.y * self.part if y_first else start

    def remote(self, src, dst, name, slot, device):
        send, recv = self.sems[name]
        return pltpu.make_async_remote_copy(
            src_ref=src, dst_ref=dst, send_sem=send.at[(self.index,) + slot],
            recv_sem=recv.at[(self.index,) + slot], device_id={"seq": device}, device_id_type=MESH,
        )

    def seat(self, z, y):
        return z * self.lines + y

    def peer_y(self, d):
        return lax.rem(self.y + d, self.lines)

    def swap(self, d):
        to = self.peer_y(d)
        if self.y_first:
            src = self.src.at[pl.ds(self.start + to * self.part, self.part)]
        else:
            src = self.total.at[pl.ds(to * self.piece, self.piece)]
        return self.remote(src, self.y_in.at[d - 1], "swap", (d - 1,), self.seat(self.z, to))

    def swaps(self):
        for d in range(1, self.lines):
            self.swap(d).start()

    def join_y(self):
        for d in range(1, self.lines):
            self.swap(d).wait_recv()
        others = [(self.y_in.at[d], 0) for d in range(self.lines - 1)]
        if self.y_first:
            add_rows((self.src, self.base), [(self.src, self.base)] + others, self.part)
        else:
            mine = self.y * self.piece
            add_rows((self.final, mine), [(self.total, mine)] + others, self.piece)

    def pass_on(self, c, z, direction, first):
        box = self.right if direction > 0 else self.left
        src = self.src.at[pl.ds(self.base + c * self.chunk, self.chunk)] if first else box.at[c]
        name = "right" if direction > 0 else "left"
        return self.remote(src, box.at[c], name, (c,), self.seat(z + direction, self.y))

    def come(self, c, direction):
        box = self.right if direction > 0 else self.left
        return self.remote(box.at[c], box.at[c], "right" if direction > 0 else "left", (c,), self.seq)

    def chain_start(self):
        @pl.when(self.z == 0)
        def _():
            for c in (3, 2, 1):
                self.pass_on(c, 0, 1, True).start()

        @pl.when(self.z == 3)
        def _():
            for c in (0, 1, 2):
                self.pass_on(c, 3, -1, True).start()

    def chain_hop(self, h):
        for z, direction, last in ((h, 1, 3), (3 - h, -1, 0)):
            box = self.right if direction > 0 else self.left

            @pl.when(self.z == z)
            def _(z=z, direction=direction, last=last, box=box):
                for c in range(last, z - direction, -direction):
                    self.come(c, direction).wait_recv()
                    if c != z:
                        add_rows((box.at[c], 0), [(box.at[c], 0), (self.src, self.base + c * self.chunk)], self.chunk)
                        self.pass_on(c, z, direction, False).start()

    def chain_end(self, seats):
        for z in seats:
            @pl.when(self.z == z)
            def _(z=z):
                terms = [(self.src, self.base + z * self.chunk)]
                if z > 0:
                    terms.append((self.right.at[z], 0))
                if z < LINE - 1:
                    terms.append((self.left.at[z], 0))
                add_rows((self.final if self.y_first else self.total, 0), terms, self.chunk)
                self.chain_done()

    def chain_done(self):
        if self.y_first:
            self.keep().start()
            self.spread_start()
            for d in range(1, self.lines):
                self.share(0, d).start()
        else:
            self.swaps()

    def place(self, z):
        first = self.y * self.part if self.y_first else 0
        return self.dst.at[pl.ds(self.start + first + z * self.chunk, self.chunk)]

    def keep(self):
        return pltpu.make_async_copy(self.final, self.place(self.z), self.sems["keep"].at[self.index])

    def spread(self, direction, h):
        src = self.final if h == 1 else self.place(self.z - direction * (h - 1))
        slot = h if direction > 0 else LINE - 1 + h
        device = self.seat(self.z + direction, self.y)
        return self.remote(src, self.place(self.z - direction * (h - 1)), "spread", (slot,), device)

    def spread_from(self, direction, h):
        slot = h if direction > 0 else LINE - 1 + h
        there = self.place(self.z - direction * h)
        return self.remote(there, there, "spread", (slot,), self.seq)

    def goes(self, direction):
        return self.z < LINE - 1 if direction > 0 else self.z > 0

    def comes(self, direction, h):
        return self.z >= h if direction > 0 else self.z < LINE - h

    def spread_start(self):
        for direction in (1, -1):
            @pl.when(self.goes(direction))
            def _(direction=direction):
                self.spread(direction, 1).start()

    def spread_hop(self, h):
        for direction in (1, -1):
            @pl.when(self.comes(direction, h))
            def _(direction=direction):
                self.spread_from(direction, h).wait_recv()
                if h < LINE - 1:
                    @pl.when(self.goes(direction))
                    def _():
                        self.spread(direction, h + 1).start()

                if self.y_first:
                    for d in range(1, self.lines):
                        self.share(h if direction > 0 else LINE - 1 + h, d).start()

    def share(self, slot, d):
        to = self.seat(self.z, self.peer_y(d))
        if self.y_first:
            if slot == 0:
                src, there = self.final, self.place(self.z)
            else:
                z = self.z - slot if slot < LINE else self.z + (slot - LINE + 1)
                src = there = self.place(z)
        else:
            src = there = self.final.at[pl.ds(self.y * self.piece, self.piece)]
        return self.remote(src, there, "share", (slot, d - 1), to)

    def share_all(self):
        for d in range(1, self.lines):
            self.share(0, d).start()

    def shared(self):
        for d in range(1, self.lines):
            self.share(0, d).wait_recv()
        self.keep().start()
        self.spread_start()

    def stages(self, make):
        def enter():
            make()
            if self.y_first:
                self.swaps()
            else:
                self.chain_start()

        def joined():
            self.join_y()
            self.chain_start()

        def second():
            self.chain_hop(2)
            self.chain_end((1, 2))

        def third():
            self.chain_hop(3)
            self.chain_end((0, 3))

        def turn():
            self.join_y()
            self.share_all()

        hops = [functools.partial(self.spread_hop, h) for h in range(1, LINE)]
        chain = [functools.partial(self.chain_hop, 1), second, third]
        if self.y_first:
            return [enter, joined] + chain + hops
        return [enter] + chain + [turn, self.shared] + hops

    def close(self):
        self.keep().wait()
        for d in range(1, self.lines):
            self.swap(d).wait_send()
            self.share(0, d).wait_send()
            if self.y_first:
                self.share(0, d).wait_recv()
        for h in range(1, LINE):
            for direction in (1, -1):
                @pl.when(self.z == (h - 1 if direction > 0 else LINE - h))
                def _(h=h, direction=direction):
                    z = h - 1 if direction > 0 else LINE - h
                    last = LINE - 1 if direction > 0 else 0
                    for c in range(last, z, -direction):
                        self.pass_on(c, z, direction, h == 1).wait_send()

                there = self.comes(direction, h - 1) if h > 1 else True

                @pl.when(jnp.logical_and(there, self.goes(direction)))
                def _(h=h, direction=direction):
                    self.spread(direction, h).wait_send()

                if self.y_first:
                    @pl.when(self.comes(direction, h))
                    def _(h=h, direction=direction):
                        for d in range(1, self.lines):
                            copy = self.share(h if direction > 0 else LINE - 1 + h, d)
                            copy.wait_send()
                            copy.wait_recv()


def sum_rows(jobs, order, lines, peers_head, *refs):
    (normed, cot, hidden, scale, gain, mix_out, d_gate, d_value, d_state, d_step, grads_v, grads_s, grads_h,
     gate_w, value_w, out_w, state_w, step_w) = refs[:18]
    outs, (every, normed_sum, mixed_sum, dots_sum) = refs[18:22], refs[22:26]
    scratch = refs[26:]
    count = len(jobs)
    y_in, right, left, total, final = (scratch[k * count : (k + 1) * count] for k in range(5))
    names = ("swap", "right", "left", "spread", "share")
    pairs = scratch[5 * count : 5 * count + 10]
    sems = {name: (pairs[2 * k], pairs[2 * k + 1]) for k, name in enumerate(names)}
    (sems["keep"], packed, out_part, gate_part, value_part, gate_m, value_m, out_m, state_m, step_m,
     blocks, block_in, normed_part, normed_in, mixed_part, mixed_in, dots, dots_in, gain_part, rest, product,
     local_sem, hs, hr) = scratch[5 * count + 10 :]
    parts = [packed, out_part, gate_part, value_part]
    tokens, features = normed.shape
    width, channels = features // peers_head, d_gate.shape[1]
    heads = channels // HEAD
    seq, head = lax.axis_index("seq"), lax.axis_index("head")
    z, y = seq // lines, lax.rem(seq, lines)
    work = [
        Job(j, y_first, parts[which], outs[which], start, rows, lines,
            y_in[j], right[j], left[j], total[j], final[j], sems, (seq, z, y))
        for j, (which, start, rows, y_first) in enumerate(jobs)
    ]
    shared = [j for j in range(count) if not jobs[j][0]][0]

    loads = [
        pltpu.make_async_copy(src, dst, local_sem.at[k])
        for k, (src, dst) in enumerate(
            ((gate_w, gate_m), (value_w, value_m), (out_w, out_m), (state_w, state_m), (step_w, step_m))
        )
    ]
    for copy in loads:
        copy.start()

    barrier = pltpu.get_barrier_semaphore()
    peers = [{"seq": z * lines + lax.rem(y + d, lines)} for d in range(1, lines)]
    peers += [{"head": lax.rem(head + d, peers_head)} for d in range(1, peers_head)]
    for peer in peers:
        pl.semaphore_signal(barrier, inc=1, device_id=peer, device_id_type=MESH)
    for direction in (1, -1):
        @pl.when(z < LINE - 1 if direction > 0 else z > 0)
        def _(direction=direction):
            pl.semaphore_signal(
                barrier, inc=1, device_id={"seq": (z + direction) * lines + y}, device_id_type=MESH
            )

    ends = jnp.logical_or(z == 0, z == LINE - 1)

    @pl.when(ends)
    def _():
        pl.semaphore_wait(barrier, len(peers) + 1)

    @pl.when(jnp.logical_not(ends))
    def _():
        pl.semaphore_wait(barrier, len(peers) + 2)

    block = blocks.shape[1]

    def head_copies(kind):
        for d in range(1, peers_head):
            to = lax.rem(head + d, peers_head)
            if kind < 4:
                src = (blocks.at[to], dots, normed_part.at[to], mixed_part.at[to])[kind]
                dst = (block_in, dots_in, normed_in, mixed_in)[kind].at[d - 1]
            else:
                src, dst = outs[0].at[pl.ds(0, width)], every.at[head]
            yield pltpu.make_async_remote_copy(
                src_ref=src, dst_ref=dst, send_sem=hs.at[kind, d - 1], recv_sem=hr.at[kind, d - 1],
                device_id={"head": to}, device_id_type=MESH,
            )

    def start(copies):
        for copy in copies:
            copy.start()

    def received(copies):
        for copy in copies:
            copy.wait_recv()

    def outer(left_ref, right_ref, target, start, rows):
        tall = 128 if rows % 128 == 0 else rows
        for r in range(start, start + rows, tall):
            turned = left_ref[:, pl.ds(r, tall)].T
            target[pl.ds(r, tall)] = jnp.dot(
                turned, right_ref[...], preferred_element_type=F32
            ).astype(target.dtype)

    def make(j):
        which, begin, rows, y_first = jobs[j]
        if not which:
            return pack
        operands = ((mix_out, cot), (normed, d_gate), (normed, d_value))[which - 1]
        return lambda: outer(*operands, parts[which], begin, rows)

    def over_head(quarter):
        if quarter == 0:
            for copy in loads:
                copy.wait()
            dots[...] = jnp.zeros_like(dots)
            gain_part[...] = jnp.zeros_like(gain_part)

        def by_head(h):
            mine = pl.ds(h * width, width)
            result = jnp.zeros((tokens, width), F32)
            for left_ref, right_ref in (
                (d_gate, gate_m), (d_value, value_m), (d_state, state_m), (d_step, step_m)
            ):
                result = result + lax.dot_general(
                    left_ref[...], right_ref[mine], (((1,), (1,)), ((), ())),
                    preferred_element_type=F32,
                )
            product[...] = result
            mixed_part[h] = jnp.dot(
                mix_out[...], out_m[:, mine], preferred_element_type=F32
            ).astype(BF16)

            @pl.loop(0, tokens // Q)
            def _(c):
                here = pl.ds(pl.multiple_of(c * Q, Q), Q)
                result = product[here]
                normed_part[h, here] = result.astype(BF16)
                rows = result * hidden[here, mine].astype(F32)
                gain_part[:, mine] = gain_part[:, mine] + jnp.sum(
                    rows * scale[here], axis=0, keepdims=True
                )
                dot = jnp.sum(rows * gain[:, mine], axis=1, keepdims=True)
                dot = jnp.broadcast_to(dot, (Q, LANES)).T
                dots[:, here] = dots[:, here] + dot[:8]

        for h in range(quarter * peers_head // 4, (quarter + 1) * peers_head // 4):
            by_head(h)

    def over_head_send():
        states = blocks.shape[2]
        rest[...] = jnp.zeros_like(rest)
        rest[0:8] = grads_s[...]
        for k in range(features // states):
            rest[8 + k : 9 + k] = gain_part[:, pl.ds(k * states, states)]
        for h in range(peers_head):
            turned = normed[:, pl.ds(h * width, width)].T
            blocks[h, pl.ds(0, width)] = jnp.dot(
                turned, d_state[...], preferred_element_type=F32
            ).astype(BF16)
            blocks[h, pl.ds(width, 16)] = rest[0:16].astype(BF16)
        for kind in range(4):
            start(head_copies(kind))
        steps = lax.dot_general(
            d_step[...], normed[...], (((0,), (0,)), ((), ())), preferred_element_type=F32
        )
        for k in range(features // states):
            rest[16 + k * heads : 16 + (k + 1) * heads] = steps[:heads, k * states : (k + 1) * states]
        at = 16 + heads * (features // states)
        for k in range(0, channels, states):
            lanes = min(states, channels - k)
            rest[at : at + 8, 0:lanes] = grads_v[:, pl.ds(k, lanes)]
            at += 8
        rest[at : at + 2, 0:LANES] = grads_h[0:2]
        packed[pl.ds(block, rest.shape[0] - 16)] = rest[16:].astype(BF16)

    def pack():
        received(head_copies(0))
        others = [(block_in.at[d], 0) for d in range(peers_head - 1)]
        add_rows((packed, 0), [(blocks.at[head], 0)] + others, block)

    def sum_heads():
        received(head_copies(1))
        summed = dots[...]
        for d in range(peers_head - 1):
            summed = summed + dots_in[d]
        dots_sum[...] = summed
        for kind, mine, boxes, target in (
            (2, normed_part, normed_in, normed_sum), (3, mixed_part, mixed_in, mixed_sum)
        ):
            received(head_copies(kind))
            others = [(boxes.at[d], 0) for d in range(peers_head - 1)]
            add_rows((target, 0), [(mine.at[head], 0)] + others, tokens, F32)

    plans = [job.stages(make(job.index)) for job in work]
    plans.append([functools.partial(over_head, q) for q in range(4)] + [over_head_send, sum_heads])
    for j, stage in order:
        plans[j][stage]()
    for job in sorted(work, key=lambda job: job.index != shared):
        job.close()
        if job.index == shared:
            mine = pltpu.make_async_copy(outs[0].at[pl.ds(0, width)], every.at[head], local_sem.at[0])
            mine.start()
            start(head_copies(4))
            mine.wait()
    received(head_copies(4))
    for kind in range(5):
        for copy in head_copies(kind):
            copy.wait_send()


def sum_over_seq(plan, order, values, grads, weights, lines, peers_head, collective_id):
    normed, d_gate, d_state = values[0], values[6], values[8]
    tokens, features = normed.shape
    channels, states, width = d_gate.shape[1], d_state.shape[1], normed.shape[1] // peers_head
    heads = channels // HEAD
    shape, dma, vmem = jax.ShapeDtypeStruct, pltpu.SemaphoreType.DMA, pltpu.VMEM
    extra = heads * (features // states) + 8 * -(-channels // states) + 8
    total = -(-(width + 16 + extra) // (8 * lines * LINE)) * 8 * lines * LINE
    whole = [
        shape((total, states), BF16), shape((channels, features), BF16),
        shape((features, channels), BF16), shape((features, channels), BF16),
    ]
    jobs = []
    for which, number, parts, y_first in plan:
        rows = whole[which].shape[0] // parts
        jobs.append((which, number * rows, rows, y_first))
    count = len(jobs)
    groups = [[] for _ in range(5)]
    for which, start, rows, y_first in jobs:
        columns = whole[which].shape[1]
        part, piece = rows // lines, rows // lines // LINE
        chunk = piece if y_first else rows // LINE
        sizes = (
            (lines - 1, part if y_first else piece), (LINE, chunk), (LINE, chunk),
            (8 if y_first else chunk,), (chunk,),
        )
        for group, size in zip(groups, sizes):
            group.append(vmem(size + (columns,), BF16))
    scratch = [one for group in groups for one in group]
    for slots in ((lines - 1,), (LINE,), (LINE,), (2 * LINE - 1,), (2 * LINE - 1, lines - 1)):
        scratch += [dma((count,) + slots)] * 2
    others = peers_head - 1
    scratch += [dma((count,))]
    scratch += [vmem(one.shape, BF16) for one in whole]
    scratch += [vmem(one.shape, BF16) for one in weights]
    scratch += [
        vmem((peers_head, width + 16, states), BF16), vmem((others, width + 16, states), BF16),
        vmem((peers_head, tokens, width), BF16), vmem((others, tokens, width), BF16),
        vmem((peers_head, tokens, width), BF16), vmem((others, tokens, width), BF16),
        vmem((8, tokens), F32), vmem((others, 8, tokens), F32), vmem((1, features), F32),
        vmem((total - width, states), F32), vmem((tokens, width), F32),
        dma((5,)), dma((5, others)), dma((5, others)),
    ]
    anywhere, inside = pl.BlockSpec(memory_space=pl.ANY), pl.BlockSpec(memory_space=pltpu.VMEM)
    operands = list(values) + list(grads)
    return pl.pallas_call(
        functools.partial(sum_rows, jobs, order, lines, peers_head),
        out_shape=whole
        + [shape((peers_head, width, states), BF16)]
        + [shape((tokens, width), F32)] * 2
        + [shape((8, tokens), F32)],
        in_specs=[inside] * len(operands) + [anywhere] * len(weights),
        out_specs=[anywhere] * 5 + [inside] * 3,
        scratch_shapes=scratch,
        compiler_params=pltpu.CompilerParams(
            collective_id=collective_id, has_side_effects=True, vmem_limit_bytes=61 * 1024 * 1024
        ),
    )(*operands, *weights)


PLAN = (
    (1, 0, 3, True), (1, 1, 3, False), (1, 2, 3, True), (2, 0, 3, False),
    (2, 1, 3, True), (2, 2, 3, True), (3, 0, 3, True), (0, 0, 1, False),
    (3, 1, 3, True), (3, 2, 3, True),
)
ORDER = (
    (2, 0), (1, 0), (4, 0), (1, 1), (2, 1), (1, 2), (5, 0), (4, 1), (2, 2), (10, 0),
    (3, 0), (0, 0), (4, 2), (2, 3), (1, 3), (2, 4), (4, 3), (10, 1), (3, 1), (0, 1),
    (1, 4), (2, 5), (3, 2), (4, 4), (1, 5), (10, 2), (6, 0), (5, 1), (2, 6), (9, 0),
    (0, 2), (10, 3), (1, 6), (10, 4), (3, 3), (4, 5), (6, 1), (0, 3), (1, 7), (3, 4),
    (6, 2), (2, 7), (0, 4), (4, 6), (1, 8), (5, 2), (8, 0), (9, 1), (6, 3), (0, 5),
    (5, 3), (3, 5), (4, 7), (9, 2), (0, 6), (7, 0), (5, 4), (3, 6), (9, 3), (6, 4),
    (8, 1), (0, 7), (6, 5), (7, 1), (8, 2), (9, 4), (7, 2), (5, 5), (7, 3), (6, 6),
    (10, 5), (6, 7), (9, 5), (8, 3), (7, 4), (5, 6), (3, 7), (9, 6), (8, 4), (5, 7),
    (8, 5), (9, 7), (7, 5), (8, 6), (3, 8), (7, 6), (8, 7), (7, 7), (7, 8),
)


def contract_rows(left, right):
    return lax.dot_general(
        left, right, (((0,), (0,)), ((), ())), preferred_element_type=jnp.float32
    )


def contract_cols(left, right):
    return lax.dot_general(
        left, right, (((1,), (1,)), ((), ())), preferred_element_type=jnp.float32
    )


def local(
    hidden_in,
    norm_gain,
    gate_weight,
    value_weight,
    step_weight,
    state_weight,
    value_filter,
    value_offset,
    state_filter,
    state_offset,
    step_bias,
    decay_log,
    skip_gain,
    mix_gain,
    out_weight,
    lengths,
    cotangent,
):
    tokens, width = hidden_in.shape
    heads, channels = step_weight.shape[1], value_weight.shape[1]
    count, peers_head = lax.axis_size("seq"), lax.axis_size("head")
    features = width * peers_head
    gain_block = jnp.broadcast_to(norm_gain.astype(F32)[None, :], (8, width))
    hidden_full, cot_full, gain_full = gather_heads([hidden_in, cotangent, gain_block], peers_head, 1)
    gain_full = gain_full[:1]
    rows_full = hidden_full.astype(F32)
    scale_in = lax.rsqrt(jnp.mean(rows_full * rows_full, axis=1, keepdims=True) + EPS)
    normed = (rows_full * scale_in * gain_full).astype(BF16)

    def project(weight):
        return jnp.dot(normed, weight, preferred_element_type=F32)

    def lanes(vector):
        return jnp.pad(vector, (0, LANES - heads))[None, :]

    step_wide = jnp.pad(step_weight, ((0, 0), (0, LANES - heads)))
    d_mix = contract_cols(cot_full, out_weight)
    mix_out, d_gate, d_value, d_state, d_step, grads_v, grads_s, grads_h = mix(
        count,
        peers_head,
        channels * peers_head,
        lengths,
        project(value_weight),
        project(state_weight),
        project(gate_weight),
        project(step_wide),
        d_mix,
        value_filter,
        state_filter,
        value_offset[None, :],
        state_offset[None, :],
        lanes(step_bias),
        lanes(decay_log),
        jnp.repeat(skip_gain, HEAD)[None, :],
        mix_gain[None, :],
        collective_id=2,
    )
    extra, out_sum, gate_sum, value_sum, state_sum, normed_sum, mixed_sum, dot_sum = sum_over_seq(
        PLAN,
        ORDER,
        (normed, cot_full, hidden_full, scale_in, gain_full, mix_out, d_gate, d_value, d_state, d_step),
        (grads_v, grads_s, grads_h),
        (gate_weight, value_weight, out_weight, state_weight, step_wide),
        count // LINE,
        peers_head,
        3,
    )
    own_rows = hidden_in.astype(F32)
    block_out = (own_rows + mixed_sum).astype(BF16)
    delta_hidden = (
        cotangent.astype(F32)
        + scale_in * (normed_sum * norm_gain.astype(F32)[None, :])
        - own_rows * scale_in**3 * (dot_sum[0] / features)[:, None]
    )
    extra = extra[width:].astype(F32)
    states = extra.shape[1]
    norm_sum = lax.dynamic_slice_in_dim(
        extra[8 : 8 + features // states].reshape(-1), lax.axis_index("head") * width, width, 0
    )
    tiles = features // states
    step_sum = extra[16 : 16 + heads * tiles].reshape(tiles, heads, states)
    step_sum = jnp.transpose(step_sum, (0, 2, 1)).reshape(features, heads)
    at = 16 + heads * tiles
    wide = -(-channels // states)
    channel_sum = extra[at : at + 8 * wide].reshape(wide, 8, states)
    channel_sum = jnp.transpose(channel_sum, (1, 0, 2)).reshape(8, wide * states)[:, :channels]
    head_sum = extra[at + 8 * wide : at + 8 * wide + 2, :heads]
    return (
        block_out,
        delta_hidden,
        norm_sum,
        gate_sum.astype(F32),
        value_sum.astype(F32),
        step_sum,
        state_sum.reshape(features, states).astype(F32),
        channel_sum[:4],
        channel_sum[4],
        extra[:4],
        extra[4],
        head_sum[0],
        head_sum[1],
        jnp.sum(channel_sum[6].reshape(heads, HEAD), axis=1),
        channel_sum[5],
        out_sum.astype(F32),
    )


def solution(mesh):
    in_specs = (
        P("seq", "head"),
        P("head"),
        P(None, "head"),
        P(None, "head"),
        P(None, "head"),
        P(),
        P(None, "head"),
        P("head"),
        P(),
        P(),
        P("head"),
        P("head"),
        P("head"),
        P("head"),
        P("head", None),
        P(),
        P("seq", "head"),
    )
    out_specs = (
        P("seq", "head"),
        P("seq", "head"),
        P("head"),
        P(None, "head"),
        P(None, "head"),
        P(None, "head"),
        P(),
        P(None, "head"),
        P("head"),
        P(),
        P(),
        P("head"),
        P("head"),
        P("head"),
        P("head"),
        P("head", None),
    )
    return jax.shard_map(local, mesh=mesh, in_specs=in_specs, out_specs=out_specs, check_vma=False)
```

```python
import functools

import jax
import jax.numpy as jnp
from jax import lax
from jax.experimental import pallas as pl
from jax.experimental.pallas import tpu as pltpu
from jax.sharding import PartitionSpec as P

MESH = pl.DeviceIdType.MESH
F32, BF16 = jnp.float32, jnp.bfloat16
HIGH = lax.Precision.HIGHEST
EPS = 1e-05
Q = 128
LANES = 128
HEAD = 64
SUB = 8
FAR = -1e30
LINE = 4


def add_rows(target, terms, rows, dtype=BF16):
    tile = next(t for t in (32, 16, 8) if rows % t == 0)

    @pl.loop(0, rows // tile)
    def _(i):
        def at(start):
            return pl.ds(pl.multiple_of(start + i * tile, 8), tile)

        total = terms[0][0][at(terms[0][1])].astype(F32)
        for ref, start in terms[1:]:
            total = total + ref[at(start)].astype(F32)
        target[0][at(target[1])] = total.astype(dtype)


def outer(left_ref, rights, target, start, rows):
    tall = 128 if rows % 128 == 0 else rows
    for r in range(start, start + rows, tall):
        turned = left_ref[:, pl.ds(r, tall)].T
        for n, right_ref in enumerate(rights):
            columns = right_ref.shape[1]
            target[pl.ds(r, tall), pl.ds(n * columns, columns)] = jnp.dot(
                turned, right_ref[...], preferred_element_type=F32
            ).astype(target.dtype)


class Job:
    def __init__(self, index, y_first, src, dst, start, rows, lines, y_in, right, left, total, final, sems, where, mode=0):
        self.index, self.y_first, self.src, self.dst, self.start = index, y_first, src, dst, start
        self.lines, self.y_in, self.right, self.left = lines, y_in, right, left
        self.total, self.final = total, final
        self.sems, self.mode = sems, mode
        self.seq, self.z, self.y = where
        self.part = rows // lines
        self.chunk = rows // lines // LINE if y_first else rows // LINE
        self.piece = rows // lines // LINE
        self.rows = rows
        self.base = 0 if mode == 2 else start + self.y * self.part if y_first else start

    def remote(self, src, dst, name, slot, device):
        send, recv = self.sems[name]
        return pltpu.make_async_remote_copy(
            src_ref=src, dst_ref=dst, send_sem=send.at[(self.index,) + slot],
            recv_sem=recv.at[(self.index,) + slot], device_id={"seq": device}, device_id_type=MESH,
        )

    def seat(self, z, y):
        return z * self.lines + y

    def peer_y(self, d):
        return lax.rem(self.y + d, self.lines)

    def swap(self, d):
        to = self.peer_y(d)
        if self.y_first:
            src = self.src.at[pl.ds(self.start + to * self.part, self.part)]
        else:
            src = self.total.at[pl.ds(to * self.piece, self.piece)]
        return self.remote(src, self.y_in.at[d - 1], "swap", (d - 1,), self.seat(self.z, to))

    def swaps(self):
        for d in range(1, self.lines):
            self.swap(d).start()

    def join_y(self):
        for d in range(1, self.lines):
            self.swap(d).wait_recv()
        others = [(self.y_in.at[d], 0) for d in range(self.lines - 1)]
        if self.y_first:
            target = (self.final, 0) if self.mode == 1 else (self.src, self.base)
            add_rows(target, [(self.src, self.base)] + others, self.part)
        else:
            mine = self.y * self.piece
            add_rows((self.final, mine), [(self.total, mine)] + others, self.piece)

    def pass_on(self, c, z, direction, first):
        box = self.right if direction > 0 else self.left
        src = self.src.at[pl.ds(self.base + c * self.chunk, self.chunk)] if first else box.at[c]
        name = "right" if direction > 0 else "left"
        return self.remote(src, box.at[c], name, (c,), self.seat(z + direction, self.y))

    def come(self, c, direction):
        box = self.right if direction > 0 else self.left
        return self.remote(box.at[c], box.at[c], "right" if direction > 0 else "left", (c,), self.seq)

    def chain_start(self):
        @pl.when(self.z == 0)
        def _():
            for c in (3, 2, 1):
                self.pass_on(c, 0, 1, True).start()

        @pl.when(self.z == 3)
        def _():
            for c in (0, 1, 2):
                self.pass_on(c, 3, -1, True).start()

    def chain_hop(self, h):
        for z, direction, last in ((h, 1, 3), (3 - h, -1, 0)):
            box = self.right if direction > 0 else self.left

            @pl.when(self.z == z)
            def _(z=z, direction=direction, last=last, box=box):
                for c in range(last, z - direction, -direction):
                    self.come(c, direction).wait_recv()
                    if c != z:
                        add_rows((box.at[c], 0), [(box.at[c], 0), (self.src, self.base + c * self.chunk)], self.chunk)
                        self.pass_on(c, z, direction, False).start()

    def chain_end(self, seats):
        for z in seats:
            @pl.when(self.z == z)
            def _(z=z):
                terms = [(self.src, self.base + z * self.chunk)]
                if z > 0:
                    terms.append((self.right.at[z], 0))
                if z < LINE - 1:
                    terms.append((self.left.at[z], 0))
                add_rows((self.final if self.y_first else self.total, 0), terms, self.chunk)
                self.chain_done()

    def chain_done(self):
        if self.y_first:
            self.keep().start()
            self.spread_start()
            for d in range(1, self.lines):
                self.share(0, d).start()
        else:
            self.swaps()

    def place(self, z):
        first = self.y * self.part if self.y_first else 0
        return self.dst.at[pl.ds(self.start + first + z * self.chunk, self.chunk)]

    def keep(self):
        return pltpu.make_async_copy(self.final, self.place(self.z), self.sems["keep"].at[self.index])

    def spread(self, direction, h):
        src = self.final if h == 1 else self.place(self.z - direction * (h - 1))
        slot = h if direction > 0 else LINE - 1 + h
        device = self.seat(self.z + direction, self.y)
        return self.remote(src, self.place(self.z - direction * (h - 1)), "spread", (slot,), device)

    def spread_from(self, direction, h):
        slot = h if direction > 0 else LINE - 1 + h
        there = self.place(self.z - direction * h)
        return self.remote(there, there, "spread", (slot,), self.seq)

    def goes(self, direction):
        return self.z < LINE - 1 if direction > 0 else self.z > 0

    def comes(self, direction, h):
        return self.z >= h if direction > 0 else self.z < LINE - h

    def spread_start(self):
        for direction in (1, -1):
            @pl.when(self.goes(direction))
            def _(direction=direction):
                self.spread(direction, 1).start()

    def spread_hop(self, h):
        for direction in (1, -1):
            @pl.when(self.comes(direction, h))
            def _(direction=direction):
                self.spread_from(direction, h).wait_recv()
                if h < LINE - 1:
                    @pl.when(self.goes(direction))
                    def _():
                        self.spread(direction, h + 1).start()

                if self.y_first:
                    for d in range(1, self.lines):
                        self.share(h if direction > 0 else LINE - 1 + h, d).start()

    def share(self, slot, d):
        to = self.seat(self.z, self.peer_y(d))
        if self.y_first:
            if slot == 0:
                src, there = self.final, self.place(self.z)
            else:
                z = self.z - slot if slot < LINE else self.z + (slot - LINE + 1)
                src = there = self.place(z)
        else:
            src = there = self.final.at[pl.ds(self.y * self.piece, self.piece)]
        return self.remote(src, there, "share", (slot, d - 1), to)

    def share_all(self):
        for d in range(1, self.lines):
            self.share(0, d).start()

    def shared(self):
        for d in range(1, self.lines):
            self.share(0, d).wait_recv()
        self.keep().start()
        self.spread_start()

    def stages(self, make):
        def enter():
            make()
            if self.y_first:
                self.swaps()
            else:
                self.chain_start()

        def joined():
            self.join_y()
            self.chain_start()

        def second():
            self.chain_hop(2)
            self.chain_end((1, 2))

        def third():
            self.chain_hop(3)
            self.chain_end((0, 3))

        def turn():
            self.join_y()
            self.share_all()

        hops = [functools.partial(self.spread_hop, h) for h in range(1, LINE)]
        chain = [functools.partial(self.chain_hop, 1), second, third]
        if self.mode == 1:
            return [enter, self.join_y]
        if self.mode == 2:
            return [self.chain_start] + chain + hops
        if self.y_first:
            return [enter, joined] + chain + hops
        return [enter] + chain + [turn, self.shared] + hops

    def close_chain(self):
        for h in range(1, LINE):
            for direction in (1, -1):
                @pl.when(self.z == (h - 1 if direction > 0 else LINE - h))
                def _(h=h, direction=direction):
                    z = h - 1 if direction > 0 else LINE - h
                    last = LINE - 1 if direction > 0 else 0
                    for c in range(last, z, -direction):
                        self.pass_on(c, z, direction, h == 1).wait_send()

    def arrived(self):
        if not self.y_first:
            return
        for d in range(1, self.lines):
            self.share(0, d).wait_recv()
        for h in range(1, LINE):
            for direction in (1, -1):
                @pl.when(self.comes(direction, h))
                def _(h=h, direction=direction):
                    for d in range(1, self.lines):
                        self.share(h if direction > 0 else LINE - 1 + h, d).wait_recv()

    def close(self, kept=False):
        if self.mode < 2:
            for d in range(1, self.lines):
                self.swap(d).wait_send()
        if self.mode == 1:
            return
        self.close_chain()
        if not kept:
            self.keep().wait()
            self.arrived()
        for d in range(1, self.lines):
            self.share(0, d).wait_send()
        for h in range(1, LINE):
            for direction in (1, -1):
                there = self.comes(direction, h - 1) if h > 1 else True

                @pl.when(jnp.logical_and(there, self.goes(direction)))
                def _(h=h, direction=direction):
                    self.spread(direction, h).wait_send()

                if self.y_first:
                    @pl.when(self.comes(direction, h))
                    def _(h=h, direction=direction):
                        for d in range(1, self.lines):
                            self.share(h if direction > 0 else LINE - 1 + h, d).wait_send()


def job_scratch(jobs, widths, lines, gathered=0, swaps=False):
    dma, groups = pltpu.SemaphoreType.DMA, [[] for _ in range(5)]
    for j, (which, start, rows, y_first) in enumerate(jobs):
        part, piece = rows // lines, rows // lines // LINE
        chunk = piece if y_first else rows // LINE
        sizes = (
            (lines - 1, part if y_first else piece), (LINE, chunk), (LINE, chunk),
            (8 if y_first else chunk,), (chunk,),
        )
        if j < gathered:
            sizes = ((1, 8),) + sizes[1:]
        if swaps:
            sizes = sizes[:1] + ((1, 8), (1, 8), (8,), (8,))
        for group, size in zip(groups, sizes):
            group.append(pltpu.VMEM(size + (widths[which],), BF16))
    scratch = [one for group in groups for one in group]
    for slots in ((lines - 1,), (LINE,), (LINE,), (2 * LINE - 1,), (2 * LINE - 1, lines - 1)):
        scratch += [dma((len(jobs),) + slots)] * 2
    return scratch


def rows_of(plan, heights):
    jobs = []
    for which, number, parts, y_first in plan:
        rows = heights[which] // parts
        jobs.append((which, number * rows, rows, y_first))
    return jobs


def mm(left, right, contract=((1,), (0,)), precision=None):
    return lax.dot_general(
        left, right, (contract, ((), ())), precision=precision, preferred_element_type=F32
    )


def split(value):
    high = value.astype(BF16)
    return high, (value - high.astype(F32)).astype(BF16)


def twice(value, axis):
    return jnp.concatenate([value, value], axis=axis)


def sigmoid(v):
    return 1.0 / (1.0 + jnp.exp(-v))


def mixer_kernel(
    count, peers_head, inner, jobs, waves,
    lengths, hidden_in, cot_in, gate_w, value_w, state_w, out_w, step_w,
    taps_v, taps_s, gain_in, off_v_in, gain_mix_in, off_s_in, bias_own, rate_own, skip_own,
    normed, scale_in, hidden, cot, gain_full, mix_out, d_gate, d_value, d_state, d_step,
    grads_v, grads_s, grads_h, *refs,
):
    finals, refs = refs[: len(jobs)], refs[len(jobs) :]
    (
    v_in, s_in, g_in, t_in, d_mix, gate_m, value_m, state_m, out_m, step_m, off_v, gain, off_s, bias_in, rate_in, skip_in, gain_own, bias, rate, skip,
    edge_v, edge_s, first_v, first_s, val, inf, inf_low, rea, rea_low, slope_v, slope_s, segs, mask_f, mask_b,
    step, sig, logs, run, run_t, tail, into, passing, pair, scaled, scaled_low, out, inter, d_u,
    states, starts, starts_low, before, total, factors, push, got, kept, prefix, spread_sum,
    rows_out, rows_in, pre_v, pre_s, back_v, back_s, back_in_v, back_in_s,
    local_sem, gather_send, gather_recv, edge_sems, p_send, p_recv, carry_send, carry_recv, row_send, row_recv, back_sems, parts_out, parts_gate,
    ) = refs[:80]
    rest = refs[80:]
    tokens, channels = v_in.shape
    chunks, pairs, heads = tokens // Q, channels // LANES, channels // HEAD
    seq, head = lax.axis_index("seq"), lax.axis_index("head")
    window = count // 2
    steps = []
    width = window // 2
    while width >= 2:
        steps.append(width)
        width //= 2

    def remote(src, dst, send, recv, device):
        return pltpu.make_async_remote_copy(
            src_ref=src, dst_ref=dst, send_sem=send, recv_sem=recv, device_id=device, device_id_type=MESH
        )

    lines, held_jobs = count // LINE, len(jobs)
    z, y = seq // lines, lax.rem(seq, lines)
    pairs_of = rest[5 * held_jobs :]
    sems = {
        name: (pairs_of[2 * k], pairs_of[2 * k + 1])
        for k, name in enumerate(("swap", "right", "left", "spread", "share"))
    }
    work = [
        Job(j, y_first, (None, parts_out, parts_gate)[which], None, start, rows, lines,
            *(rest[k * held_jobs + j] for k in range(4)), finals[j], sems, (seq, z, y), 1)
        for j, (which, start, rows, y_first) in enumerate(jobs)
    ]

    def make(j):
        which, start, rows, y_first = jobs[j]
        if which == 1:
            return lambda: outer(mix_out, [cot.at[h] for h in range(peers_head)], parts_out, start, rows)
        return lambda: outer(normed, [d_gate], parts_gate, start, rows)

    plans = [job.stages(make(job.index)) for job in work]
    turns = list(waves)

    def wave():
        if turns:
            for j, stage in turns.pop(0):
                plans[j][stage]()

    barrier = pltpu.get_barrier_semaphore()
    others = [{"seq": lax.rem(seq + d, count)} for d in range(1, count)]
    others += [{"head": lax.rem(head + d, peers_head)} for d in range(1, peers_head)]
    for other in others:
        pl.semaphore_signal(barrier, inc=1, device_id=other, device_id_type=MESH)
    pl.semaphore_wait(barrier, len(others))

    def edge_copies():
        there = {"seq": lax.rem(seq + 1, count)}
        return [
            remote(v_in.at[pl.ds(tokens - SUB, SUB)], edge_v, edge_sems.at[0], edge_sems.at[1], there),
            remote(s_in.at[pl.ds(tokens - SUB, SUB)], edge_s, edge_sems.at[2], edge_sems.at[3], there),
        ]

    chips = peers_head // 2
    x, core = head // 2, lax.rem(head, 2)
    gain_own[...] = jnp.broadcast_to(gain_in[...].astype(F32).reshape(1, -1), gain_own.shape)
    sources, boxes = (hidden_in, gain_own, cot_in), (hidden, gain_full, cot)

    def gather(k, slot):
        mine, src = head, sources[k]
        if slot == 0 or slot >= chips:
            device = x * 2 + (1 - core)
        else:
            device = lax.rem(x + slot, chips) * 2 + core
        if slot >= chips:
            mine = lax.rem(x + 2 * chips - 1 - slot, chips) * 2 + core
            src = boxes[k].at[mine]
        return remote(
            src, boxes[k].at[mine], gather_send.at[k, slot], gather_recv.at[k, slot], {"head": device}
        )

    def gather_start(k):
        for slot in range(1, chips):
            gather(k, slot).start()
        gather(k, 0).start()

    def gather_forward(k):
        for slot in range(1, chips):
            gather(k, slot).wait_recv()
            gather(k, chips - 1 + slot).start()

    def gather_end(k):
        own[k].wait()
        gather(k, 0).wait_recv()
        for slot in range(chips, 2 * chips - 1):
            gather(k, slot).wait_recv()

    weights = [
        pltpu.make_async_copy(src, dst, local_sem.at[n])
        for n, (src, dst) in enumerate(
            (
                (value_w, value_m), (state_w, state_m), (step_w, step_m), (gate_w, gate_m), (out_w, out_m),
                (off_v_in, off_v.at[0]), (gain_mix_in, gain.at[0]), (off_s_in, off_s.at[0]),
                (bias_own, bias_in.at[0]), (rate_own, rate_in.at[0]), (skip_own, skip_in.at[0]),
            )
        )
    ]
    own = [
        pltpu.make_async_copy(sources[k], boxes[k].at[head], local_sem.at[len(weights) + k]) for k in range(3)
    ]
    gather_start(0)
    gather_start(1)
    for copy in own[:2] + weights:
        copy.start()
    gather_start(2)
    own[2].start()

    lane = lax.broadcasted_iota(jnp.int32, (Q, LANES), 1)
    row = lax.broadcasted_iota(jnp.int32, (Q, LANES), 0)
    left = lane < HEAD

    anchor = seq * tokens
    bounds, bound = [], 0
    for k in range(lengths.shape[0]):
        bound = bound + lengths[k]
        bounds.append(bound)

    def sequence(places):
        number = jnp.zeros(places.shape, F32)
        for bound in bounds:
            number = number + jnp.where(places >= bound, 1.0, 0.0)
        return number

    places = lax.broadcasted_iota(jnp.int32, (tokens + 2 * SUB, LANES), 0) + (anchor - SUB)
    segs[...] = sequence(places)
    for k in range(3):
        same = segs[pl.ds(SUB, tokens)] == segs[pl.ds(SUB - 3 + k, tokens)]
        mask_f[k] = jnp.where(same, 1.0, 0.0)
        same = segs[pl.ds(0, tokens + SUB)] == segs[pl.ds(3 - k, tokens + SUB)]
        mask_b[k] = jnp.where(same, 1.0, 0.0)
    head_of = lax.broadcasted_iota(jnp.int32, (channels, LANES), 0) // HEAD
    column = lax.broadcasted_iota(jnp.int32, (channels, LANES), 1)
    spread_sum[...] = jnp.where(head_of == column, 1.0, 0.0).astype(BF16)
    grads_v[...] = jnp.zeros_like(grads_v)
    grads_s[...] = jnp.zeros_like(grads_s)

    for copy in weights[5:]:
        copy.wait()
    bias[...] = jnp.zeros_like(bias)
    rate[...] = jnp.zeros_like(rate)
    bias[:, 0:heads] = bias_in[...]
    rate[:, 0:heads] = rate_in[...]
    t_in[...] = jnp.zeros_like(t_in)
    for p in range(pairs):
        skip[:, pl.ds(p * LANES, LANES)] = jnp.where(
            left[:1], skip_in[:, 2 * p : 2 * p + 1], skip_in[:, 2 * p + 1 : 2 * p + 2]
        )

    gather_forward(0)
    gather_forward(1)
    gather_end(0)
    gather_end(1)
    width = hidden_in.shape[1]

    @pl.loop(0, chunks)
    def _(c):
        here = pl.ds(pl.multiple_of(c * Q, Q), Q)
        squares = jnp.zeros((Q, 1), F32)
        for h in range(peers_head):
            rows = hidden[h, here].astype(F32)
            squares = squares + jnp.sum(rows * rows, axis=1, keepdims=True)
        scale = lax.rsqrt(squares / (width * peers_head) + EPS)
        scale_in[here] = scale
        for h in range(peers_head):
            rows = hidden[h, here].astype(F32)
            normed[here, pl.ds(h * width, width)] = (rows * scale * gain_full[h, 0:1]).astype(BF16)

    def project(weight, target):
        columns = weight.shape[1]
        tile = next(t for t in (256, 128, columns) if columns % t == 0)

        @pl.loop(0, columns // tile)
        def _(n):
            lanes = pl.ds(pl.multiple_of(n * tile, tile), tile)
            target[:, lanes] = mm(normed[...], weight[:, lanes])

    for copy in weights[:2]:
        copy.wait()
    project(value_m, v_in)
    project(state_m, s_in)

    @pl.when(seq < count - 1)
    def _():
        for copy in edge_copies():
            copy.start()

    weights[2].wait()
    t_in[:, 0:heads] = mm(normed[...], step_m[...], ((1,), (1,)))
    weights[3].wait()
    project(gate_m, g_in)
    gather_forward(2)

    raw = t_in[...] + bias[...]
    step[...] = jnp.maximum(raw, 0.0) + jnp.log1p(jnp.exp(-jnp.abs(raw)))
    sig[...] = sigmoid(raw)
    logs[...] = -jnp.exp(rate[...]) * step[...]
    lower = jnp.where(row >= lane, 1.0, 0.0)

    @pl.loop(0, chunks)
    def _(c):
        here = pl.ds(pl.multiple_of(c * Q, Q), Q)
        run[here] = mm(lower, logs[here], precision=HIGH)
        summed = run[here]
        run_t[c] = summed.T[:16]
        last = run[pl.ds(c * Q + Q - 1, 1)]
        mine = segs[pl.ds(pl.multiple_of(c * Q + SUB, SUB), Q)]
        at_end = segs[pl.ds(c * Q + SUB + Q - 1, 1)]
        entering = segs[pl.ds(c * Q + SUB - 1, 1)]
        tail[here] = jnp.exp(last - summed) * jnp.where(mine == at_end, 1.0, 0.0)
        into[here] = jnp.exp(summed) * jnp.where(mine == entering, 1.0, 0.0)
        through = jnp.exp(last) * jnp.where(at_end == entering, 1.0, 0.0)
        passing[c] = jnp.broadcast_to(through, (Q, LANES)).T[:16]

    product = jnp.ones((16, LANES), F32)
    for c in range(chunks):
        before[c] = product
        product = product * passing[c]
    factors[seq] = product

    def factor_copies():
        return [
            remote(
                factors.at[seq], factors.at[seq], p_send.at[d - 1], p_recv.at[d - 1],
                {"seq": lax.rem(seq + d, count)},
            )
            for d in range(1, count)
        ]

    for copy in factor_copies():
        copy.start()

    def convolve(source, base, rows, lanes, taps, offset):
        begin, size = rows
        summed = offset[:, lanes] + taps[3:4, lanes] * source[pl.ds(base, size), lanes]
        for k in range(3):
            term = taps[k : k + 1, lanes] * source[pl.ds(base - 3 + k, size), lanes]
            summed = summed + term * mask_f[k, pl.ds(begin, size)]
        s = sigmoid(summed)
        return summed * s, s * (1.0 + summed * (1.0 - s))

    def convolve_rows(c):
        rows = (c * Q, Q)
        span = pl.ds(c * Q, Q)

        @pl.loop(0, pairs)
        def _(b):
            lanes = pl.ds(pl.multiple_of(b * LANES, LANES), LANES)
            source, base = (v_in, c * Q) if c else (first_v, SUB)
            val[span, lanes], slope_v[span, lanes] = convolve(source, base, rows, lanes, taps_v, off_v)

        for b, (target, low) in enumerate(((inf, inf_low), (rea, rea_low))):
            lanes = pl.ds(b * LANES, LANES)
            source, base = (s_in, c * Q) if c else (first_s, SUB)
            active, slope_s[span, lanes] = convolve(source, base, rows, lanes, taps_s, off_s)
            target[span], low[span] = split(active)

    for c in range(1, chunks):
        convolve_rows(c)

    @pl.when(seq > 0)
    def _():
        for copy in edge_copies():
            copy.wait_recv()

    @pl.when(seq == 0)
    def _():
        edge_v[...] = jnp.zeros_like(edge_v)
        edge_s[...] = jnp.zeros_like(edge_s)

    first_v[pl.ds(0, SUB)] = edge_v[...]
    first_s[pl.ds(0, SUB)] = edge_s[...]
    first_v[pl.ds(SUB, Q)] = v_in[pl.ds(0, Q)]
    first_s[pl.ds(SUB, Q)] = s_in[pl.ds(0, Q)]
    convolve_rows(0)

    def both(ref, here, p):
        return jnp.where(left, ref[here, 2 * p : 2 * p + 1], ref[here, 2 * p + 1 : 2 * p + 2])

    def halves(value):
        return jnp.concatenate(
            [jnp.where(left, value, 0.0), jnp.where(left, 0.0, value)], axis=0
        ).astype(BF16)

    @pl.loop(0, chunks)
    def _(c):
        here = pl.ds(pl.multiple_of(c * Q, Q), Q)
        for p in range(pairs):
            lanes = pl.ds(p * LANES, LANES)
            weighted = both(step, here, p) * val[here, lanes]
            scaled[here, lanes], scaled_low[here, lanes] = split(both(tail, here, p) * weighted)
        states[c] = mm(
            twice(scaled[here], 0), jnp.concatenate([inf[here], inf_low[here]], axis=0), ((0,), (0,))
        )

    def pass_chunks(h):
        rows = pl.ds(h * HEAD, HEAD)
        held = jnp.zeros((HEAD, LANES), F32)
        for c in range(chunks):
            added = states[c, rows]
            states[c, rows] = held
            held = passing[c, h : h + 1] * held + added
        total[rows] = held

    share = channels // 2
    heads_of = (range(heads // 2), range(heads // 2, heads))

    def carry(direction):
        bank = 0 if direction == 1 else 1

        def reach(d):
            there = seq + direction * d
            return jnp.logical_and(there >= 0, there < count)

        def heard(d):
            there = seq - direction * d
            return jnp.logical_and(there >= 0, there < count)

        def copy(slot, d, half):
            source, rows = min(slot, len(steps)), pl.ds(half * share, share)
            return remote(
                push.at[bank, source, rows], got.at[bank, slot, rows],
                carry_send.at[bank, slot, half], carry_recv.at[bank, slot, half],
                {"seq": lax.rem(seq + direction * d + count, count)},
            )

        plan = [(k, d) for k, d in enumerate(steps)]
        ends = [(len(steps), 1), (len(steps) + 1, 2)]

        def send(slot, d, half):
            @pl.when(reach(d))
            def _():
                copy(slot, d, half).start()

        def factor(first, many, h):
            product = factors[first, h : h + 1]
            for i in range(1, many):
                product = product * factors[first - direction * i, h : h + 1]
            return product

        def launch(slot, half):
            rows = pl.ds(half * share, share)
            push[bank, slot, rows] = total[rows].astype(BF16)
            if slot < len(steps):
                send(*plan[slot], half)
            else:
                for end in ends:
                    send(*end, half)

        def join(slot, half):
            d = plan[slot][1]

            @pl.when(heard(d))
            def _():
                copy(slot, d, half).wait_recv()
                for h in heads_of[half]:
                    rows = pl.ds(h * HEAD, HEAD)
                    total[rows] = total[rows] + factor(seq, d, h) * got[bank, slot, rows].astype(F32)

            launch(slot + 1, half)

        def finish(half):
            part = pl.ds(half * share, share)
            total[part] = jnp.zeros((share, LANES), F32)

            @pl.when(heard(1))
            def _():
                copy(*ends[0], half).wait_recv()
                total[part] = got[bank, ends[0][0], part].astype(F32)

            @pl.when(heard(2))
            def _():
                copy(*ends[1], half).wait_recv()
                for h in heads_of[half]:
                    rows = pl.ds(h * HEAD, HEAD)
                    far = got[bank, ends[1][0], rows].astype(F32)
                    total[rows] = total[rows] + factor(seq - direction, 1, h) * far

        def close():
            for slot, d in plan + ends:
                @pl.when(reach(d))
                def _(slot=slot, d=d):
                    for half in range(2):
                        copy(slot, d, half).wait_send()

        return launch, join, finish, close

    launch, join, finish, close_forward = carry(1)
    for half in range(2):
        for h in heads_of[half]:
            pass_chunks(h)
        launch(0, half)
    gather_end(2)
    weights[4].wait()

    @pl.loop(0, tokens // (2 * Q))
    def _(n):
        here = pl.ds(pl.multiple_of(n * 2 * Q, 2 * Q), 2 * Q)
        result = jnp.zeros((2 * Q, channels), F32)
        for h in range(peers_head):
            result = result + mm(cot[h, here], out_m[:, pl.ds(h * width, width)], ((1,), (1,)))
        d_mix[here] = result

    def products(here):
        read = jnp.concatenate([rea[here], rea[here], rea_low[here]], axis=1)
        return mm(read, jnp.concatenate([inf[here], inf_low[here], inf[here]], axis=1), ((1,), (1,)))

    def from_state(high, low, c, lanes):
        state = jnp.concatenate([starts[c, lanes], starts_low[c, lanes], starts[c, lanes]], axis=1)
        return mm(jnp.concatenate([high, high, low], axis=1), state, ((1,), (1,)))

    def with_state(high, low, c, lanes):
        state = jnp.concatenate([starts[c, lanes], starts_low[c, lanes], starts[c, lanes]], axis=0)
        return mm(jnp.concatenate([high, high, low], axis=1), state)

    def within(c):
        here = pl.ds(pl.multiple_of(c * Q, Q), Q)
        mine = segs[pl.ds(pl.multiple_of(c * Q + SUB, SUB), Q)]
        across = sequence(lane + (anchor + c * Q))
        hidden = jnp.where(jnp.logical_and(mine == across, row >= lane), 0.0, FAR)
        cross = products(here)
        for p in range(pairs):
            lanes = pl.ds(p * LANES, LANES)
            mixing = []
            for h in (2 * p, 2 * p + 1):
                gap = (run[here, h : h + 1] - run_t[c, h : h + 1]) + hidden
                decay = jnp.exp(gap)
                pair[c * heads + h] = decay
                mixing.append((decay * cross).astype(BF16))
            weighted = both(step, here, p) * val[here, lanes]
            out[here, lanes] = mm(jnp.concatenate(mixing, axis=1), halves(weighted))

    @pl.loop(0, chunks // 2)
    def _(c):
        within(c)

    for copy in factor_copies():
        copy.wait_recv()
    for k in range(len(steps)):
        for half in range(2):
            join(k, half)

    @pl.loop(chunks // 2, chunks)
    def _(c):
        within(c)

    for h in range(heads):
        if h * 2 % heads == 0:
            finish(h * 2 // heads)
        rows = pl.ds(h * HEAD, HEAD)
        incoming = total[rows]
        for c in range(chunks):
            starts[c, rows], starts_low[c, rows] = split(
                states[c, rows] + before[c, h : h + 1] * incoming
            )

    rows_out[...] = jnp.zeros_like(rows_out)

    @pl.loop(0, chunks)
    def _(c):
        here = pl.ds(pl.multiple_of(c * Q, Q), Q)
        squares, dots = jnp.zeros((Q, LANES), F32), jnp.zeros((Q, LANES), F32)
        for p in range(pairs):
            lanes = pl.ds(p * LANES, LANES)
            reached = from_state(rea[here], rea_low[here], c, lanes)
            reached = reached * both(into, here, p)
            inter[here, lanes] = reached
            mixed = out[here, lanes] + reached + skip[:, lanes] * val[here, lanes]
            out[here, lanes] = mixed
            gate = g_in[here, lanes]
            gated = mixed * (gate * sigmoid(gate))
            squares = squares + gated * gated
            dots = dots + d_mix[here, lanes] * gain[:, lanes] * gated
        rows_out[0:1, here] = jnp.sum(squares.T, axis=0, keepdims=True)
        rows_out[1:2, here] = jnp.sum(dots.T, axis=0, keepdims=True)

    row_copies = [
        remote(
            rows_out, rows_in.at[d - 1], row_send.at[d - 1], row_recv.at[d - 1],
            {"head": lax.rem(head + d, peers_head)},
        )
        for d in range(1, peers_head)
    ]
    for copy in row_copies:
        copy.start()
    summed = rows_out[...]
    for d, copy in enumerate(row_copies):
        copy.wait_recv()
        summed = summed + rows_in[d]
    for copy in row_copies:
        copy.wait_send()
    rows_out[0:1] = lax.rsqrt(summed[0:1] / inner + EPS)
    rows_out[1:2] = summed[1:2] / inner

    @pl.loop(0, chunks)
    def _(c):
        here = pl.ds(pl.multiple_of(c * Q, Q), Q)
        scale = jnp.broadcast_to(rows_out[0:1, here], (Q, LANES)).T
        dot = jnp.broadcast_to(rows_out[1:2, here], (Q, LANES)).T
        cubed = scale * scale * scale * dot
        for p in range(pairs):
            lanes = pl.ds(p * LANES, LANES)
            gate, mixed, slope = g_in[here, lanes], out[here, lanes], d_mix[here, lanes]
            s = sigmoid(gate)
            opened = gate * s
            gated = mixed * opened
            normed = gated * scale
            mix_out[here, lanes] = (normed * gain[:, lanes]).astype(BF16)
            d_gated = scale * (slope * gain[:, lanes]) - gated * cubed
            d_mixer = d_gated * opened
            d_gate[here, lanes] = (d_gated * mixed * (s * (1.0 + gate * (1.0 - s)))).astype(BF16)
            out[here, lanes] = d_mixer
            d_u[here, lanes] = both(into, here, p) * d_mixer
            grads_v[5:6, lanes] = grads_v[5:6, lanes] + jnp.sum(slope * normed, axis=0, keepdims=True)
            grads_v[6:7, lanes] = grads_v[6:7, lanes] + jnp.sum(
                d_mixer * val[here, lanes], axis=0, keepdims=True
            )
        carried = d_u[here].astype(BF16)
        states[c] = mm(
            twice(carried, 0), jnp.concatenate([rea[here], rea_low[here]], axis=0), ((0,), (0,))
        )
        d_read = jnp.zeros((Q, LANES), F32)
        for p in range(pairs):
            lanes = pl.ds(p * LANES, LANES)
            d_read = d_read + with_state(*split(d_u[here, lanes]), c, lanes)
        pre_s[pl.ds(pl.multiple_of(c * Q + SUB, SUB), Q), pl.ds(LANES, LANES)] = d_read

    launch, join, finish, close_backward = carry(-1)
    for half in range(2):
        for h in heads_of[half]:
            rows = pl.ds(h * HEAD, HEAD)
            held = jnp.zeros((HEAD, LANES), F32)
            for c in reversed(range(chunks)):
                held = states[c, rows] + passing[c, h : h + 1] * held
            total[rows] = held
        launch(0, half)
    wave()
    upper = jnp.where(row < lane, 1.0, 0.0).astype(BF16)

    def within_back(c):
        here = pl.ds(pl.multiple_of(c * Q, Q), Q)
        padded = pl.ds(pl.multiple_of(c * Q + SUB, SUB), Q)
        cross = products(here)
        d_cross = jnp.zeros((Q, LANES), F32)
        from_inter = jnp.zeros((Q, LANES), F32)
        for p in range(pairs):
            lanes = pl.ds(p * LANES, LANES)
            weighted = (both(step, here, p) * val[here, lanes]).astype(BF16)
            d_out = out[here, lanes]
            d_halves = halves(d_out)
            d_pair = mm(d_halves, weighted, ((1,), (1,)))
            mixing, terms = [], []
            for i, h in enumerate((2 * p, 2 * p + 1)):
                decay = pair[c * heads + h]
                shared = d_pair[i * Q : (i + 1) * Q] * decay
                d_cross = d_cross + shared
                terms.append((shared * cross).astype(BF16))
                mixing.append((decay * cross).astype(BF16))
            d_u[here, lanes] = mm(jnp.concatenate(mixing, axis=0), d_halves, ((0,), (0,)))
            ahead = mm(jnp.concatenate(terms, axis=0), upper)
            for i, h in enumerate((2 * p, 2 * p + 1)):
                crossing = jnp.where(row >= lane, ahead[i * Q : (i + 1) * Q], 0.0)
                prefix[c, h : h + 1] = jnp.sum(crossing, axis=0, keepdims=True)
            from_inter = from_inter + mm(
                (d_out * inter[here, lanes]).astype(BF16), spread_sum[lanes]
            )
        kept[0, here] = from_inter
        d_cross = d_cross.astype(BF16)
        pre_s[padded, pl.ds(LANES, LANES)] = pre_s[padded, pl.ds(LANES, LANES)] + mm(
            d_cross, inf[here]
        )
        pre_s[padded, pl.ds(0, LANES)] = mm(d_cross, rea[here], ((0,), (0,)))

    prefix[...] = jnp.zeros_like(prefix)

    for c in range(chunks):
        if c == chunks // 2:
            for k in range(len(steps)):
                for half in range(2):
                    join(k, half)
            wave()
        within_back(c)
        wave()
    for h in range(heads):
        if h * 2 % heads == 0:
            finish(h * 2 // heads)
        rows = pl.ds(h * HEAD, HEAD)
        held = total[rows]
        for c in reversed(range(chunks)):
            start = starts[c, rows].astype(F32) + starts_low[c, rows].astype(F32)
            met = jnp.sum(held * start, axis=0, keepdims=True)
            met = jnp.sum(met, axis=1, keepdims=True) * passing[c, h : h + 1]
            prefix[c, h : h + 1] = prefix[c, h : h + 1] + met
            added = states[c, rows]
            starts[c, rows], starts_low[c, rows] = split(held)
            held = added + passing[c, h : h + 1] * held

    wave()
    from_here = jnp.where(row <= lane, 1.0, 0.0)
    under = jnp.where(row > lane, 1.0, 0.0)
    rates = -jnp.exp(rate[...])
    grads_h[...] = jnp.zeros_like(grads_h)
    pre_v[pl.ds(0, SUB)] = jnp.zeros((SUB, channels), F32)
    pre_v[pl.ds(tokens + SUB, SUB)] = jnp.zeros((SUB, channels), F32)
    pre_s[pl.ds(0, SUB)] = jnp.zeros((SUB, 2 * LANES), F32)
    pre_s[pl.ds(tokens + SUB, SUB)] = jnp.zeros((SUB, 2 * LANES), F32)

    @pl.loop(0, chunks)
    def _(c):
        here = pl.ds(pl.multiple_of(c * Q, Q), Q)
        padded = pl.ds(pl.multiple_of(c * Q + SUB, SUB), Q)
        from_tail, from_step = jnp.zeros((Q, LANES), F32), jnp.zeros((Q, LANES), F32)
        d_in = jnp.zeros((Q, LANES), F32)
        for p in range(pairs):
            lanes = pl.ds(p * LANES, LANES)
            sizes = both(step, here, p)
            value = val[here, lanes]
            d_tail = from_state(inf[here], inf_low[here], c, lanes)
            d_tail = d_tail * both(tail, here, p)
            d_weighted = d_u[here, lanes] + d_tail
            from_tail = from_tail + mm((sizes * value * d_tail).astype(BF16), spread_sum[lanes])
            from_step = from_step + mm((value * d_weighted).astype(BF16), spread_sum[lanes])
            d_val = sizes * d_weighted + skip[:, lanes] * out[here, lanes]
            pre_v[padded, lanes] = d_val * slope_v[here, lanes]
            d_in = d_in + with_state(scaled[here, lanes], scaled_low[here, lanes], c, lanes)
        inflow, readout = pl.ds(0, LANES), pl.ds(LANES, LANES)
        pre_s[padded, inflow] = (pre_s[padded, inflow] + d_in) * slope_s[here, inflow]
        pre_s[padded, readout] = pre_s[padded, readout] * slope_s[here, readout]
        d_log = mm(from_here, kept[0, here], precision=HIGH) + mm(under, from_tail, precision=HIGH)
        filled = jnp.concatenate([prefix[c], jnp.zeros((Q - 16, LANES), F32)], axis=0)
        d_log = d_log + filled.T
        d_size = (from_step + rates * d_log) * sig[here]
        d_step[here] = d_size.astype(BF16)
        grads_h[0:1] = grads_h[0:1] + jnp.sum(d_size, axis=0, keepdims=True)
        grads_h[1:2] = grads_h[1:2] + jnp.sum(d_log * logs[here], axis=0, keepdims=True)

    wave()

    def back(source, base, size, lanes, taps):
        summed = taps[3:4, lanes] * source[pl.ds(base, size), lanes]
        for k in range(3):
            term = taps[k : k + 1, lanes] * source[pl.ds(base + 3 - k, size), lanes]
            summed = summed + term * mask_b[k, pl.ds(base, size)]
        return summed

    def back_copies():
        there = {"seq": lax.rem(seq + count - 1, count)}
        return [
            remote(back_v, back_in_v, back_sems.at[0], back_sems.at[1], there),
            remote(back_s, back_in_s, back_sems.at[2], back_sems.at[3], there),
        ]

    for b in range(pairs):
        lanes = pl.ds(b * LANES, LANES)
        back_v[:, lanes] = back(pre_v, 0, SUB, lanes, taps_v)
    for b in range(2):
        lanes = pl.ds(b * LANES, LANES)
        back_s[:, lanes] = back(pre_s, 0, SUB, lanes, taps_s)

    @pl.when(seq > 0)
    def _():
        for copy in back_copies():
            copy.start()

    def filter_grads(pre, source, base, c, lanes, grads):
        rows = pl.ds(c * Q + SUB, Q)
        slope = pre[rows, lanes]
        for k in range(3):
            term = slope * mask_f[k, pl.ds(c * Q, Q)] * source[pl.ds(base - 3 + k, Q), lanes]
            grads[k : k + 1, lanes] = grads[k : k + 1, lanes] + jnp.sum(term, axis=0, keepdims=True)
        term = slope * source[pl.ds(base, Q), lanes]
        grads[3:4, lanes] = grads[3:4, lanes] + jnp.sum(term, axis=0, keepdims=True)
        grads[4:5, lanes] = grads[4:5, lanes] + jnp.sum(slope, axis=0, keepdims=True)

    for c in range(chunks):
        if c == chunks - 1:
            @pl.when(seq < count - 1)
            def _():
                for copy in back_copies():
                    copy.wait_recv()

            @pl.when(seq == count - 1)
            def _():
                back_in_v[...] = jnp.zeros_like(back_in_v)
                back_in_s[...] = jnp.zeros_like(back_in_s)

        def one(pre, source, base, c, lanes, taps, grads, target, received):
            result = back(pre, c * Q + SUB, Q, lanes, taps)
            if c == chunks - 1:
                result = jnp.concatenate(
                    [result[: Q - SUB], result[Q - SUB :] + received[:, lanes]], axis=0
                )
            target[pl.ds(c * Q, Q), lanes] = result.astype(BF16)
            filter_grads(pre, source, base, c, lanes, grads)

        @pl.loop(0, pairs)
        def _(b, c=c):
            lanes = pl.ds(pl.multiple_of(b * LANES, LANES), LANES)
            source, base = (v_in, c * Q) if c else (first_v, SUB)
            one(pre_v, source, base, c, lanes, taps_v, grads_v, d_value, back_in_v)

        wave()
        for b in range(2):
            lanes = pl.ds(b * LANES, LANES)
            source, base = (s_in, c * Q) if c else (first_s, SUB)
            one(pre_s, source, base, c, lanes, taps_s, grads_s, d_state, back_in_s)

    @pl.when(seq < count - 1)
    def _():
        for copy in edge_copies():
            copy.wait_send()

    @pl.when(seq > 0)
    def _():
        for copy in back_copies():
            copy.wait_send()

    while turns:
        wave()
    for job in work:
        job.close()
    for k in range(3):
        for slot in range(2 * chips - 1):
            gather(k, slot).wait_send()
    for copy in factor_copies():
        copy.wait_send()
    close_forward()
    close_backward()


def mix(count, peers_head, lengths, hidden, cot, weights, filters, gain, vectors, plan, waves, collective_id):
    tokens, width = hidden.shape
    channels = weights[0].shape[1]
    chunks, heads, inner = tokens // Q, channels // HEAD, channels * peers_head
    chips = peers_head // 2
    slots = 1
    reach = count // 4
    while reach >= 2:
        slots += 1
        reach //= 2
    vmem, dma = pltpu.VMEM, pltpu.SemaphoreType.DMA
    shape = jax.ShapeDtypeStruct
    outs = [
        shape((tokens, width * peers_head), BF16), shape((tokens, 1), F32),
        shape((peers_head, tokens, width), BF16), shape((peers_head, tokens, width), BF16),
        shape((peers_head, 8, width), F32),
        shape((tokens, channels), BF16), shape((tokens, channels), BF16),
        shape((tokens, channels), BF16), shape((tokens, 2 * LANES), BF16),
        shape((tokens, LANES), BF16),
        shape((8, channels), F32), shape((8, 2 * LANES), F32), shape((8, LANES), F32),
    ]
    features = width * peers_head
    jobs = rows_of(plan, (0, channels, features))
    for which, start, rows, y_first in jobs:
        outs.append(shape((rows // (count // LINE), (0, features, channels)[which]), BF16))
    wide, narrow = (tokens, channels), (tokens, LANES)
    scratch = [
        vmem(wide, F32), vmem((tokens, 2 * LANES), F32), vmem(wide, F32), vmem(narrow, F32), vmem(wide, F32),
    ]
    scratch += [vmem(weight.shape, BF16) for weight in weights]
    scratch += [vmem((1,) + vector.shape, F32) for vector in vectors]
    scratch += [
        vmem((8, width), F32), vmem((1, LANES), F32), vmem((1, LANES), F32), vmem((1, channels), F32),
        vmem((SUB, channels), F32), vmem((SUB, 2 * LANES), F32),
        vmem((Q + SUB, channels), F32), vmem((Q + SUB, 2 * LANES), F32),
        vmem(wide, F32), vmem(narrow, BF16), vmem(narrow, BF16), vmem(narrow, BF16), vmem(narrow, BF16),
        vmem(wide, F32), vmem((tokens, 2 * LANES), F32),
        vmem((tokens + 2 * SUB, LANES), F32),
        vmem((3, tokens, LANES), F32), vmem((3, tokens + SUB, LANES), F32),
        vmem(narrow, F32), vmem(narrow, F32), vmem(narrow, F32), vmem(narrow, F32),
        vmem((chunks, 16, LANES), F32), vmem(narrow, F32), vmem(narrow, F32),
        vmem((chunks, 16, LANES), F32),
        vmem((chunks * heads, Q, LANES), F32), vmem(wide, BF16), vmem(wide, BF16),
        vmem(wide, F32), vmem(wide, F32), vmem(wide, F32),
        vmem((chunks, channels, LANES), F32),
        vmem((chunks, channels, LANES), BF16), vmem((chunks, channels, LANES), BF16),
        vmem((chunks, 16, LANES), F32), vmem((channels, LANES), F32),
        vmem((count, 16, LANES), F32),
        vmem((2, slots, channels, LANES), BF16), vmem((2, slots + 1, channels, LANES), BF16),
        vmem((1, tokens, LANES), F32), vmem((chunks, 16, LANES), F32),
        vmem((channels, LANES), BF16),
        vmem((8, tokens), F32), vmem((peers_head - 1, 8, tokens), F32),
        vmem((tokens + 2 * SUB, channels), F32), vmem((tokens + 2 * SUB, 2 * LANES), F32),
        vmem((SUB, channels), F32), vmem((SUB, 2 * LANES), F32),
        vmem((SUB, channels), F32), vmem((SUB, 2 * LANES), F32),
        dma((14,)), dma((3, 2 * chips - 1)), dma((3, 2 * chips - 1)),
        dma((4,)), dma((count - 1,)), dma((count - 1,)),
        dma((2, slots + 1, 2)), dma((2, slots + 1, 2)),
        dma((peers_head - 1,)), dma((peers_head - 1,)), dma((4,)),
        vmem((channels, features), BF16),
        vmem((max([start + rows for which, start, rows, _ in jobs if which == 2] + [8]), channels), BF16),
    ]
    scratch += job_scratch(jobs, (0, features, channels), count // LINE, 0, True)
    inside, anywhere = pl.BlockSpec(memory_space=pltpu.VMEM), pl.BlockSpec(memory_space=pl.ANY)
    return pl.pallas_call(
        functools.partial(mixer_kernel, count, peers_head, inner, jobs, waves),
        out_shape=outs,
        in_specs=[pl.BlockSpec(memory_space=pltpu.SMEM)]
        + [anywhere] * 7 + [inside] * 3 + [anywhere] * len(vectors),
        out_specs=[inside] * len(outs),
        scratch_shapes=scratch,
        compiler_params=pltpu.CompilerParams(
            collective_id=collective_id, has_side_effects=True, vmem_limit_bytes=61 * 1024 * 1024
        ),
    )(lengths, hidden, cot, *weights, *filters, gain, *vectors)


def sum_rows(jobs, order, lines, peers_head, early, *refs):
    (normed, cot, hidden, scale, gain, mix_out, d_gate, d_value, d_state, d_step, grads_v, grads_s, grads_h,
     gate_w, value_w, out_w, state_w, step_w) = refs[:18]
    given, refs = refs[18 : 18 + early], refs[18 + early :]
    outs, (every, normed_sum, mixed_sum, dots_sum) = refs[:4], refs[4:8]
    scratch = refs[8:]
    count = len(jobs)
    y_in, right, left, total, final = (scratch[k * count : (k + 1) * count] for k in range(5))
    names = ("swap", "right", "left", "spread", "share")
    pairs = scratch[5 * count : 5 * count + 10]
    sems = {name: (pairs[2 * k], pairs[2 * k + 1]) for k, name in enumerate(names)}
    (sems["keep"], packed, out_part, gate_part, value_part, gate_m, value_m, out_m, state_m, step_m,
     blocks, block_in, normed_part, normed_in, mixed_part, mixed_in, dots, dots_in, gain_part, rest, product,
     local_sem, hs, hr) = scratch[5 * count + 10 :]
    parts = [packed, out_part, gate_part, value_part]
    tokens, features = normed.shape
    width, channels = features // peers_head, d_gate.shape[1]
    heads = channels // HEAD
    seq, head = lax.axis_index("seq"), lax.axis_index("head")
    z, y = seq // lines, lax.rem(seq, lines)
    work = [
        Job(j, y_first, given[j] if j < early else parts[which], outs[which], start, rows, lines,
            y_in[j], right[j], left[j], total[j], final[j], sems, (seq, z, y), 2 if j < early else 0)
        for j, (which, start, rows, y_first) in enumerate(jobs)
    ]
    shared = [j for j in range(count) if not jobs[j][0]][0]

    loads = [
        pltpu.make_async_copy(src, dst, local_sem.at[k])
        for k, (src, dst) in enumerate(
            ((gate_w, gate_m), (value_w, value_m), (out_w, out_m), (state_w, state_m), (step_w, step_m))
        )
    ]
    for copy in loads:
        copy.start()

    barrier = pltpu.get_barrier_semaphore()
    peers = [{"seq": z * lines + lax.rem(y + d, lines)} for d in range(1, lines)]
    peers += [{"head": lax.rem(head + d, peers_head)} for d in range(1, peers_head)]
    for peer in peers:
        pl.semaphore_signal(barrier, inc=1, device_id=peer, device_id_type=MESH)
    for direction in (1, -1):
        @pl.when(z < LINE - 1 if direction > 0 else z > 0)
        def _(direction=direction):
            pl.semaphore_signal(
                barrier, inc=1, device_id={"seq": (z + direction) * lines + y}, device_id_type=MESH
            )

    ends = jnp.logical_or(z == 0, z == LINE - 1)

    @pl.when(ends)
    def _():
        pl.semaphore_wait(barrier, len(peers) + 1)

    @pl.when(jnp.logical_not(ends))
    def _():
        pl.semaphore_wait(barrier, len(peers) + 2)

    block = blocks.shape[1]

    def head_copies(kind):
        for d in range(1, peers_head):
            to = lax.rem(head + d, peers_head)
            if kind < 4:
                src = (blocks.at[to], dots, normed_part.at[to], mixed_part.at[to])[kind]
                dst = (block_in, dots_in, normed_in, mixed_in)[kind].at[d - 1]
            else:
                src, dst = outs[0].at[pl.ds(0, width)], every.at[head]
            yield pltpu.make_async_remote_copy(
                src_ref=src, dst_ref=dst, send_sem=hs.at[kind, d - 1], recv_sem=hr.at[kind, d - 1],
                device_id={"head": to}, device_id_type=MESH,
            )

    def start(copies):
        for copy in copies:
            copy.start()

    def received(copies):
        for copy in copies:
            copy.wait_recv()

    def make(j):
        which, begin, rows, y_first = jobs[j]
        if j < early:
            return None
        if not which:
            return pack
        if which == 1:
            return lambda: outer(mix_out, [cot.at[h] for h in range(peers_head)], out_part, begin, rows)
        return lambda: outer(normed, [(d_gate, d_value)[which - 2]], parts[which], begin, rows)

    def over_head(quarter):
        if quarter == 0:
            for copy in loads:
                copy.wait()
            dots[...] = jnp.zeros_like(dots)
            gain_part[...] = jnp.zeros_like(gain_part)

        def by_head(h):
            mine = pl.ds(h * width, width)
            result = jnp.zeros((tokens, width), F32)
            for left_ref, right_ref in (
                (d_gate, gate_m), (d_value, value_m), (d_state, state_m)
            ):
                result = result + lax.dot_general(
                    left_ref[...], right_ref[mine], (((1,), (1,)), ((), ())), preferred_element_type=F32
                )
            result = result + jnp.dot(d_step[:, 0:heads], step_m[:, mine], preferred_element_type=F32)
            product[...] = result
            mixed_part[h] = jnp.dot(
                mix_out[...], out_m[:, mine], preferred_element_type=F32
            ).astype(BF16)

            @pl.loop(0, tokens // Q)
            def _(c):
                here = pl.ds(pl.multiple_of(c * Q, Q), Q)
                result = product[here]
                normed_part[h, here] = result.astype(BF16)
                rows = result * hidden[h, here].astype(F32)
                gain_part[:, mine] = gain_part[:, mine] + jnp.sum(
                    rows * scale[here], axis=0, keepdims=True
                )
                dot = jnp.sum(rows * gain[h, 0:1], axis=1, keepdims=True)
                dot = jnp.broadcast_to(dot, (Q, LANES)).T
                dots[:, here] = dots[:, here] + dot[:8]

        for h in range(quarter * peers_head // 4, (quarter + 1) * peers_head // 4):
            by_head(h)

    def over_head_send():
        states = blocks.shape[2]
        rest[...] = jnp.zeros_like(rest)
        rest[0:8] = grads_s[...]
        for k in range(features // states):
            rest[8 + k : 9 + k] = gain_part[:, pl.ds(k * states, states)]
        for h in range(peers_head):
            turned = normed[:, pl.ds(h * width, width)].T
            blocks[h, pl.ds(0, width)] = jnp.dot(
                turned, d_state[...], preferred_element_type=F32
            ).astype(BF16)
            blocks[h, pl.ds(width, 16)] = rest[0:16].astype(BF16)
        for kind in range(4):
            start(head_copies(kind))
        steps = lax.dot_general(
            d_step[...], normed[...], (((0,), (0,)), ((), ())), preferred_element_type=F32
        )
        for k in range(features // states):
            rest[16 + k * heads : 16 + (k + 1) * heads] = steps[:heads, k * states : (k + 1) * states]
        at = 16 + heads * (features // states)
        for k in range(0, channels, states):
            lanes = min(states, channels - k)
            rest[at : at + 8, 0:lanes] = grads_v[:, pl.ds(k, lanes)]
            at += 8
        rest[at : at + 2, 0:LANES] = grads_h[0:2]
        packed[pl.ds(block, rest.shape[0] - 16)] = rest[16:].astype(BF16)

    def pack():
        received(head_copies(0))
        others = [(block_in.at[d], 0) for d in range(peers_head - 1)]
        add_rows((packed, 0), [(blocks.at[head], 0)] + others, block)

    def sum_heads():
        received(head_copies(1))
        summed = dots[...]
        for d in range(peers_head - 1):
            summed = summed + dots_in[d]
        dots_sum[...] = summed
        for kind, mine, boxes, target in (
            (2, normed_part, normed_in, normed_sum), (3, mixed_part, mixed_in, mixed_sum)
        ):
            received(head_copies(kind))
            others = [(boxes.at[d], 0) for d in range(peers_head - 1)]
            add_rows((target, 0), [(mine.at[head], 0)] + others, tokens, F32)

    plans = [job.stages(make(job.index)) for job in work]

    def give():
        work[shared].keep().wait()
        work[shared].arrived()
        mine = pltpu.make_async_copy(outs[0].at[pl.ds(0, width)], every.at[head], local_sem.at[0])
        mine.start()
        start(head_copies(4))
        mine.wait()

    plans[shared].append(give)
    plans.append([functools.partial(over_head, q) for q in range(4)] + [over_head_send, sum_heads])
    for j, stage in order:
        plans[j][stage]()
    for job in work:
        job.close(job.index == shared)
    received(head_copies(4))
    for kind in range(5):
        for copy in head_copies(kind):
            copy.wait_send()


def sum_over_seq(plan, order, values, grads, weights, given, lines, peers_head, collective_id):
    normed, d_gate, d_state = values[0], values[6], values[8]
    tokens, features = normed.shape
    channels, states, width = d_gate.shape[1], d_state.shape[1], normed.shape[1] // peers_head
    heads = channels // HEAD
    shape, dma, vmem = jax.ShapeDtypeStruct, pltpu.SemaphoreType.DMA, pltpu.VMEM
    extra = heads * (features // states) + 8 * -(-channels // states) + 8
    total = -(-(width + 16 + extra) // (8 * lines * LINE)) * 8 * lines * LINE
    whole = [
        shape((total, states), BF16), shape((channels, features), BF16),
        shape((features, channels), BF16), shape((features, channels), BF16),
    ]
    jobs = rows_of(plan, [one.shape[0] for one in whole])
    count = len(jobs)
    scratch = job_scratch(jobs, [one.shape[1] for one in whole], lines, len(given))
    others = peers_head - 1
    scratch += [dma((count,))]
    scratch += [vmem(one.shape, BF16) for one in whole]
    scratch += [vmem(one.shape, BF16) for one in weights]
    scratch += [
        vmem((peers_head, width + 16, states), BF16), vmem((others, width + 16, states), BF16),
        vmem((peers_head, tokens, width), BF16), vmem((others, tokens, width), BF16),
        vmem((peers_head, tokens, width), BF16), vmem((others, tokens, width), BF16),
        vmem((8, tokens), F32), vmem((others, 8, tokens), F32), vmem((1, features), F32),
        vmem((total - width, states), F32), vmem((tokens, width), F32),
        dma((5,)), dma((5, others)), dma((5, others)),
    ]
    anywhere, inside = pl.BlockSpec(memory_space=pl.ANY), pl.BlockSpec(memory_space=pltpu.VMEM)
    operands = list(values) + list(grads)
    return pl.pallas_call(
        functools.partial(sum_rows, jobs, order, lines, peers_head, len(given)),
        out_shape=whole
        + [shape((peers_head, width, states), BF16)]
        + [shape((tokens, width), F32)] * 2
        + [shape((8, tokens), F32)],
        in_specs=[inside] * len(operands) + [anywhere] * 5 + [inside] * len(given),
        out_specs=[anywhere] * 5 + [inside] * 3,
        scratch_shapes=scratch,
        compiler_params=pltpu.CompilerParams(
            collective_id=collective_id, has_side_effects=True, vmem_limit_bytes=61 * 1024 * 1024
        ),
    )(*operands, *weights, *given)


def finish_kernel(
    features, steps, out_sum, gate_sum, value_sum, state_sum, hidden, cot, scale, gain, normed_sum, mixed_sum,
    dots, extra,
    out_grad, gate_grad, value_grad, state_grad, block_out, delta_hidden, step_grad, filter_v, filter_s,
    norm_grad, offset_v, offset_s, bias_grad, decay_grad, skip_grad, mix_grad,
    small, row, flat, head_row, column,
):
    step = pl.program_id(0)
    width, channels = hidden.shape[1], filter_v.shape[1]
    heads, states = channels // HEAD, extra.shape[1]
    for source, target in (
        (out_sum, out_grad), (gate_sum, gate_grad), (value_sum, value_grad), (state_sum, state_grad)
    ):
        target[...] = source[...].astype(F32)
    rows = hidden[...].astype(F32)
    block_out[...] = (rows + mixed_sum[...]).astype(BF16)

    @pl.when(step == 0)
    def _():
        dot = jnp.broadcast_to(dots[0:1] / features, (Q, dots.shape[1]))
        column[...] = jnp.concatenate(
            [dot[:, c * Q : (c + 1) * Q].T for c in range(dots.shape[1] // Q)], axis=0
        )[:, 0:1]

    count = rows.shape[0]
    mine = column[pl.ds(pl.multiple_of(step * count, count), count)]
    size = scale[...]
    delta_hidden[...] = (
        cot[...].astype(F32)
        + size * (normed_sum[...] * gain[...].astype(F32).reshape(1, width))
        - rows * (size * size * size) * mine
    )

    @pl.when(step == 1)
    def _():
        small[...] = extra[...].astype(F32)
        at = width + 16
        tiles = features // states
        for k in range(tiles):
            step_grad[:, pl.ds(k * states, states)] = small[at + k * heads : at + (k + 1) * heads]
            flat[0:1, pl.ds(k * states, states)] = small[width + 8 + k : width + 9 + k]
        at += tiles * heads
        for k in range(0, channels, states):
            lanes = min(states, channels - k)
            row[:, pl.ds(k, lanes)] = small[at : at + 8, 0:lanes]
            at += 8
        filter_v[...] = row[0:4]
        filter_s[...] = small[width : width + 4]
        head = lax.axis_index("head")
        chosen = flat[0:1, 0:width]
        for h in range(1, features // width):
            chosen = jnp.where(head == h, flat[0:1, pl.ds(h * width, width)], chosen)
        norm_grad[...] = chosen.reshape(width)
        offset_v[...] = row[4:5].reshape(channels)
        offset_s[...] = small[width + 4 : width + 5].reshape(states)
        mix_grad[...] = row[5:6].reshape(channels)
        of_head = lax.broadcasted_iota(jnp.int32, (channels, LANES), 0) // HEAD
        lane = lax.broadcasted_iota(jnp.int32, (channels, LANES), 1)
        gather = jnp.where(of_head == lane, 1.0, 0.0)
        summed = jnp.dot(row[...], gather, precision=HIGH, preferred_element_type=F32)
        head_row[0:1] = small[at : at + 1, 0:LANES]
        head_row[1:2] = small[at + 1 : at + 2, 0:LANES]
        head_row[2:3] = summed[6:7]
        for k, target in enumerate((bias_grad, decay_grad, skip_grad)):
            target[...] = head_row[k : k + 1, 0:heads].reshape(heads)


def finish(out_sum, gate_sum, value_sum, state_sum, hidden, cot, scale, gain, normed_sum, mixed_sum, dots, extra):
    tokens, width = hidden.shape
    channels, features = out_sum.shape
    heads, states, steps = channels // HEAD, extra.shape[1], 8
    shape = jax.ShapeDtypeStruct

    def tiles(array):
        return pl.BlockSpec((array.shape[0] // steps, array.shape[1]), lambda k: (k, 0))

    def all_of(array):
        return pl.BlockSpec(array.shape, lambda k: (0,) * len(array.shape))

    state_sum = state_sum.reshape(features, states)
    tiled = [out_sum, gate_sum, value_sum, state_sum]
    rows = [hidden, cot, scale]
    outs = [shape(one.shape, F32) for one in tiled]
    outs += [shape(hidden.shape, BF16), shape(hidden.shape, F32)]
    small = [(heads, features), (4, channels), (4, states)]
    small += [(width,), (channels,), (states,), (heads,), (heads,), (heads,), (channels,)]
    small = [shape(one, F32) for one in small]
    return pl.pallas_call(
        functools.partial(finish_kernel, features, steps),
        grid=(steps,),
        out_shape=outs + small,
        in_specs=[tiles(one) for one in tiled + rows]
        + [all_of(gain), tiles(normed_sum), tiles(mixed_sum), all_of(dots), all_of(extra)],
        out_specs=[tiles(one) for one in outs] + [all_of(one) for one in small],
        scratch_shapes=[
            pltpu.VMEM(extra.shape, F32), pltpu.VMEM((8, channels), F32), pltpu.VMEM((8, features), F32),
            pltpu.VMEM((8, LANES), F32), pltpu.VMEM((tokens, 1), F32),
        ],
        compiler_params=pltpu.CompilerParams(dimension_semantics=("arbitrary",)),
    )(*tiled, *rows, gain, normed_sum, mixed_sum, dots, extra)


PLAN = (
    (1, 0, 3, True), (1, 1, 3, True), (1, 2, 3, True), (2, 0, 3, False),
    (2, 1, 3, True), (2, 2, 3, True), (0, 0, 1, True), (3, 0, 3, False),
    (3, 1, 3, True), (3, 2, 3, True),
)
EARLY = 2
WAVES = (
    ((0, 0),), (), (), ((1, 0),),
    (), (), (), ((0, 1),),
    (), (), (), ((1, 1),),
)
ORDER = (
    (0, 0), (2, 0), (10, 0), (3, 0), (5, 0), (0, 1), (4, 0), (0, 2), (10, 1), (0, 3),
    (10, 2), (3, 1), (0, 4), (10, 3), (2, 1), (3, 2), (5, 1), (2, 2), (10, 4), (9, 0),
    (5, 2), (3, 3), (2, 3), (5, 3), (4, 1), (4, 2), (2, 4), (3, 4), (1, 0), (5, 4),
    (2, 5), (6, 0), (4, 3), (3, 5), (0, 5), (4, 4), (9, 1), (1, 1), (8, 0), (3, 6),
    (1, 2), (0, 6), (7, 0), (3, 7), (1, 3), (9, 2), (5, 5), (6, 1), (2, 6), (9, 3),
    (7, 1), (4, 5), (5, 6), (9, 4), (7, 2), (6, 2), (9, 5), (6, 3), (8, 1), (4, 6),
    (7, 3), (8, 2), (5, 7), (2, 7), (3, 8), (9, 6), (6, 4), (7, 4), (6, 5), (8, 3),
    (8, 4), (1, 4), (6, 6), (1, 5), (7, 5), (6, 7), (9, 7), (4, 7), (10, 5), (8, 5),
    (7, 6), (1, 6), (6, 8), (8, 6), (8, 7), (7, 7), (7, 8),
)


def contract_rows(left, right):
    return lax.dot_general(
        left, right, (((0,), (0,)), ((), ())), preferred_element_type=jnp.float32
    )


def contract_cols(left, right):
    return lax.dot_general(
        left, right, (((1,), (1,)), ((), ())), preferred_element_type=jnp.float32
    )


def local(
    hidden_in,
    norm_gain,
    gate_weight,
    value_weight,
    step_weight,
    state_weight,
    value_filter,
    value_offset,
    state_filter,
    state_offset,
    step_bias,
    decay_log,
    skip_gain,
    mix_gain,
    out_weight,
    lengths,
    cotangent,
):
    tokens, width = hidden_in.shape
    heads, channels = step_weight.shape[1], value_weight.shape[1]
    count, peers_head = lax.axis_size("seq"), lax.axis_size("head")
    features = width * peers_head
    step_turned = step_weight.T
    normed, scale_in, *values = mix(
        count,
        peers_head,
        lengths,
        hidden_in,
        cotangent,
        (gate_weight, value_weight, state_weight, out_weight, step_turned),
        (value_filter, state_filter),
        norm_gain,
        (value_offset, mix_gain, state_offset, step_bias, decay_log, skip_gain),
        PLAN[:EARLY],
        WAVES,
        collective_id=2,
    )
    hidden_full, cot_full, gain_full, mix_out, d_gate, d_value, d_state, d_step = values[:8]
    grads_v, grads_s, grads_h = values[8:11]
    extra, out_sum, gate_sum, value_sum, state_sum, normed_sum, mixed_sum, dot_sum = sum_over_seq(
        PLAN,
        ORDER,
        (normed, cot_full, hidden_full, scale_in, gain_full, mix_out, d_gate, d_value, d_state, d_step),
        (grads_v, grads_s, grads_h),
        (gate_weight, value_weight, out_weight, state_weight, step_turned),
        values[11:],
        count // LINE,
        peers_head,
        3,
    )
    (
        out_grad, gate_grad, value_grad, state_grad, block_out, delta_hidden, step_grad, filter_v, filter_s,
        norm_grad, offset_v, offset_s, bias_grad, decay_grad, skip_grad, mix_grad,
    ) = finish(
        out_sum, gate_sum, value_sum, state_sum, hidden_in, cotangent, scale_in, norm_gain,
        normed_sum, mixed_sum, dot_sum, extra,
    )
    return (
        block_out,
        delta_hidden,
        norm_grad,
        gate_grad,
        value_grad,
        step_grad.T,
        state_grad,
        filter_v,
        offset_v,
        filter_s,
        offset_s,
        bias_grad,
        decay_grad,
        skip_grad,
        mix_grad,
        out_grad,
    )


def solution(mesh):
    in_specs = (
        P("seq", "head"),
        P("head"),
        P(None, "head"),
        P(None, "head"),
        P(None, "head"),
        P(),
        P(None, "head"),
        P("head"),
        P(),
        P(),
        P("head"),
        P("head"),
        P("head"),
        P("head"),
        P("head", None),
        P(),
        P("seq", "head"),
    )
    out_specs = (
        P("seq", "head"),
        P("seq", "head"),
        P("head"),
        P(None, "head"),
        P(None, "head"),
        P(None, "head"),
        P(),
        P(None, "head"),
        P("head"),
        P(),
        P(),
        P("head"),
        P("head"),
        P("head"),
        P("head"),
        P("head", None),
    )
    return jax.shard_map(local, mesh=mesh, in_specs=in_specs, out_specs=out_specs, check_vma=False)
```

```python
import functools

import jax
import jax.numpy as jnp
from jax import lax
from jax.experimental import pallas as pl
from jax.experimental.pallas import tpu as pltpu
from jax.sharding import PartitionSpec as P

MESH = pl.DeviceIdType.MESH
F32, BF16 = jnp.float32, jnp.bfloat16
HIGH = lax.Precision.HIGHEST
EPS = 1e-05
Q = 128
LANES = 128
HEAD = 64
SUB = 8
FAR = -1e30
LINE = 4


def add_rows(target, terms, rows, dtype=BF16):
    tile = next(t for t in (32, 16, 8) if rows % t == 0)

    @pl.loop(0, rows // tile)
    def _(i):
        def at(start):
            return pl.ds(pl.multiple_of(start + i * tile, 8), tile)

        total = terms[0][0][at(terms[0][1])].astype(F32)
        for ref, start in terms[1:]:
            total = total + ref[at(start)].astype(F32)
        target[0][at(target[1])] = total.astype(dtype)


def outer(left_ref, rights, target, start, rows):
    tall = 128 if rows % 128 == 0 else rows
    for r in range(start, start + rows, tall):
        turned = left_ref[:, pl.ds(r, tall)].T
        for n, right_ref in enumerate(rights):
            columns = right_ref.shape[1]
            target[pl.ds(r, tall), pl.ds(n * columns, columns)] = jnp.dot(
                turned, right_ref[...], preferred_element_type=F32
            ).astype(target.dtype)


class Job:
    def __init__(self, index, y_first, src, dst, start, rows, lines, y_in, right, left, total, final, sems, where, mode=0):
        self.index, self.y_first, self.src, self.dst, self.start = index, y_first, src, dst, start
        self.lines, self.y_in, self.right, self.left = lines, y_in, right, left
        self.total, self.final = total, final
        self.sems, self.mode = sems, mode
        self.seq, self.z, self.y = where
        self.part = rows // lines
        self.chunk = rows // lines // LINE if y_first else rows // LINE
        self.piece = rows // lines // LINE
        self.rows = rows
        self.base = 0 if mode == 2 else start + self.y * self.part if y_first else start

    def remote(self, src, dst, name, slot, device):
        send, recv = self.sems[name]
        return pltpu.make_async_remote_copy(
            src_ref=src, dst_ref=dst, send_sem=send.at[(self.index,) + slot],
            recv_sem=recv.at[(self.index,) + slot], device_id={"seq": device}, device_id_type=MESH,
        )

    def seat(self, z, y):
        return z * self.lines + y

    def peer_y(self, d):
        return lax.rem(self.y + d, self.lines)

    def swap(self, d):
        to = self.peer_y(d)
        if self.y_first:
            src = self.src.at[pl.ds(self.start + to * self.part, self.part)]
        else:
            src = self.total.at[pl.ds(to * self.piece, self.piece)]
        return self.remote(src, self.y_in.at[d - 1], "swap", (d - 1,), self.seat(self.z, to))

    def swaps(self):
        for d in range(1, self.lines):
            self.swap(d).start()

    def join_y(self):
        for d in range(1, self.lines):
            self.swap(d).wait_recv()
        others = [(self.y_in.at[d], 0) for d in range(self.lines - 1)]
        if self.y_first:
            target = (self.final, 0) if self.mode == 1 else (self.src, self.base)
            add_rows(target, [(self.src, self.base)] + others, self.part)
        else:
            mine = self.y * self.piece
            add_rows((self.final, mine), [(self.total, mine)] + others, self.piece)

    def pass_on(self, c, z, direction, first):
        box = self.right if direction > 0 else self.left
        src = self.src.at[pl.ds(self.base + c * self.chunk, self.chunk)] if first else box.at[c]
        name = "right" if direction > 0 else "left"
        return self.remote(src, box.at[c], name, (c,), self.seat(z + direction, self.y))

    def come(self, c, direction):
        box = self.right if direction > 0 else self.left
        return self.remote(box.at[c], box.at[c], "right" if direction > 0 else "left", (c,), self.seq)

    def chain_start(self):
        @pl.when(self.z == 0)
        def _():
            for c in (3, 2, 1):
                self.pass_on(c, 0, 1, True).start()

        @pl.when(self.z == 3)
        def _():
            for c in (0, 1, 2):
                self.pass_on(c, 3, -1, True).start()

    def chain_hop(self, h):
        for z, direction, last in ((h, 1, 3), (3 - h, -1, 0)):
            box = self.right if direction > 0 else self.left

            @pl.when(self.z == z)
            def _(z=z, direction=direction, last=last, box=box):
                for c in range(last, z - direction, -direction):
                    self.come(c, direction).wait_recv()
                    if c != z:
                        add_rows((box.at[c], 0), [(box.at[c], 0), (self.src, self.base + c * self.chunk)], self.chunk)
                        self.pass_on(c, z, direction, False).start()

    def chain_end(self, seats):
        for z in seats:
            @pl.when(self.z == z)
            def _(z=z):
                terms = [(self.src, self.base + z * self.chunk)]
                if z > 0:
                    terms.append((self.right.at[z], 0))
                if z < LINE - 1:
                    terms.append((self.left.at[z], 0))
                add_rows((self.final if self.y_first else self.total, 0), terms, self.chunk)
                self.chain_done()

    def chain_done(self):
        if self.y_first:
            self.keep().start()
            self.spread_start()
            for d in range(1, self.lines):
                self.share(0, d).start()
        else:
            self.swaps()

    def place(self, z):
        first = self.y * self.part if self.y_first else 0
        return self.dst.at[pl.ds(self.start + first + z * self.chunk, self.chunk)]

    def keep(self):
        return pltpu.make_async_copy(self.final, self.place(self.z), self.sems["keep"].at[self.index])

    def spread(self, direction, h):
        src = self.final if h == 1 else self.place(self.z - direction * (h - 1))
        slot = h if direction > 0 else LINE - 1 + h
        device = self.seat(self.z + direction, self.y)
        return self.remote(src, self.place(self.z - direction * (h - 1)), "spread", (slot,), device)

    def spread_from(self, direction, h):
        slot = h if direction > 0 else LINE - 1 + h
        there = self.place(self.z - direction * h)
        return self.remote(there, there, "spread", (slot,), self.seq)

    def goes(self, direction):
        return self.z < LINE - 1 if direction > 0 else self.z > 0

    def comes(self, direction, h):
        return self.z >= h if direction > 0 else self.z < LINE - h

    def spread_start(self):
        for direction in (1, -1):
            @pl.when(self.goes(direction))
            def _(direction=direction):
                self.spread(direction, 1).start()

    def spread_hop(self, h):
        for direction in (1, -1):
            @pl.when(self.comes(direction, h))
            def _(direction=direction):
                self.spread_from(direction, h).wait_recv()
                if h < LINE - 1:
                    @pl.when(self.goes(direction))
                    def _():
                        self.spread(direction, h + 1).start()

                if self.y_first:
                    for d in range(1, self.lines):
                        self.share(h if direction > 0 else LINE - 1 + h, d).start()

    def share(self, slot, d):
        to = self.seat(self.z, self.peer_y(d))
        if self.y_first:
            if slot == 0:
                src, there = self.final, self.place(self.z)
            else:
                z = self.z - slot if slot < LINE else self.z + (slot - LINE + 1)
                src = there = self.place(z)
        else:
            src = there = self.final.at[pl.ds(self.y * self.piece, self.piece)]
        return self.remote(src, there, "share", (slot, d - 1), to)

    def share_all(self):
        for d in range(1, self.lines):
            self.share(0, d).start()

    def shared(self):
        for d in range(1, self.lines):
            self.share(0, d).wait_recv()
        self.keep().start()
        self.spread_start()

    def stages(self, make):
        def enter():
            make()
            if self.y_first:
                self.swaps()
            else:
                self.chain_start()

        def joined():
            self.join_y()
            self.chain_start()

        def second():
            self.chain_hop(2)
            self.chain_end((1, 2))

        def third():
            self.chain_hop(3)
            self.chain_end((0, 3))

        def turn():
            self.join_y()
            self.share_all()

        hops = [functools.partial(self.spread_hop, h) for h in range(1, LINE)]
        chain = [functools.partial(self.chain_hop, 1), second, third]
        if self.mode == 1:
            return [enter, self.join_y]
        if self.mode == 2:
            return [self.chain_start] + chain + hops
        if self.y_first:
            return [enter, joined] + chain + hops
        return [enter] + chain + [turn, self.shared] + hops

    def close_chain(self):
        for h in range(1, LINE):
            for direction in (1, -1):
                @pl.when(self.z == (h - 1 if direction > 0 else LINE - h))
                def _(h=h, direction=direction):
                    z = h - 1 if direction > 0 else LINE - h
                    last = LINE - 1 if direction > 0 else 0
                    for c in range(last, z, -direction):
                        self.pass_on(c, z, direction, h == 1).wait_send()

    def arrived(self):
        if not self.y_first:
            return
        for d in range(1, self.lines):
            self.share(0, d).wait_recv()
        for h in range(1, LINE):
            for direction in (1, -1):
                @pl.when(self.comes(direction, h))
                def _(h=h, direction=direction):
                    for d in range(1, self.lines):
                        self.share(h if direction > 0 else LINE - 1 + h, d).wait_recv()

    def close(self, kept=False):
        if self.mode < 2:
            for d in range(1, self.lines):
                self.swap(d).wait_send()
        if self.mode == 1:
            return
        self.close_chain()
        if not kept:
            self.keep().wait()
            self.arrived()
        for d in range(1, self.lines):
            self.share(0, d).wait_send()
        for h in range(1, LINE):
            for direction in (1, -1):
                there = self.comes(direction, h - 1) if h > 1 else True

                @pl.when(jnp.logical_and(there, self.goes(direction)))
                def _(h=h, direction=direction):
                    self.spread(direction, h).wait_send()

                if self.y_first:
                    @pl.when(self.comes(direction, h))
                    def _(h=h, direction=direction):
                        for d in range(1, self.lines):
                            self.share(h if direction > 0 else LINE - 1 + h, d).wait_send()


def job_scratch(jobs, widths, lines, gathered=0, swaps=False):
    dma, groups = pltpu.SemaphoreType.DMA, [[] for _ in range(5)]
    for j, (which, start, rows, y_first) in enumerate(jobs):
        part, piece = rows // lines, rows // lines // LINE
        chunk = piece if y_first else rows // LINE
        sizes = (
            (lines - 1, part if y_first else piece), (LINE, chunk), (LINE, chunk),
            (8 if y_first else chunk,), (chunk,),
        )
        if j < gathered:
            sizes = ((1, 8),) + sizes[1:]
        if swaps:
            sizes = sizes[:1] + ((1, 8), (1, 8), (8,), (8,))
        for group, size in zip(groups, sizes):
            group.append(pltpu.VMEM(size + (widths[which],), BF16))
    scratch = [one for group in groups for one in group]
    for slots in ((lines - 1,), (LINE,), (LINE,), (2 * LINE - 1,), (2 * LINE - 1, lines - 1)):
        scratch += [dma((len(jobs),) + slots)] * 2
    return scratch


def rows_of(plan, heights):
    jobs = []
    for which, number, parts, y_first in plan:
        rows = heights[which] // parts
        jobs.append((which, number * rows, rows, y_first))
    return jobs


def mm(left, right, contract=((1,), (0,)), precision=None):
    return lax.dot_general(
        left, right, (contract, ((), ())), precision=precision, preferred_element_type=F32
    )


def split(value):
    high = value.astype(BF16)
    return high, (value - high.astype(F32)).astype(BF16)


def twice(value, axis):
    return jnp.concatenate([value, value], axis=axis)


def sigmoid(v):
    return 1.0 / (1.0 + jnp.exp(-v))


def mixer_kernel(
    count, peers_head, inner, jobs, waves,
    lengths, hidden_in, cot_in, gate_w, value_w, state_w, out_w, step_w,
    taps_v, taps_s, gain_in, off_v_in, gain_mix_in, off_s_in, bias_own, rate_own, skip_own,
    normed_out, scale_in, hidden_out, cot_out, gain_full, mix_out_out, d_gate_out, d_value, d_state, d_step,
    grads_v, grads_s, grads_h, *refs,
):
    finals, refs = refs[: len(jobs)], refs[len(jobs) :]
    (
    normed, hidden, cot, mix_out, d_gate, out_sem, v_in, s_in, g_in, t_in, d_mix, gate_m, value_m, state_m, out_m, step_m, off_v, gain, off_s, bias_in, rate_in, skip_in, gain_own, bias, rate, skip,
    edge_v, edge_s, first_v, first_s, val, inf, inf_low, rea, rea_low, slope_v, slope_s, segs, mask_f, mask_b,
    step, sig, logs, run, run_t, tail, into, passing, pair, scaled, scaled_low, out, inter, d_u,
    states, starts, starts_low, before, total, factors, push, got, kept, prefix, spread_sum,
    rows_out, rows_in, pre_v, pre_s, back_v, back_s, back_in_v, back_in_s,
    local_sem, gather_send, gather_recv, edge_sems, p_send, p_recv, carry_send, carry_recv, row_send, row_recv, back_sems, parts_out, parts_gate,
    ) = refs[:86]
    rest = refs[86:]
    tokens, channels = v_in.shape
    chunks, pairs, heads = tokens // Q, channels // LANES, channels // HEAD
    seq, head = lax.axis_index("seq"), lax.axis_index("head")
    window = count // 2
    steps = []
    width = window // 2
    while width >= 2:
        steps.append(width)
        width //= 2

    def remote(src, dst, send, recv, device):
        return pltpu.make_async_remote_copy(
            src_ref=src, dst_ref=dst, send_sem=send, recv_sem=recv, device_id=device, device_id_type=MESH
        )

    lines, held_jobs = count // LINE, len(jobs)
    z, y = seq // lines, lax.rem(seq, lines)
    pairs_of = rest[5 * held_jobs :]
    sems = {
        name: (pairs_of[2 * k], pairs_of[2 * k + 1])
        for k, name in enumerate(("swap", "right", "left", "spread", "share"))
    }
    work = [
        Job(j, y_first, (None, parts_out, parts_gate)[which], None, start, rows, lines,
            *(rest[k * held_jobs + j] for k in range(4)), finals[j], sems, (seq, z, y), 1)
        for j, (which, start, rows, y_first) in enumerate(jobs)
    ]

    def make(j):
        which, start, rows, y_first = jobs[j]
        if which == 1:
            return lambda: outer(mix_out, [cot.at[h] for h in range(peers_head)], parts_out, start, rows)
        return lambda: outer(normed, [d_gate], parts_gate, start, rows)

    plans = [job.stages(make(job.index)) for job in work]
    turns = list(waves)

    def wave():
        if turns:
            for j, stage in turns.pop(0):
                plans[j][stage]()

    barrier = pltpu.get_barrier_semaphore()
    others = [{"seq": lax.rem(seq + d, count)} for d in range(1, count)]
    others += [{"head": lax.rem(head + d, peers_head)} for d in range(1, peers_head)]
    for other in others:
        pl.semaphore_signal(barrier, inc=1, device_id=other, device_id_type=MESH)
    pl.semaphore_wait(barrier, len(others))

    def edge_copies():
        there = {"seq": lax.rem(seq + 1, count)}
        return [
            remote(v_in.at[pl.ds(tokens - SUB, SUB)], edge_v, edge_sems.at[0], edge_sems.at[1], there),
            remote(s_in.at[pl.ds(tokens - SUB, SUB)], edge_s, edge_sems.at[2], edge_sems.at[3], there),
        ]

    chips = peers_head // 2
    x, core = head // 2, lax.rem(head, 2)
    gain_own[...] = jnp.broadcast_to(gain_in[...].astype(F32).reshape(1, -1), gain_own.shape)
    sources, boxes = (hidden_in, gain_own, cot_in), (hidden, gain_full, cot)

    def gather(k, slot):
        mine, src = head, sources[k]
        if slot == 0 or slot >= chips:
            device = x * 2 + (1 - core)
        else:
            device = lax.rem(x + slot, chips) * 2 + core
        if slot >= chips:
            mine = lax.rem(x + 2 * chips - 1 - slot, chips) * 2 + core
            src = boxes[k].at[mine]
        return remote(
            src, boxes[k].at[mine], gather_send.at[k, slot], gather_recv.at[k, slot], {"head": device}
        )

    def gather_start(k):
        for slot in range(1, chips):
            gather(k, slot).start()
        gather(k, 0).start()

    def gather_forward(k):
        for slot in range(1, chips):
            gather(k, slot).wait_recv()
            gather(k, chips - 1 + slot).start()

    def gather_end(k):
        own[k].wait()
        gather(k, 0).wait_recv()
        for slot in range(chips, 2 * chips - 1):
            gather(k, slot).wait_recv()

    weights = [
        pltpu.make_async_copy(src, dst, local_sem.at[n])
        for n, (src, dst) in enumerate(
            (
                (value_w, value_m), (state_w, state_m), (step_w, step_m), (gate_w, gate_m), (out_w, out_m),
                (off_v_in, off_v.at[0]), (gain_mix_in, gain.at[0]), (off_s_in, off_s.at[0]),
                (bias_own, bias_in.at[0]), (rate_own, rate_in.at[0]), (skip_own, skip_in.at[0]),
            )
        )
    ]
    own = [
        pltpu.make_async_copy(sources[k], boxes[k].at[head], local_sem.at[len(weights) + k]) for k in range(3)
    ]
    gather_start(0)
    gather_start(1)
    for copy in own[:2] + weights:
        copy.start()
    gather_start(2)
    own[2].start()

    lane = lax.broadcasted_iota(jnp.int32, (Q, LANES), 1)
    row = lax.broadcasted_iota(jnp.int32, (Q, LANES), 0)
    left = lane < HEAD

    anchor = seq * tokens
    bounds, bound = [], 0
    for k in range(lengths.shape[0]):
        bound = bound + lengths[k]
        bounds.append(bound)

    def sequence(places):
        number = jnp.zeros(places.shape, F32)
        for bound in bounds:
            number = number + jnp.where(places >= bound, 1.0, 0.0)
        return number

    places = lax.broadcasted_iota(jnp.int32, (tokens + 2 * SUB, LANES), 0) + (anchor - SUB)
    segs[...] = sequence(places)
    for k in range(3):
        same = segs[pl.ds(SUB, tokens)] == segs[pl.ds(SUB - 3 + k, tokens)]
        mask_f[k] = jnp.where(same, 1.0, 0.0)
        same = segs[pl.ds(0, tokens + SUB)] == segs[pl.ds(3 - k, tokens + SUB)]
        mask_b[k] = jnp.where(same, 1.0, 0.0)
    head_of = lax.broadcasted_iota(jnp.int32, (channels, LANES), 0) // HEAD
    column = lax.broadcasted_iota(jnp.int32, (channels, LANES), 1)
    spread_sum[...] = jnp.where(head_of == column, 1.0, 0.0).astype(BF16)
    grads_v[...] = jnp.zeros_like(grads_v)
    grads_s[...] = jnp.zeros_like(grads_s)

    for copy in weights[5:]:
        copy.wait()
    bias[...] = jnp.zeros_like(bias)
    rate[...] = jnp.zeros_like(rate)
    bias[:, 0:heads] = bias_in[...]
    rate[:, 0:heads] = rate_in[...]
    t_in[...] = jnp.zeros_like(t_in)
    for p in range(pairs):
        skip[:, pl.ds(p * LANES, LANES)] = jnp.where(
            left[:1], skip_in[:, 2 * p : 2 * p + 1], skip_in[:, 2 * p + 1 : 2 * p + 2]
        )

    leave = [
        pltpu.make_async_copy(src, dst, out_sem.at[n])
        for n, (src, dst) in enumerate(
            (
                (normed, normed_out), (hidden, hidden_out), (cot, cot_out), (mix_out, mix_out_out),
                (d_gate, d_gate_out),
            )
        )
    ]

    gather_forward(0)
    gather_forward(1)
    gather_end(0)
    gather_end(1)
    width = hidden_in.shape[1]

    @pl.loop(0, chunks)
    def _(c):
        here = pl.ds(pl.multiple_of(c * Q, Q), Q)
        squares = jnp.zeros((Q, 1), F32)
        for h in range(peers_head):
            rows = hidden[h, here].astype(F32)
            squares = squares + jnp.sum(rows * rows, axis=1, keepdims=True)
        scale = lax.rsqrt(squares / (width * peers_head) + EPS)
        scale_in[here] = scale
        for h in range(peers_head):
            rows = hidden[h, here].astype(F32)
            normed[here, pl.ds(h * width, width)] = (rows * scale * gain_full[h, 0:1]).astype(BF16)

    for copy in leave[:2]:
        copy.start()

    def project(weight, target):
        columns = weight.shape[1]
        tile = next(t for t in (256, 128, columns) if columns % t == 0)

        @pl.loop(0, columns // tile)
        def _(n):
            lanes = pl.ds(pl.multiple_of(n * tile, tile), tile)
            target[:, lanes] = mm(normed[...], weight[:, lanes])

    for copy in weights[:2]:
        copy.wait()
    project(value_m, v_in)
    project(state_m, s_in)

    @pl.when(seq < count - 1)
    def _():
        for copy in edge_copies():
            copy.start()

    weights[2].wait()
    t_in[:, 0:heads] = mm(normed[...], step_m[...], ((1,), (1,)))
    weights[3].wait()
    project(gate_m, g_in)
    gather_forward(2)

    raw = t_in[...] + bias[...]
    step[...] = jnp.maximum(raw, 0.0) + jnp.log1p(jnp.exp(-jnp.abs(raw)))
    sig[...] = sigmoid(raw)
    logs[...] = -jnp.exp(rate[...]) * step[...]
    lower = jnp.where(row >= lane, 1.0, 0.0)

    @pl.loop(0, chunks)
    def _(c):
        here = pl.ds(pl.multiple_of(c * Q, Q), Q)
        run[here] = mm(lower, logs[here], precision=HIGH)
        summed = run[here]
        run_t[c] = summed.T[:16]
        last = run[pl.ds(c * Q + Q - 1, 1)]
        mine = segs[pl.ds(pl.multiple_of(c * Q + SUB, SUB), Q)]
        at_end = segs[pl.ds(c * Q + SUB + Q - 1, 1)]
        entering = segs[pl.ds(c * Q + SUB - 1, 1)]
        tail[here] = jnp.exp(last - summed) * jnp.where(mine == at_end, 1.0, 0.0)
        into[here] = jnp.exp(summed) * jnp.where(mine == entering, 1.0, 0.0)
        through = jnp.exp(last) * jnp.where(at_end == entering, 1.0, 0.0)
        passing[c] = jnp.broadcast_to(through, (Q, LANES)).T[:16]

    product = jnp.ones((16, LANES), F32)
    for c in range(chunks):
        before[c] = product
        product = product * passing[c]
    factors[seq] = product

    def factor_copies():
        return [
            remote(
                factors.at[seq], factors.at[seq], p_send.at[d - 1], p_recv.at[d - 1],
                {"seq": lax.rem(seq + d, count)},
            )
            for d in range(1, count)
        ]

    for copy in factor_copies():
        copy.start()

    def convolve(source, base, rows, lanes, taps, offset):
        begin, size = rows
        summed = offset[:, lanes] + taps[3:4, lanes] * source[pl.ds(base, size), lanes]
        for k in range(3):
            term = taps[k : k + 1, lanes] * source[pl.ds(base - 3 + k, size), lanes]
            summed = summed + term * mask_f[k, pl.ds(begin, size)]
        s = sigmoid(summed)
        return summed * s, s * (1.0 + summed * (1.0 - s))

    def convolve_rows(c):
        rows = (c * Q, Q)
        span = pl.ds(c * Q, Q)

        @pl.loop(0, pairs)
        def _(b):
            lanes = pl.ds(pl.multiple_of(b * LANES, LANES), LANES)
            source, base = (v_in, c * Q) if c else (first_v, SUB)
            val[span, lanes], slope_v[span, lanes] = convolve(source, base, rows, lanes, taps_v, off_v)

        for b, (target, low) in enumerate(((inf, inf_low), (rea, rea_low))):
            lanes = pl.ds(b * LANES, LANES)
            source, base = (s_in, c * Q) if c else (first_s, SUB)
            active, slope_s[span, lanes] = convolve(source, base, rows, lanes, taps_s, off_s)
            target[span], low[span] = split(active)

    for c in range(1, chunks):
        convolve_rows(c)

    @pl.when(seq > 0)
    def _():
        for copy in edge_copies():
            copy.wait_recv()

    @pl.when(seq == 0)
    def _():
        edge_v[...] = jnp.zeros_like(edge_v)
        edge_s[...] = jnp.zeros_like(edge_s)

    first_v[pl.ds(0, SUB)] = edge_v[...]
    first_s[pl.ds(0, SUB)] = edge_s[...]
    first_v[pl.ds(SUB, Q)] = v_in[pl.ds(0, Q)]
    first_s[pl.ds(SUB, Q)] = s_in[pl.ds(0, Q)]
    convolve_rows(0)

    def both(ref, here, p):
        return jnp.where(left, ref[here, 2 * p : 2 * p + 1], ref[here, 2 * p + 1 : 2 * p + 2])

    def halves_split(value):
        return split(jnp.concatenate([jnp.where(left, value, 0.0), jnp.where(left, 0.0, value)], axis=0))

    @pl.loop(0, chunks)
    def _(c):
        here = pl.ds(pl.multiple_of(c * Q, Q), Q)
        for p in range(pairs):
            lanes = pl.ds(p * LANES, LANES)
            weighted = both(step, here, p) * val[here, lanes]
            scaled[here, lanes], scaled_low[here, lanes] = split(both(tail, here, p) * weighted)
        states[c] = mm(
            twice(scaled[here], 0), jnp.concatenate([inf[here], inf_low[here]], axis=0), ((0,), (0,))
        )

    def pass_chunks(h):
        rows = pl.ds(h * HEAD, HEAD)
        held = jnp.zeros((HEAD, LANES), F32)
        for c in range(chunks):
            added = states[c, rows]
            states[c, rows] = held
            held = passing[c, h : h + 1] * held + added
        total[rows] = held

    share = channels // 2
    heads_of = (range(heads // 2), range(heads // 2, heads))

    def carry(direction):
        bank = 0 if direction == 1 else 1

        def reach(d):
            there = seq + direction * d
            return jnp.logical_and(there >= 0, there < count)

        def heard(d):
            there = seq - direction * d
            return jnp.logical_and(there >= 0, there < count)

        def copy(slot, d, half):
            source, rows = min(slot, len(steps)), pl.ds(half * share, share)
            return remote(
                push.at[bank, source, rows], got.at[bank, slot, rows],
                carry_send.at[bank, slot, half], carry_recv.at[bank, slot, half],
                {"seq": lax.rem(seq + direction * d + count, count)},
            )

        plan = [(k, d) for k, d in enumerate(steps)]
        ends = [(len(steps), 1), (len(steps) + 1, 2)]

        def send(slot, d, half):
            @pl.when(reach(d))
            def _():
                copy(slot, d, half).start()

        def factor(first, many, h):
            product = factors[first, h : h + 1]
            for i in range(1, many):
                product = product * factors[first - direction * i, h : h + 1]
            return product

        def launch(slot, half):
            rows = pl.ds(half * share, share)
            push[bank, slot, rows] = total[rows].astype(BF16)
            if slot < len(steps):
                send(*plan[slot], half)
            else:
                for end in ends:
                    send(*end, half)

        def join(slot, half):
            d = plan[slot][1]

            @pl.when(heard(d))
            def _():
                copy(slot, d, half).wait_recv()
                for h in heads_of[half]:
                    rows = pl.ds(h * HEAD, HEAD)
                    total[rows] = total[rows] + factor(seq, d, h) * got[bank, slot, rows].astype(F32)

            launch(slot + 1, half)

        def finish(half):
            part = pl.ds(half * share, share)
            total[part] = jnp.zeros((share, LANES), F32)

            @pl.when(heard(1))
            def _():
                copy(*ends[0], half).wait_recv()
                total[part] = got[bank, ends[0][0], part].astype(F32)

            @pl.when(heard(2))
            def _():
                copy(*ends[1], half).wait_recv()
                for h in heads_of[half]:
                    rows = pl.ds(h * HEAD, HEAD)
                    far = got[bank, ends[1][0], rows].astype(F32)
                    total[rows] = total[rows] + factor(seq - direction, 1, h) * far

        def close():
            for slot, d in plan + ends:
                @pl.when(reach(d))
                def _(slot=slot, d=d):
                    for half in range(2):
                        copy(slot, d, half).wait_send()

        return launch, join, finish, close

    launch, join, finish, close_forward = carry(1)
    for half in range(2):
        for h in heads_of[half]:
            pass_chunks(h)
        launch(0, half)
    gather_end(2)
    leave[2].start()
    weights[4].wait()

    @pl.loop(0, tokens // (2 * Q))
    def _(n):
        here = pl.ds(pl.multiple_of(n * 2 * Q, 2 * Q), 2 * Q)
        result = jnp.zeros((2 * Q, channels), F32)
        for h in range(peers_head):
            result = result + mm(cot[h, here], out_m[:, pl.ds(h * width, width)], ((1,), (1,)))
        d_mix[here] = result

    def products(here):
        read = jnp.concatenate([rea[here], rea[here], rea_low[here]], axis=1)
        return mm(read, jnp.concatenate([inf[here], inf_low[here], inf[here]], axis=1), ((1,), (1,)))

    def from_state(high, low, c, lanes):
        state = jnp.concatenate([starts[c, lanes], starts_low[c, lanes], starts[c, lanes]], axis=1)
        return mm(jnp.concatenate([high, high, low], axis=1), state, ((1,), (1,)))

    def with_state(high, low, c, lanes):
        state = jnp.concatenate([starts[c, lanes], starts_low[c, lanes], starts[c, lanes]], axis=0)
        return mm(jnp.concatenate([high, high, low], axis=1), state)

    def within(c):
        here = pl.ds(pl.multiple_of(c * Q, Q), Q)
        mine = segs[pl.ds(pl.multiple_of(c * Q + SUB, SUB), Q)]
        across = sequence(lane + (anchor + c * Q))
        hidden = jnp.where(jnp.logical_and(mine == across, row >= lane), 0.0, FAR)
        cross = products(here)
        for p in range(pairs):
            lanes = pl.ds(p * LANES, LANES)
            mixing = []
            for h in (2 * p, 2 * p + 1):
                gap = (run[here, h : h + 1] - run_t[c, h : h + 1]) + hidden
                decay = jnp.exp(gap)
                pair[c * heads + h] = decay
                mixing.append(decay * cross)
            high, low = split(jnp.concatenate(mixing, axis=1))
            first, rest_of = halves_split(both(step, here, p) * val[here, lanes])
            out[here, lanes] = mm(
                jnp.concatenate([high, high, low], axis=1),
                jnp.concatenate([first, rest_of, first], axis=0),
            )

    @pl.loop(0, chunks // 2)
    def _(c):
        within(c)

    for copy in factor_copies():
        copy.wait_recv()
    for k in range(len(steps)):
        for half in range(2):
            join(k, half)

    @pl.loop(chunks // 2, chunks)
    def _(c):
        within(c)

    for h in range(heads):
        if h * 2 % heads == 0:
            finish(h * 2 // heads)
        rows = pl.ds(h * HEAD, HEAD)
        incoming = total[rows]
        for c in range(chunks):
            starts[c, rows], starts_low[c, rows] = split(
                states[c, rows] + before[c, h : h + 1] * incoming
            )

    rows_out[...] = jnp.zeros_like(rows_out)

    @pl.loop(0, chunks)
    def _(c):
        here = pl.ds(pl.multiple_of(c * Q, Q), Q)
        squares, dots = jnp.zeros((Q, LANES), F32), jnp.zeros((Q, LANES), F32)
        for p in range(pairs):
            lanes = pl.ds(p * LANES, LANES)
            reached = from_state(rea[here], rea_low[here], c, lanes)
            reached = reached * both(into, here, p)
            inter[here, lanes] = reached
            mixed = out[here, lanes] + reached + skip[:, lanes] * val[here, lanes]
            out[here, lanes] = mixed
            gate = g_in[here, lanes]
            gated = mixed * (gate * sigmoid(gate))
            squares = squares + gated * gated
            dots = dots + d_mix[here, lanes] * gain[:, lanes] * gated
        rows_out[0:1, here] = jnp.sum(squares.T, axis=0, keepdims=True)
        rows_out[1:2, here] = jnp.sum(dots.T, axis=0, keepdims=True)

    row_copies = [
        remote(
            rows_out, rows_in.at[d - 1], row_send.at[d - 1], row_recv.at[d - 1],
            {"head": lax.rem(head + d, peers_head)},
        )
        for d in range(1, peers_head)
    ]
    for copy in row_copies:
        copy.start()
    summed = rows_out[...]
    for d, copy in enumerate(row_copies):
        copy.wait_recv()
        summed = summed + rows_in[d]
    for copy in row_copies:
        copy.wait_send()
    rows_out[0:1] = lax.rsqrt(summed[0:1] / inner + EPS)
    rows_out[1:2] = summed[1:2] / inner

    @pl.loop(0, chunks)
    def _(c):
        here = pl.ds(pl.multiple_of(c * Q, Q), Q)
        scale = jnp.broadcast_to(rows_out[0:1, here], (Q, LANES)).T
        dot = jnp.broadcast_to(rows_out[1:2, here], (Q, LANES)).T
        cubed = scale * scale * scale * dot
        for p in range(pairs):
            lanes = pl.ds(p * LANES, LANES)
            gate, mixed, slope = g_in[here, lanes], out[here, lanes], d_mix[here, lanes]
            s = sigmoid(gate)
            opened = gate * s
            gated = mixed * opened
            normed = gated * scale
            mix_out[here, lanes] = (normed * gain[:, lanes]).astype(BF16)
            d_gated = scale * (slope * gain[:, lanes]) - gated * cubed
            d_mixer = d_gated * opened
            d_gate[here, lanes] = (d_gated * mixed * (s * (1.0 + gate * (1.0 - s)))).astype(BF16)
            out[here, lanes] = d_mixer
            d_u[here, lanes] = both(into, here, p) * d_mixer
            grads_v[5:6, lanes] = grads_v[5:6, lanes] + jnp.sum(slope * normed, axis=0, keepdims=True)
            grads_v[6:7, lanes] = grads_v[6:7, lanes] + jnp.sum(
                d_mixer * val[here, lanes], axis=0, keepdims=True
            )
        carried = d_u[here].astype(BF16)
        states[c] = mm(
            twice(carried, 0), jnp.concatenate([rea[here], rea_low[here]], axis=0), ((0,), (0,))
        )
        d_read = jnp.zeros((Q, LANES), F32)
        for p in range(pairs):
            lanes = pl.ds(p * LANES, LANES)
            d_read = d_read + with_state(*split(d_u[here, lanes]), c, lanes)
        pre_s[pl.ds(pl.multiple_of(c * Q + SUB, SUB), Q), pl.ds(LANES, LANES)] = d_read

    for copy in leave[3:]:
        copy.start()
    launch, join, finish, close_backward = carry(-1)
    for half in range(2):
        for h in heads_of[half]:
            rows = pl.ds(h * HEAD, HEAD)
            held = jnp.zeros((HEAD, LANES), F32)
            for c in reversed(range(chunks)):
                held = states[c, rows] + passing[c, h : h + 1] * held
            total[rows] = held
        launch(0, half)
    wave()
    upper = jnp.where(row < lane, 1.0, 0.0).astype(BF16)

    def within_back(c):
        here = pl.ds(pl.multiple_of(c * Q, Q), Q)
        padded = pl.ds(pl.multiple_of(c * Q + SUB, SUB), Q)
        cross = products(here)
        d_cross = jnp.zeros((Q, LANES), F32)
        from_inter = jnp.zeros((Q, LANES), F32)
        for p in range(pairs):
            lanes = pl.ds(p * LANES, LANES)
            weighted, weighted_low = split(both(step, here, p) * val[here, lanes])
            d_out = out[here, lanes]
            d_halves, d_low = halves_split(d_out)
            d_pair = mm(
                jnp.concatenate([d_halves, d_halves, d_low], axis=1),
                jnp.concatenate([weighted, weighted_low, weighted], axis=1),
                ((1,), (1,)),
            )
            mixing, terms = [], []
            for i, h in enumerate((2 * p, 2 * p + 1)):
                decay = pair[c * heads + h]
                shared = d_pair[i * Q : (i + 1) * Q] * decay
                d_cross = d_cross + shared
                terms.append((shared * cross).astype(BF16))
                mixing.append((decay * cross).astype(BF16))
            d_u[here, lanes] = mm(jnp.concatenate(mixing, axis=0), d_halves, ((0,), (0,)))
            ahead = mm(jnp.concatenate(terms, axis=0), upper)
            for i, h in enumerate((2 * p, 2 * p + 1)):
                crossing = jnp.where(row >= lane, ahead[i * Q : (i + 1) * Q], 0.0)
                prefix[c, h : h + 1] = jnp.sum(crossing, axis=0, keepdims=True)
            from_inter = from_inter + mm(
                (d_out * inter[here, lanes]).astype(BF16), spread_sum[lanes]
            )
        kept[0, here] = from_inter
        high, low = split(d_cross)
        pre_s[padded, pl.ds(LANES, LANES)] = pre_s[padded, pl.ds(LANES, LANES)] + mm(
            jnp.concatenate([high, high, low], axis=1),
            jnp.concatenate([inf[here], inf_low[here], inf[here]], axis=0),
        )
        pre_s[padded, pl.ds(0, LANES)] = mm(
            jnp.concatenate([high, high, low], axis=0),
            jnp.concatenate([rea[here], rea_low[here], rea[here]], axis=0),
            ((0,), (0,)),
        )

    prefix[...] = jnp.zeros_like(prefix)

    for c in range(chunks):
        if c == chunks // 2:
            for k in range(len(steps)):
                for half in range(2):
                    join(k, half)
            wave()
        within_back(c)
        wave()
    for h in range(heads):
        if h * 2 % heads == 0:
            finish(h * 2 // heads)
        rows = pl.ds(h * HEAD, HEAD)
        held = total[rows]
        for c in reversed(range(chunks)):
            start = starts[c, rows].astype(F32) + starts_low[c, rows].astype(F32)
            met = jnp.sum(held * start, axis=0, keepdims=True)
            met = jnp.sum(met, axis=1, keepdims=True) * passing[c, h : h + 1]
            prefix[c, h : h + 1] = prefix[c, h : h + 1] + met
            added = states[c, rows]
            starts[c, rows], starts_low[c, rows] = split(held)
            held = added + passing[c, h : h + 1] * held

    wave()
    from_here = jnp.where(row <= lane, 1.0, 0.0)
    under = jnp.where(row > lane, 1.0, 0.0)
    rates = -jnp.exp(rate[...])
    grads_h[...] = jnp.zeros_like(grads_h)
    pre_v[pl.ds(0, SUB)] = jnp.zeros((SUB, channels), F32)
    pre_v[pl.ds(tokens + SUB, SUB)] = jnp.zeros((SUB, channels), F32)
    pre_s[pl.ds(0, SUB)] = jnp.zeros((SUB, 2 * LANES), F32)
    pre_s[pl.ds(tokens + SUB, SUB)] = jnp.zeros((SUB, 2 * LANES), F32)

    @pl.loop(0, chunks)
    def _(c):
        here = pl.ds(pl.multiple_of(c * Q, Q), Q)
        padded = pl.ds(pl.multiple_of(c * Q + SUB, SUB), Q)
        from_tail, from_step = jnp.zeros((Q, LANES), F32), jnp.zeros((Q, LANES), F32)
        d_in = jnp.zeros((Q, LANES), F32)
        for p in range(pairs):
            lanes = pl.ds(p * LANES, LANES)
            sizes = both(step, here, p)
            value = val[here, lanes]
            d_tail = from_state(inf[here], inf_low[here], c, lanes)
            d_tail = d_tail * both(tail, here, p)
            d_weighted = d_u[here, lanes] + d_tail
            from_tail = from_tail + mm((sizes * value * d_tail).astype(BF16), spread_sum[lanes])
            from_step = from_step + mm((value * d_weighted).astype(BF16), spread_sum[lanes])
            d_val = sizes * d_weighted + skip[:, lanes] * out[here, lanes]
            pre_v[padded, lanes] = d_val * slope_v[here, lanes]
            d_in = d_in + with_state(scaled[here, lanes], scaled_low[here, lanes], c, lanes)
        inflow, readout = pl.ds(0, LANES), pl.ds(LANES, LANES)
        pre_s[padded, inflow] = (pre_s[padded, inflow] + d_in) * slope_s[here, inflow]
        pre_s[padded, readout] = pre_s[padded, readout] * slope_s[here, readout]
        d_log = mm(from_here, kept[0, here], precision=HIGH) + mm(under, from_tail, precision=HIGH)
        filled = jnp.concatenate([prefix[c], jnp.zeros((Q - 16, LANES), F32)], axis=0)
        d_log = d_log + filled.T
        d_size = (from_step + rates * d_log) * sig[here]
        d_step[here] = d_size.astype(BF16)
        grads_h[0:1] = grads_h[0:1] + jnp.sum(d_size, axis=0, keepdims=True)
        grads_h[1:2] = grads_h[1:2] + jnp.sum(d_log * logs[here], axis=0, keepdims=True)

    wave()

    def back(source, base, size, lanes, taps):
        summed = taps[3:4, lanes] * source[pl.ds(base, size), lanes]
        for k in range(3):
            term = taps[k : k + 1, lanes] * source[pl.ds(base + 3 - k, size), lanes]
            summed = summed + term * mask_b[k, pl.ds(base, size)]
        return summed

    def back_copies():
        there = {"seq": lax.rem(seq + count - 1, count)}
        return [
            remote(back_v, back_in_v, back_sems.at[0], back_sems.at[1], there),
            remote(back_s, back_in_s, back_sems.at[2], back_sems.at[3], there),
        ]

    for b in range(pairs):
        lanes = pl.ds(b * LANES, LANES)
        back_v[:, lanes] = back(pre_v, 0, SUB, lanes, taps_v)
    for b in range(2):
        lanes = pl.ds(b * LANES, LANES)
        back_s[:, lanes] = back(pre_s, 0, SUB, lanes, taps_s)

    @pl.when(seq > 0)
    def _():
        for copy in back_copies():
            copy.start()

    def filter_grads(pre, source, base, c, lanes, grads):
        rows = pl.ds(c * Q + SUB, Q)
        slope = pre[rows, lanes]
        for k in range(3):
            term = slope * mask_f[k, pl.ds(c * Q, Q)] * source[pl.ds(base - 3 + k, Q), lanes]
            grads[k : k + 1, lanes] = grads[k : k + 1, lanes] + jnp.sum(term, axis=0, keepdims=True)
        term = slope * source[pl.ds(base, Q), lanes]
        grads[3:4, lanes] = grads[3:4, lanes] + jnp.sum(term, axis=0, keepdims=True)
        grads[4:5, lanes] = grads[4:5, lanes] + jnp.sum(slope, axis=0, keepdims=True)

    for c in range(chunks):
        if c == chunks - 1:
            @pl.when(seq < count - 1)
            def _():
                for copy in back_copies():
                    copy.wait_recv()

            @pl.when(seq == count - 1)
            def _():
                back_in_v[...] = jnp.zeros_like(back_in_v)
                back_in_s[...] = jnp.zeros_like(back_in_s)

        def one(pre, source, base, c, lanes, taps, grads, target, received):
            result = back(pre, c * Q + SUB, Q, lanes, taps)
            if c == chunks - 1:
                result = jnp.concatenate(
                    [result[: Q - SUB], result[Q - SUB :] + received[:, lanes]], axis=0
                )
            target[pl.ds(c * Q, Q), lanes] = result.astype(BF16)
            filter_grads(pre, source, base, c, lanes, grads)

        @pl.loop(0, pairs)
        def _(b, c=c):
            lanes = pl.ds(pl.multiple_of(b * LANES, LANES), LANES)
            source, base = (v_in, c * Q) if c else (first_v, SUB)
            one(pre_v, source, base, c, lanes, taps_v, grads_v, d_value, back_in_v)

        wave()
        for b in range(2):
            lanes = pl.ds(b * LANES, LANES)
            source, base = (s_in, c * Q) if c else (first_s, SUB)
            one(pre_s, source, base, c, lanes, taps_s, grads_s, d_state, back_in_s)

    @pl.when(seq < count - 1)
    def _():
        for copy in edge_copies():
            copy.wait_send()

    @pl.when(seq > 0)
    def _():
        for copy in back_copies():
            copy.wait_send()

    while turns:
        wave()
    for copy in leave:
        copy.wait()
    for job in work:
        job.close()
    for k in range(3):
        for slot in range(2 * chips - 1):
            gather(k, slot).wait_send()
    for copy in factor_copies():
        copy.wait_send()
    close_forward()
    close_backward()


def mix(count, peers_head, lengths, hidden, cot, weights, filters, gain, vectors, plan, waves, collective_id):
    tokens, width = hidden.shape
    channels = weights[0].shape[1]
    chunks, heads, inner = tokens // Q, channels // HEAD, channels * peers_head
    chips = peers_head // 2
    slots = 1
    reach = count // 4
    while reach >= 2:
        slots += 1
        reach //= 2
    vmem, dma = pltpu.VMEM, pltpu.SemaphoreType.DMA
    shape = jax.ShapeDtypeStruct
    outs = [
        shape((tokens, width * peers_head), BF16), shape((tokens, 1), F32),
        shape((peers_head, tokens, width), BF16), shape((peers_head, tokens, width), BF16),
        shape((peers_head, 8, width), F32),
        shape((tokens, channels), BF16), shape((tokens, channels), BF16),
        shape((tokens, channels), BF16), shape((tokens, 2 * LANES), BF16),
        shape((tokens, LANES), BF16),
        shape((8, channels), F32), shape((8, 2 * LANES), F32), shape((8, LANES), F32),
    ]
    features = width * peers_head
    jobs = rows_of(plan, (0, channels, features))
    for which, start, rows, y_first in jobs:
        outs.append(shape((rows // (count // LINE), (0, features, channels)[which]), BF16))
    wide, narrow = (tokens, channels), (tokens, LANES)
    early = (0, 2, 3, 5, 6)
    scratch = [vmem(outs[k].shape, BF16) for k in early] + [dma((5,))]
    scratch += [
        vmem(wide, F32), vmem((tokens, 2 * LANES), F32), vmem(wide, F32), vmem(narrow, F32), vmem(wide, F32),
    ]
    scratch += [vmem(weight.shape, BF16) for weight in weights]
    scratch += [vmem((1,) + vector.shape, F32) for vector in vectors]
    scratch += [
        vmem((8, width), F32), vmem((1, LANES), F32), vmem((1, LANES), F32), vmem((1, channels), F32),
        vmem((SUB, channels), F32), vmem((SUB, 2 * LANES), F32),
        vmem((Q + SUB, channels), F32), vmem((Q + SUB, 2 * LANES), F32),
        vmem(wide, F32), vmem(narrow, BF16), vmem(narrow, BF16), vmem(narrow, BF16), vmem(narrow, BF16),
        vmem(wide, F32), vmem((tokens, 2 * LANES), F32),
        vmem((tokens + 2 * SUB, LANES), F32),
        vmem((3, tokens, LANES), F32), vmem((3, tokens + SUB, LANES), F32),
        vmem(narrow, F32), vmem(narrow, F32), vmem(narrow, F32), vmem(narrow, F32),
        vmem((chunks, 16, LANES), F32), vmem(narrow, F32), vmem(narrow, F32),
        vmem((chunks, 16, LANES), F32),
        vmem((chunks * heads, Q, LANES), F32), vmem(wide, BF16), vmem(wide, BF16),
        vmem(wide, F32), vmem(wide, F32), vmem(wide, F32),
        vmem((chunks, channels, LANES), F32),
        vmem((chunks, channels, LANES), BF16), vmem((chunks, channels, LANES), BF16),
        vmem((chunks, 16, LANES), F32), vmem((channels, LANES), F32),
        vmem((count, 16, LANES), F32),
        vmem((2, slots, channels, LANES), BF16), vmem((2, slots + 1, channels, LANES), BF16),
        vmem((1, tokens, LANES), F32), vmem((chunks, 16, LANES), F32),
        vmem((channels, LANES), BF16),
        vmem((8, tokens), F32), vmem((peers_head - 1, 8, tokens), F32),
        vmem((tokens + 2 * SUB, channels), F32), vmem((tokens + 2 * SUB, 2 * LANES), F32),
        vmem((SUB, channels), F32), vmem((SUB, 2 * LANES), F32),
        vmem((SUB, channels), F32), vmem((SUB, 2 * LANES), F32),
        dma((14,)), dma((3, 2 * chips - 1)), dma((3, 2 * chips - 1)),
        dma((4,)), dma((count - 1,)), dma((count - 1,)),
        dma((2, slots + 1, 2)), dma((2, slots + 1, 2)),
        dma((peers_head - 1,)), dma((peers_head - 1,)), dma((4,)),
        vmem((channels, features), BF16),
        vmem((max([start + rows for which, start, rows, _ in jobs if which == 2] + [8]), channels), BF16),
    ]
    scratch += job_scratch(jobs, (0, features, channels), count // LINE, 0, True)
    inside, anywhere = pl.BlockSpec(memory_space=pltpu.VMEM), pl.BlockSpec(memory_space=pl.ANY)
    return pl.pallas_call(
        functools.partial(mixer_kernel, count, peers_head, inner, jobs, waves),
        out_shape=outs,
        in_specs=[pl.BlockSpec(memory_space=pltpu.SMEM)]
        + [anywhere] * 7 + [inside] * 3 + [anywhere] * len(vectors),
        out_specs=[anywhere if k in early else inside for k in range(len(outs))],
        scratch_shapes=scratch,
        compiler_params=pltpu.CompilerParams(
            collective_id=collective_id, has_side_effects=True, vmem_limit_bytes=61 * 1024 * 1024
        ),
    )(lengths, hidden, cot, *weights, *filters, gain, *vectors)


def sum_rows(jobs, order, lines, peers_head, early, *refs):
    (scale, gain, grads_v, grads_s, grads_h, normed_in_, cot_in, hidden_in, mix_out_in, d_gate_in, d_value_in,
     d_state_in, d_step_in, gate_w, value_w, out_w, state_w, step_w) = refs[:18]
    given, refs = refs[18 : 18 + early], refs[18 + early :]
    outs, (every, normed_sum, mixed_sum, dots_sum) = refs[:4], refs[4:8]
    scratch = refs[8:]
    count = len(jobs)
    y_in, right, left, total, final = (scratch[k * count : (k + 1) * count] for k in range(5))
    names = ("swap", "right", "left", "spread", "share")
    pairs = scratch[5 * count : 5 * count + 10]
    sems = {name: (pairs[2 * k], pairs[2 * k + 1]) for k, name in enumerate(names)}
    (sems["keep"], packed, out_part, gate_part, value_part, gate_m, value_m, out_m, state_m, step_m,
     blocks, block_in, normed_part, normed_in, mixed_part, mixed_in, dots, dots_in, gain_part, rest, product,
     local_sem, hs, hr, normed, cot, hidden, mix_out, d_gate, d_value, d_state, d_step) = scratch[5 * count + 10 :]
    parts = [packed, out_part, gate_part, value_part]
    tokens, features = normed.shape
    width, channels = features // peers_head, d_gate.shape[1]
    heads = channels // HEAD
    seq, head = lax.axis_index("seq"), lax.axis_index("head")
    z, y = seq // lines, lax.rem(seq, lines)
    work = [
        Job(j, y_first, given[j] if j < early else parts[which], outs[which], start, rows, lines,
            y_in[j], right[j], left[j], total[j], final[j], sems, (seq, z, y), 2 if j < early else 0)
        for j, (which, start, rows, y_first) in enumerate(jobs)
    ]
    shared = [j for j in range(count) if not jobs[j][0]][0]

    loads = [
        pltpu.make_async_copy(src, dst, local_sem.at[k])
        for k, (src, dst) in enumerate(
            ((gate_w, gate_m), (value_w, value_m), (out_w, out_m), (state_w, state_m), (step_w, step_m))
        )
    ]
    operands = {
        name: pltpu.make_async_copy(src, dst, local_sem.at[5 + n])
        for n, (name, src, dst) in enumerate(
            (
                ("mix_out", mix_out_in, mix_out), ("cot", cot_in, cot), ("normed", normed_in_, normed),
                ("d_gate", d_gate_in, d_gate), ("d_value", d_value_in, d_value), ("d_state", d_state_in, d_state),
                ("d_step", d_step_in, d_step), ("hidden", hidden_in, hidden),
            )
        )
    }
    for copy in list(operands.values()) + loads:
        copy.start()

    def need(*names):
        for name in names:
            if name in operands:
                operands.pop(name).wait()

    barrier = pltpu.get_barrier_semaphore()
    peers = [{"seq": z * lines + lax.rem(y + d, lines)} for d in range(1, lines)]
    peers += [{"head": lax.rem(head + d, peers_head)} for d in range(1, peers_head)]
    for peer in peers:
        pl.semaphore_signal(barrier, inc=1, device_id=peer, device_id_type=MESH)
    for direction in (1, -1):
        @pl.when(z < LINE - 1 if direction > 0 else z > 0)
        def _(direction=direction):
            pl.semaphore_signal(
                barrier, inc=1, device_id={"seq": (z + direction) * lines + y}, device_id_type=MESH
            )

    ends = jnp.logical_or(z == 0, z == LINE - 1)

    @pl.when(ends)
    def _():
        pl.semaphore_wait(barrier, len(peers) + 1)

    @pl.when(jnp.logical_not(ends))
    def _():
        pl.semaphore_wait(barrier, len(peers) + 2)

    block = blocks.shape[1]

    def head_copies(kind):
        for d in range(1, peers_head):
            to = lax.rem(head + d, peers_head)
            if kind < 4:
                src = (blocks.at[to], dots, normed_part.at[to], mixed_part.at[to])[kind]
                dst = (block_in, dots_in, normed_in, mixed_in)[kind].at[d - 1]
            else:
                src, dst = outs[0].at[pl.ds(0, width)], every.at[head]
            yield pltpu.make_async_remote_copy(
                src_ref=src, dst_ref=dst, send_sem=hs.at[kind, d - 1], recv_sem=hr.at[kind, d - 1],
                device_id={"head": to}, device_id_type=MESH,
            )

    def start(copies):
        for copy in copies:
            copy.start()

    def received(copies):
        for copy in copies:
            copy.wait_recv()

    def make(j):
        which, begin, rows, y_first = jobs[j]
        if j < early:
            return None
        if not which:
            return pack

        def compute():
            if which == 1:
                need("mix_out", "cot")
                outer(mix_out, [cot.at[h] for h in range(peers_head)], out_part, begin, rows)
            else:
                need("normed", ("d_gate", "d_value")[which - 2])
                outer(normed, [(d_gate, d_value)[which - 2]], parts[which], begin, rows)

        return compute

    def over_head(quarter):
        if quarter == 0:
            need(*list(operands))
            for copy in loads:
                copy.wait()
            dots[...] = jnp.zeros_like(dots)
            gain_part[...] = jnp.zeros_like(gain_part)

        def by_head(h):
            mine = pl.ds(h * width, width)
            result = jnp.zeros((tokens, width), F32)
            for left_ref, right_ref in (
                (d_gate, gate_m), (d_value, value_m), (d_state, state_m)
            ):
                result = result + lax.dot_general(
                    left_ref[...], right_ref[mine], (((1,), (1,)), ((), ())), preferred_element_type=F32
                )
            result = result + jnp.dot(d_step[:, 0:heads], step_m[:, mine], preferred_element_type=F32)
            product[...] = result
            mixed_part[h] = jnp.dot(
                mix_out[...], out_m[:, mine], preferred_element_type=F32
            ).astype(BF16)

            @pl.loop(0, tokens // Q)
            def _(c):
                here = pl.ds(pl.multiple_of(c * Q, Q), Q)
                result = product[here]
                normed_part[h, here] = result.astype(BF16)
                rows = result * hidden[h, here].astype(F32)
                gain_part[:, mine] = gain_part[:, mine] + jnp.sum(
                    rows * scale[here], axis=0, keepdims=True
                )
                dot = jnp.sum(rows * gain[h, 0:1], axis=1, keepdims=True)
                dot = jnp.broadcast_to(dot, (Q, LANES)).T
                dots[0:8, here] = dots[0:8, here] + dot[:8]

        for h in range(quarter * peers_head // 4, (quarter + 1) * peers_head // 4):
            by_head(h)

    def over_head_send():
        states = blocks.shape[2]
        rest[...] = jnp.zeros_like(rest)
        rest[0:8] = grads_s[...]
        for k in range(features // states):
            rest[8 + k : 9 + k] = gain_part[:, pl.ds(k * states, states)]
        for h in range(peers_head):
            turned = normed[:, pl.ds(h * width, width)].T
            blocks[h, pl.ds(0, width)] = jnp.dot(
                turned, d_state[...], preferred_element_type=F32
            ).astype(BF16)
            blocks[h, pl.ds(width, 16)] = rest[0:16].astype(BF16)
        dots[8:16, 0:states] = grads_s[...]
        for kind in range(4):
            start(head_copies(kind))
        steps = lax.dot_general(
            d_step[...], normed[...], (((0,), (0,)), ((), ())), preferred_element_type=F32
        )
        for k in range(features // states):
            rest[16 + k * heads : 16 + (k + 1) * heads] = steps[:heads, k * states : (k + 1) * states]
        at = 16 + heads * (features // states)
        for k in range(0, channels, states):
            lanes = min(states, channels - k)
            rest[at : at + 8, 0:lanes] = grads_v[:, pl.ds(k, lanes)]
            at += 8
        rest[at : at + 2, 0:LANES] = grads_h[0:2]
        packed[pl.ds(block, rest.shape[0] - 16)] = rest[16:].astype(BF16)

    waited = []

    def dots_total():
        if not waited:
            waited.append(received(head_copies(1)))
        summed = dots[...]
        for d in range(peers_head - 1):
            summed = summed + dots_in[d]
        return summed

    def pack():
        received(head_copies(0))
        others = [(block_in.at[d], 0) for d in range(peers_head - 1)]
        add_rows((packed, 0), [(blocks.at[head], 0)] + others, block)
        filters = dots_total()[8:16, 0 : packed.shape[1]]
        kept = packed[pl.ds(width, 16)].astype(F32)
        packed[pl.ds(width, 16)] = jnp.concatenate([filters, kept[8:16]], axis=0).astype(BF16)

    def sum_heads():
        dots_sum[...] = dots_total()[0:8]
        for kind, mine, boxes, target in (
            (2, normed_part, normed_in, normed_sum), (3, mixed_part, mixed_in, mixed_sum)
        ):
            received(head_copies(kind))
            others = [(boxes.at[d], 0) for d in range(peers_head - 1)]
            add_rows((target, 0), [(mine.at[head], 0)] + others, tokens, F32)

    plans = [job.stages(make(job.index)) for job in work]

    def give():
        work[shared].keep().wait()
        work[shared].arrived()
        mine = pltpu.make_async_copy(outs[0].at[pl.ds(0, width)], every.at[head], local_sem.at[0])
        mine.start()
        start(head_copies(4))
        mine.wait()

    plans[shared].append(give)
    plans.append([functools.partial(over_head, q) for q in range(4)] + [over_head_send, sum_heads])
    for j, stage in order:
        plans[j][stage]()
    for job in work:
        job.close(job.index == shared)
    received(head_copies(4))
    for kind in range(5):
        for copy in head_copies(kind):
            copy.wait_send()


def sum_over_seq(plan, order, values, grads, weights, given, lines, peers_head, collective_id):
    normed, d_gate, d_state = values[0], values[6], values[8]
    tokens, features = normed.shape
    channels, states, width = d_gate.shape[1], d_state.shape[1], normed.shape[1] // peers_head
    heads = channels // HEAD
    shape, dma, vmem = jax.ShapeDtypeStruct, pltpu.SemaphoreType.DMA, pltpu.VMEM
    extra = heads * (features // states) + 8 * -(-channels // states) + 8
    total = -(-(width + 16 + extra) // (8 * lines * LINE)) * 8 * lines * LINE
    whole = [
        shape((total, states), BF16), shape((channels, features), BF16),
        shape((features, channels), BF16), shape((features, channels), BF16),
    ]
    jobs = rows_of(plan, [one.shape[0] for one in whole])
    count = len(jobs)
    scratch = job_scratch(jobs, [one.shape[1] for one in whole], lines, len(given))
    others = peers_head - 1
    scratch += [dma((count,))]
    scratch += [vmem(one.shape, BF16) for one in whole]
    scratch += [vmem(one.shape, BF16) for one in weights]
    scratch += [
        vmem((peers_head, width + 16, states), BF16), vmem((others, width + 16, states), BF16),
        vmem((peers_head, tokens, width), BF16), vmem((others, tokens, width), BF16),
        vmem((peers_head, tokens, width), BF16), vmem((others, tokens, width), BF16),
        vmem((16, tokens), F32), vmem((others, 16, tokens), F32), vmem((1, features), F32),
        vmem((total - width, states), F32), vmem((tokens, width), F32),
        dma((13,)), dma((5, others)), dma((5, others)),
    ]
    large = [0, 1, 2, 5, 6, 7, 8, 9]
    scratch += [vmem(values[k].shape, BF16) for k in large]
    anywhere, inside = pl.BlockSpec(memory_space=pl.ANY), pl.BlockSpec(memory_space=pltpu.VMEM)
    operands = [values[3], values[4], *grads] + [values[k] for k in large]
    return pl.pallas_call(
        functools.partial(sum_rows, jobs, order, lines, peers_head, len(given)),
        out_shape=whole
        + [shape((peers_head, width, states), BF16)]
        + [shape((tokens, width), F32)] * 2
        + [shape((8, tokens), F32)],
        in_specs=[inside] * 5 + [anywhere] * 13 + [inside] * len(given),
        out_specs=[anywhere] * 5 + [inside] * 3,
        scratch_shapes=scratch,
        compiler_params=pltpu.CompilerParams(
            collective_id=collective_id, has_side_effects=True, vmem_limit_bytes=61 * 1024 * 1024
        ),
    )(*operands, *weights, *given)


def finish_kernel(
    features, steps, out_sum, gate_sum, value_sum, state_sum, hidden, cot, scale, gain, normed_sum, mixed_sum,
    dots, extra,
    out_grad, gate_grad, value_grad, state_grad, block_out, delta_hidden, step_grad, filter_v, filter_s,
    norm_grad, offset_v, offset_s, bias_grad, decay_grad, skip_grad, mix_grad,
    small, row, flat, head_row, column,
):
    step = pl.program_id(0)
    width, channels = hidden.shape[1], filter_v.shape[1]
    heads, states = channels // HEAD, extra.shape[1]
    for source, target in (
        (out_sum, out_grad), (gate_sum, gate_grad), (value_sum, value_grad), (state_sum, state_grad)
    ):
        target[...] = source[...].astype(F32)
    rows = hidden[...].astype(F32)
    block_out[...] = (rows + mixed_sum[...]).astype(BF16)

    @pl.when(step == 0)
    def _():
        dot = jnp.broadcast_to(dots[0:1] / features, (Q, dots.shape[1]))
        column[...] = jnp.concatenate(
            [dot[:, c * Q : (c + 1) * Q].T for c in range(dots.shape[1] // Q)], axis=0
        )[:, 0:1]

    count = rows.shape[0]
    mine = column[pl.ds(pl.multiple_of(step * count, count), count)]
    size = scale[...]
    delta_hidden[...] = (
        cot[...].astype(F32)
        + size * (normed_sum[...] * gain[...].astype(F32).reshape(1, width))
        - rows * (size * size * size) * mine
    )

    @pl.when(step == 1)
    def _():
        small[...] = extra[...].astype(F32)
        at = width + 16
        tiles = features // states
        for k in range(tiles):
            step_grad[:, pl.ds(k * states, states)] = small[at + k * heads : at + (k + 1) * heads]
            flat[0:1, pl.ds(k * states, states)] = small[width + 8 + k : width + 9 + k]
        at += tiles * heads
        for k in range(0, channels, states):
            lanes = min(states, channels - k)
            row[:, pl.ds(k, lanes)] = small[at : at + 8, 0:lanes]
            at += 8
        filter_v[...] = row[0:4]
        filter_s[...] = small[width : width + 4]
        head = lax.axis_index("head")
        chosen = flat[0:1, 0:width]
        for h in range(1, features // width):
            chosen = jnp.where(head == h, flat[0:1, pl.ds(h * width, width)], chosen)
        norm_grad[...] = chosen.reshape(width)
        offset_v[...] = row[4:5].reshape(channels)
        offset_s[...] = small[width + 4 : width + 5].reshape(states)
        mix_grad[...] = row[5:6].reshape(channels)
        of_head = lax.broadcasted_iota(jnp.int32, (channels, LANES), 0) // HEAD
        lane = lax.broadcasted_iota(jnp.int32, (channels, LANES), 1)
        gather = jnp.where(of_head == lane, 1.0, 0.0)
        summed = jnp.dot(row[...], gather, precision=HIGH, preferred_element_type=F32)
        head_row[0:1] = small[at : at + 1, 0:LANES]
        head_row[1:2] = small[at + 1 : at + 2, 0:LANES]
        head_row[2:3] = summed[6:7]
        for k, target in enumerate((bias_grad, decay_grad, skip_grad)):
            target[...] = head_row[k : k + 1, 0:heads].reshape(heads)


def finish(out_sum, gate_sum, value_sum, state_sum, hidden, cot, scale, gain, normed_sum, mixed_sum, dots, extra):
    tokens, width = hidden.shape
    channels, features = out_sum.shape
    heads, states, steps = channels // HEAD, extra.shape[1], 8
    shape = jax.ShapeDtypeStruct

    def tiles(array):
        return pl.BlockSpec((array.shape[0] // steps, array.shape[1]), lambda k: (k, 0))

    def all_of(array):
        return pl.BlockSpec(array.shape, lambda k: (0,) * len(array.shape))

    state_sum = state_sum.reshape(features, states)
    tiled = [out_sum, gate_sum, value_sum, state_sum]
    rows = [hidden, cot, scale]
    outs = [shape(one.shape, F32) for one in tiled]
    outs += [shape(hidden.shape, BF16), shape(hidden.shape, F32)]
    small = [(heads, features), (4, channels), (4, states)]
    small += [(width,), (channels,), (states,), (heads,), (heads,), (heads,), (channels,)]
    small = [shape(one, F32) for one in small]
    return pl.pallas_call(
        functools.partial(finish_kernel, features, steps),
        grid=(steps,),
        out_shape=outs + small,
        in_specs=[tiles(one) for one in tiled + rows]
        + [all_of(gain), tiles(normed_sum), tiles(mixed_sum), all_of(dots), all_of(extra)],
        out_specs=[tiles(one) for one in outs] + [all_of(one) for one in small],
        scratch_shapes=[
            pltpu.VMEM(extra.shape, F32), pltpu.VMEM((8, channels), F32), pltpu.VMEM((8, features), F32),
            pltpu.VMEM((8, LANES), F32), pltpu.VMEM((tokens, 1), F32),
        ],
        compiler_params=pltpu.CompilerParams(dimension_semantics=("arbitrary",)),
    )(*tiled, *rows, gain, normed_sum, mixed_sum, dots, extra)


PLAN = (
    (1, 0, 3, True), (1, 1, 3, True), (1, 2, 3, True), (2, 0, 3, False),
    (2, 1, 3, True), (2, 2, 3, True), (0, 0, 1, True), (3, 0, 3, False),
    (3, 1, 3, True), (3, 2, 3, True),
)
EARLY = 2
WAVES = (
    ((0, 0),), (), (), ((1, 0),),
    (), (), (), ((0, 1),),
    (), (), (), ((1, 1),),
)
ORDER = (
    (0, 0), (2, 0), (10, 0), (3, 0), (5, 0), (0, 1), (4, 0), (0, 2), (10, 1), (0, 3),
    (10, 2), (3, 1), (0, 4), (10, 3), (2, 1), (3, 2), (5, 1), (2, 2), (10, 4), (9, 0),
    (5, 2), (3, 3), (2, 3), (5, 3), (4, 1), (4, 2), (2, 4), (3, 4), (1, 0), (5, 4),
    (2, 5), (6, 0), (4, 3), (3, 5), (0, 5), (4, 4), (9, 1), (1, 1), (8, 0), (3, 6),
    (1, 2), (0, 6), (7, 0), (3, 7), (1, 3), (9, 2), (5, 5), (6, 1), (2, 6), (9, 3),
    (7, 1), (4, 5), (5, 6), (9, 4), (7, 2), (6, 2), (9, 5), (6, 3), (8, 1), (4, 6),
    (7, 3), (8, 2), (5, 7), (2, 7), (3, 8), (9, 6), (6, 4), (7, 4), (6, 5), (8, 3),
    (8, 4), (1, 4), (6, 6), (1, 5), (7, 5), (6, 7), (9, 7), (4, 7), (10, 5), (8, 5),
    (7, 6), (1, 6), (6, 8), (8, 6), (8, 7), (7, 7), (7, 8),
)


def contract_rows(left, right):
    return lax.dot_general(
        left, right, (((0,), (0,)), ((), ())), preferred_element_type=jnp.float32
    )


def contract_cols(left, right):
    return lax.dot_general(
        left, right, (((1,), (1,)), ((), ())), preferred_element_type=jnp.float32
    )


def local(
    hidden_in,
    norm_gain,
    gate_weight,
    value_weight,
    step_weight,
    state_weight,
    value_filter,
    value_offset,
    state_filter,
    state_offset,
    step_bias,
    decay_log,
    skip_gain,
    mix_gain,
    out_weight,
    lengths,
    cotangent,
):
    tokens, width = hidden_in.shape
    heads, channels = step_weight.shape[1], value_weight.shape[1]
    count, peers_head = lax.axis_size("seq"), lax.axis_size("head")
    features = width * peers_head
    step_turned = step_weight.T
    normed, scale_in, *values = mix(
        count,
        peers_head,
        lengths,
        hidden_in,
        cotangent,
        (gate_weight, value_weight, state_weight, out_weight, step_turned),
        (value_filter, state_filter),
        norm_gain,
        (value_offset, mix_gain, state_offset, step_bias, decay_log, skip_gain),
        PLAN[:EARLY],
        WAVES,
        collective_id=2,
    )
    hidden_full, cot_full, gain_full, mix_out, d_gate, d_value, d_state, d_step = values[:8]
    grads_v, grads_s, grads_h = values[8:11]
    extra, out_sum, gate_sum, value_sum, state_sum, normed_sum, mixed_sum, dot_sum = sum_over_seq(
        PLAN,
        ORDER,
        (normed, cot_full, hidden_full, scale_in, gain_full, mix_out, d_gate, d_value, d_state, d_step),
        (grads_v, grads_s, grads_h),
        (gate_weight, value_weight, out_weight, state_weight, step_turned),
        values[11:],
        count // LINE,
        peers_head,
        3,
    )
    (
        out_grad, gate_grad, value_grad, state_grad, block_out, delta_hidden, step_grad, filter_v, filter_s,
        norm_grad, offset_v, offset_s, bias_grad, decay_grad, skip_grad, mix_grad,
    ) = finish(
        out_sum, gate_sum, value_sum, state_sum, hidden_in, cotangent, scale_in, norm_gain,
        normed_sum, mixed_sum, dot_sum, extra,
    )
    return (
        block_out,
        delta_hidden,
        norm_grad,
        gate_grad,
        value_grad,
        step_grad.T,
        state_grad,
        filter_v,
        offset_v,
        filter_s,
        offset_s,
        bias_grad,
        decay_grad,
        skip_grad,
        mix_grad,
        out_grad,
    )


def solution(mesh):
    in_specs = (
        P("seq", "head"),
        P("head"),
        P(None, "head"),
        P(None, "head"),
        P(None, "head"),
        P(),
        P(None, "head"),
        P("head"),
        P(),
        P(),
        P("head"),
        P("head"),
        P("head"),
        P("head"),
        P("head", None),
        P(),
        P("seq", "head"),
    )
    out_specs = (
        P("seq", "head"),
        P("seq", "head"),
        P("head"),
        P(None, "head"),
        P(None, "head"),
        P(None, "head"),
        P(),
        P(None, "head"),
        P("head"),
        P(),
        P(),
        P("head"),
        P("head"),
        P("head"),
        P("head"),
        P("head", None),
    )
    return jax.shard_map(local, mesh=mesh, in_specs=in_specs, out_specs=out_specs, check_vma=False)
```
